32 devices in a mesh: col: 4 (over z), row: 8 (over y, x, core).
Axes of the slice: x: 2, y: 2, z: 4, core: 2. Of those that a mesh axis runs over, the one named last changes fastest.
Arguments:
- vel_u: float32 [62, 1024, 256], P(None, 'row', 'col')
- vel_v: float32 [62, 1024, 256], P(None, 'row', 'col')
- temperature: float32 [62, 1024, 256], P(None, 'row', 'col')
- salinity: float32 [62, 1024, 256], P(None, 'row', 'col')
- sea_level: float32 [1024, 256], P('row', 'col')
- trans_u: float32 [1024, 256], P('row', 'col')
- trans_v: float32 [1024, 256], P('row', 'col')
- col_depth: float32 [1024, 256], P('row', 'col')
- kmt_levels: int32 [1024, 256], P('row', 'col')
Outputs:
- output 1: float32 [1024, 256], P('row', 'col')
- output 2: float32 [1024, 256], P('row', 'col')
- output 3: float32 [1024, 256], P('row', 'col')
- output 4: float32 [62, 1024, 256], P(None, 'row', 'col')
- output 5: float32 [62, 1024, 256], P(None, 'row', 'col')
- output 6: float32 [62, 1024, 256], P(None, 'row', 'col')
- output 7: float32 [62, 1024, 256], P(None, 'row', 'col')
All inputs are finite; a program needn't handle non-finite values.
Results may differ from the reference program's by a relative error of at most 0.001.
Values sent between devices are 32-bit elements.
A program may use at most 1 GiB of HBM per device.

```python
import jax
import jax.numpy as jnp
from jax import lax

LEVELS = 62
GRID_Y = 1024
GRID_X = 256
SUBCYCLES = 30
ADV_COURANT = 0.25
WAVE_COURANT = 0.5
VISC_NUM = 4.0
DIFF_NUM = 1.0
ALPHA_T = 0.3
BETA_S = 0.6


def setup_inputs(seed: int = 0) -> dict:
    sub_keys = jax.random.split(jax.random.key(seed), 12)
    kmt_draw = jax.random.randint(sub_keys[0], (GRID_Y, GRID_X), LEVELS // 3, LEVELS + 1)
    land_draw = jax.random.randint(sub_keys[1], (GRID_Y, GRID_X), 0, 8)
    kmt_levels = jnp.where(land_draw == 0, 0, kmt_draw).astype(jnp.int32)
    kmt_levels = kmt_levels.at[0, 0].set(0).at[0, 1].set(LEVELS)
    col_depth = jax.random.uniform(sub_keys[2], (GRID_Y, GRID_X), jnp.float32, 0.3, 1.0)
    level_frac = jnp.arange(LEVELS, dtype=jnp.float32)[:, None, None] / LEVELS
    shape_3d = (LEVELS, GRID_Y, GRID_X)
    plane_shape = (1, GRID_Y, GRID_X)
    temperature = 1.5 * (1.0 - 2.0 * level_frac) + jax.random.normal(sub_keys[3], plane_shape, jnp.float32) + 0.5 * jax.random.normal(sub_keys[4], shape_3d, jnp.float32)
    salinity = 0.8 * level_frac + 0.8 * jax.random.normal(sub_keys[5], plane_shape, jnp.float32) + 0.4 * jax.random.normal(sub_keys[6], shape_3d, jnp.float32)
    vel_u = 0.5 * jax.random.normal(sub_keys[7], shape_3d, jnp.float32)
    vel_v = 0.5 * jax.random.normal(sub_keys[8], shape_3d, jnp.float32)
    sea_level = 0.5 * jax.random.normal(sub_keys[9], (GRID_Y, GRID_X), jnp.float32)
    trans_u = 0.4 * jax.random.normal(sub_keys[10], (GRID_Y, GRID_X), jnp.float32)
    trans_v = 0.4 * jax.random.normal(sub_keys[11], (GRID_Y, GRID_X), jnp.float32)
    return {'vel_u': vel_u, 'vel_v': vel_v, 'temperature': temperature, 'salinity': salinity, 'sea_level': sea_level, 'trans_u': trans_u, 'trans_v': trans_v, 'col_depth': col_depth, 'kmt_levels': kmt_levels}


def pad_halo(field_in):
    wide_pad = jnp.concatenate([field_in[..., -1:], field_in, field_in[..., :1]], axis=-1)
    zero_row = jnp.zeros_like(wide_pad[..., :1, :])
    return jnp.concatenate([zero_row, wide_pad, zero_row], axis=-2)


def column_solve(wet_mask, diffusivity, rhs_list):
    link_mask = wet_mask[:-1] * wet_mask[1:]
    zero_level = jnp.zeros_like(wet_mask[:1])
    upper_band = diffusivity * jnp.concatenate([link_mask, zero_level], axis=0)
    lower_band = diffusivity * jnp.concatenate([zero_level, link_mask], axis=0)
    diag_band = 1.0 + upper_band + lower_band

    def forward(state_in, level_in):
        c_prev, d_prev = state_in
        up_k, lo_k, dg_k, rhs_k = level_in
        pivot = dg_k - lo_k * c_prev
        c_ratio = up_k / pivot
        d_new = tuple((r + lo_k * p) / pivot for r, p in zip(rhs_k, d_prev))
        return (c_ratio, d_new), (c_ratio, d_new)

    def backward(x_next, level_in):
        c_k, d_k = level_in
        x_new = tuple(d + c_k * x for d, x in zip(d_k, x_next))
        return x_new, x_new

    zero_plane = jnp.zeros_like(wet_mask[0])
    start_state = (zero_plane, tuple(zero_plane for _ in rhs_list))
    _, (c_all, d_all) = lax.scan(forward, start_state, (upper_band, lower_band, diag_band, tuple(rhs_list)))
    _, x_all = lax.scan(backward, tuple(zero_plane for _ in rhs_list), (c_all, d_all), reverse=True)
    return x_all


def upwind_div(u_pad, v_pad, tracer_pad, face_u, face_v):
    u_face = u_pad[:, 1:-1, :-1]
    flux_e = face_u[:, 1:-1, :] * (jnp.maximum(u_face, 0.0) * tracer_pad[:, 1:-1, :-1] + jnp.minimum(u_face, 0.0) * tracer_pad[:, 1:-1, 1:])
    v_face = v_pad[:, :-1, 1:-1]
    flux_n = face_v[:, :, 1:-1] * (jnp.maximum(v_face, 0.0) * tracer_pad[:, :-1, 1:-1] + jnp.minimum(v_face, 0.0) * tracer_pad[:, 1:, 1:-1])
    return flux_e[:, :, 1:] - flux_e[:, :, :-1] + flux_n[:, 1:, :] - flux_n[:, :-1, :]


def baroclinic(u_pad, v_pad, t_pad, s_pad, kmt_pad, depth_pad):
    level_idx = jnp.arange(u_pad.shape[0], dtype=jnp.int32)[:, None, None]
    cell_p = (level_idx < kmt_pad[None]).astype(jnp.float32)
    kmin_u = jnp.minimum(kmt_pad[:, :-1], kmt_pad[:, 1:])
    kmin_v = jnp.minimum(kmt_pad[:-1, :], kmt_pad[1:, :])
    face_u = (level_idx < kmin_u[None]).astype(jnp.float32)
    face_v = (level_idx < kmin_v[None]).astype(jnp.float32)
    thickness = depth_pad / jnp.maximum(kmt_pad, 1).astype(jnp.float32)
    density = (BETA_S * s_pad - ALPHA_T * t_pad) * cell_p
    pressure = (jnp.cumsum(density, axis=0) - 0.5 * density) * thickness[None]
    u_c = u_pad[:, 1:-1, 1:-1]
    v_c = v_pad[:, 1:-1, 1:-1]
    p_c = pressure[:, 1:-1, 1:-1]
    mask_u = face_u[:, 1:-1, 1:]
    mask_v = face_v[:, 1:, 1:-1]
    cell_c = cell_p[:, 1:-1, 1:-1]
    v_at_u = 0.25 * (v_c + v_pad[:, 1:-1, 2:] + v_pad[:, :-2, 1:-1] + v_pad[:, :-2, 2:])
    u_at_v = 0.25 * (u_c + u_pad[:, 1:-1, :-2] + u_pad[:, 2:, 1:-1] + u_pad[:, 2:, :-2])
    tend_u = mask_u * (p_c - pressure[:, 1:-1, 2:] - 0.5 * (u_c * (u_pad[:, 1:-1, 2:] - u_pad[:, 1:-1, :-2]) + v_at_u * (u_pad[:, 2:, 1:-1] - u_pad[:, :-2, 1:-1])))
    tend_v = mask_v * (p_c - pressure[:, 2:, 1:-1] - 0.5 * (u_at_v * (v_pad[:, 1:-1, 2:] - v_pad[:, 1:-1, :-2]) + v_c * (v_pad[:, 2:, 1:-1] - v_pad[:, :-2, 1:-1])))
    new_u = column_solve(mask_u, VISC_NUM, (mask_u * (u_c + ADV_COURANT * tend_u),))[0]
    new_v = column_solve(mask_v, VISC_NUM, (mask_v * (v_c + ADV_COURANT * tend_v),))[0]
    pred_t = cell_c * (t_pad[:, 1:-1, 1:-1] - ADV_COURANT * upwind_div(u_pad, v_pad, t_pad, face_u, face_v))
    pred_s = cell_c * (s_pad[:, 1:-1, 1:-1] - ADV_COURANT * upwind_div(u_pad, v_pad, s_pad, face_u, face_v))
    new_t, new_s = column_solve(cell_c, DIFF_NUM, (pred_t, pred_s))
    count_u = kmin_u[1:-1, 1:]
    count_v = kmin_v[1:, 1:-1]
    wet_u = (count_u > 0).astype(jnp.float32)
    wet_v = (count_v > 0).astype(jnp.float32)
    wet_c = (kmt_pad[1:-1, 1:-1] > 0).astype(jnp.float32)
    inv_u = 1.0 / jnp.maximum(count_u, 1).astype(jnp.float32)
    inv_v = 1.0 / jnp.maximum(count_v, 1).astype(jnp.float32)
    depth_u = 0.5 * (depth_pad[1:-1, 1:-1] + depth_pad[1:-1, 2:]) * wet_u
    depth_v = 0.5 * (depth_pad[1:-1, 1:-1] + depth_pad[2:, 1:-1]) * wet_v
    force_u = depth_u * inv_u * jnp.sum(tend_u, axis=0)
    force_v = depth_v * inv_v * jnp.sum(tend_v, axis=0)
    base_u = new_u - mask_u * (inv_u * jnp.sum(new_u, axis=0))[None]
    base_v = new_v - mask_v * (inv_v * jnp.sum(new_v, axis=0))[None]
    return (base_u, base_v, mask_u, mask_v, new_t, new_s, force_u, force_v, depth_u, depth_v, wet_u, wet_v, wet_c)


def sm_weights():
    frac_step = jnp.arange(1, SUBCYCLES + 1, dtype=jnp.float32) / (SUBCYCLES + 1)
    raw_shape = frac_step ** 2 * (1.0 - frac_step ** 4)
    return raw_shape / jnp.sum(raw_shape)


def barotropic_whole(sea_level, trans_u, trans_v, force_u, force_v, depth_u, depth_v, wet_u, wet_v, wet_c):
    wave_u = WAVE_COURANT * depth_u
    wave_v = WAVE_COURANT * depth_v
    push_u = (ADV_COURANT / SUBCYCLES) * force_u
    push_v = (ADV_COURANT / SUBCYCLES) * force_v

    def subcycle(state_in, weight):
        level_now, flow_u, flow_v, mean_u, mean_v = state_in
        west_u = jnp.roll(flow_u, 1, axis=1)
        south_v = jnp.concatenate([jnp.zeros_like(flow_v[:1]), flow_v[:-1]], axis=0)
        level_new = wet_c * (level_now - WAVE_COURANT * (flow_u - west_u + flow_v - south_v))
        east_level = jnp.roll(level_new, -1, axis=1)
        north_level = jnp.concatenate([level_new[1:], jnp.zeros_like(level_new[:1])], axis=0)
        flow_u = wet_u * (flow_u - wave_u * (east_level - level_new) + push_u)
        flow_v = wet_v * (flow_v - wave_v * (north_level - level_new) + push_v)
        return (level_new, flow_u, flow_v, mean_u + weight * flow_u, mean_v + weight * flow_v), None

    start_state = (wet_c * sea_level, wet_u * trans_u, wet_v * trans_v, jnp.zeros_like(trans_u), jnp.zeros_like(trans_v))
    final_state, _ = lax.scan(subcycle, start_state, sm_weights())
    return final_state


def finish(base_vel, face_mask, mean_flow, face_depth):
    return base_vel + face_mask * (mean_flow / jnp.where(face_depth > 0, face_depth, 1.0))[None]


def reference(vel_u, vel_v, temperature, salinity, sea_level, trans_u, trans_v, col_depth, kmt_levels):
    (base_u, base_v, mask_u, mask_v, new_t, new_s, force_u, force_v, depth_u, depth_v, wet_u, wet_v, wet_c) = baroclinic(pad_halo(vel_u), pad_halo(vel_v), pad_halo(temperature), pad_halo(salinity), pad_halo(kmt_levels), pad_halo(col_depth))
    level_new, flow_u, flow_v, mean_u, mean_v = barotropic_whole(sea_level, trans_u, trans_v, force_u, force_v, depth_u, depth_v, wet_u, wet_v, wet_c)
    return (level_new, flow_u, flow_v, finish(base_u, mask_u, mean_u, depth_u), finish(base_v, mask_v, mean_v, depth_v), new_t, new_s)
```

```python
import functools

import jax
import jax.numpy as jnp
import numpy as np
from jax import lax
from jax.experimental import pallas as pl
from jax.experimental.pallas import tpu as pltpu
from jax.sharding import PartitionSpec as P

LEVELS = 62
NI = 64
NJ = 128
HALO = 32
SUBCYCLES = 30
ADV_COURANT = 0.25
WAVE_COURANT = 0.5
VISC_NUM = 4.0
DIFF_NUM = 1.0
ALPHA_T = 0.3
BETA_S = 0.6

F32 = jnp.float32
MESH = pl.DeviceIdType.MESH
VMEM = pltpu.VMEM
OFF = 8
IPAD = NI + 16
IEXT = NI + 2 * HALO
JEXT = NJ + 2 * HALO


def solve_constants(diff):
    ratio, inner, last = [], [], []
    c_prev = 0.0
    for k in range(LEVELS):
        lower = diff if k > 0 else 0.0
        pivot = 1.0 + diff + lower - lower * c_prev
        inner.append(1.0 / pivot)
        last.append(1.0 / (1.0 + lower - lower * c_prev))
        c_prev = diff / pivot
        ratio.append(c_prev)
    return ratio, inner, last


RATIO_V, INNER_V, LAST_V = solve_constants(VISC_NUM)
RATIO_D, INNER_D, LAST_D = solve_constants(DIFF_NUM)


def sm_weights():
    s = np.arange(1, SUBCYCLES + 1, dtype=np.float64) / (SUBCYCLES + 1)
    raw = s ** 2 * (1.0 - s ** 4)
    return 1.0 / np.sum(raw)


W_NORM = float(sm_weights())


def rot(x, shift, axis=1):
    n = x.shape[axis]
    shift = shift % n
    return x if shift == 0 else pltpu.roll(x, shift, axis)


def exchange_kernel(
    col_count, row_count,
    u_hbm, v_hbm, t_hbm, s_hbm, eta_hbm, tu_hbm, tv_hbm, dep_hbm, kmt_hbm,
    du_o, dv_o, dt_o, ds_o, flat_o,
    u3, v3, t3, s3, p3, st2, kmt_i, ext2, pk2n, pk2s, hs2, hn2,
    pack, mn, ms, in_s, in_n, rr,
    ff, extf, pkfn, pkfs, hsf, hnf,
    kmu, kmw, kmv, kmc, hu2, hv2, smt, smr,
    b_eta, b_u, b_v, b_wu, b_wv, b_pu, b_pv, b_mu, b_mv,
    ld3, ld2, snd, rcv,
):
    c = lax.axis_index("col")
    r = lax.axis_index("row")
    has_n = r < row_count - 1
    has_s = r > 0
    east = lax.rem(c + 1, col_count)
    west = lax.rem(c + col_count - 1, col_count)
    up, down = r + 1, r - 1

    loads3 = []
    for f, (src, dst) in enumerate(((t_hbm, t3), (s_hbm, s3), (u_hbm, u3), (v_hbm, v3))):
        cp = pltpu.make_async_copy(src, dst.at[:, OFF:OFF + NI, :], ld3.at[f])
        cp.start()
        loads3.append(cp)
    loads2 = []
    for f, src in enumerate((eta_hbm, tu_hbm, tv_hbm, dep_hbm)):
        loads2.append(pltpu.make_async_copy(src, st2.at[f], ld2.at[f]))
    loads2.append(pltpu.make_async_copy(kmt_hbm, kmt_i, ld2.at[4]))
    for cp in loads2:
        cp.start()

    barrier = pltpu.get_barrier_semaphore()

    def greet(cc, row):
        pl.semaphore_signal(barrier, inc=1, device_id=(cc, row), device_id_type=MESH)

    greet(east, r)
    greet(west, r)

    @pl.when(has_n)
    def _():
        for cc in (west, c, east):
            greet(cc, up)

    @pl.when(has_s)
    def _():
        for cc in (west, c, east):
            greet(cc, down)

    pl.semaphore_wait(barrier, 2 + 3 * has_n.astype(jnp.int32) + 3 * has_s.astype(jnp.int32))

    def remote(n, src, dst, cc, row):
        return pltpu.make_async_remote_copy(
            src_ref=src, dst_ref=dst, send_sem=snd.at[n], recv_sem=rcv.at[n],
            device_id=(cc, row), device_id_type=MESH)

    g1 = []
    for f, (src, dst) in enumerate(((u_hbm, u3), (v_hbm, v3), (t_hbm, t3), (s_hbm, s3))):
        g1.append(remote(2 * f, src.at[:, NI - 1:NI, :], dst.at[:, OFF - 1:OFF, :], east, r))
        g1.append(remote(2 * f + 1, src.at[:, 0:1, :], dst.at[:, OFF + NI:OFF + NI + 1, :], west, r))
    for cp in g1:
        cp.start()

    for cp in loads2:
        cp.wait()
    st2[4] = kmt_i[...].astype(F32)

    def flat_messages(base, own, ext, pn, ps, hs, hn):
        ew = [
            remote(base, own.at[:, NI - HALO:NI, :], ext.at[:, 0:HALO, :], east, r),
            remote(base + 1, own.at[:, 0:HALO, :], ext.at[:, HALO + NI:IEXT, :], west, r),
        ]
        no = [
            remote(base + 2, pn, hs.at[:, HALO:HALO + NI, :], c, up),
            remote(base + 3, pn.at[:, NI - HALO:NI, :], hs.at[:, 0:HALO, :], east, up),
            remote(base + 4, pn.at[:, 0:HALO, :], hs.at[:, HALO + NI:IEXT, :], west, up),
        ]
        so = [
            remote(base + 5, ps, hn.at[:, HALO:HALO + NI, :], c, down),
            remote(base + 6, ps.at[:, NI - HALO:NI, :], hn.at[:, 0:HALO, :], east, down),
            remote(base + 7, ps.at[:, 0:HALO, :], hn.at[:, HALO + NI:IEXT, :], west, down),
        ]
        return ew, no, so

    def start_all(ew, no, so):
        for cp in ew:
            cp.start()

        @pl.when(has_n)
        def _():
            for cp in no:
                cp.start()

        @pl.when(has_s)
        def _():
            for cp in so:
                cp.start()

    def wait_recv_all(ew, no, so):
        for cp in ew:
            cp.wait_recv()

        @pl.when(has_s)
        def _():
            for cp in no:
                cp.wait_recv()

        @pl.when(has_n)
        def _():
            for cp in so:
                cp.wait_recv()

    def wait_send_all(ew, no, so):
        for cp in ew:
            cp.wait_send()

        @pl.when(has_n)
        def _():
            for cp in no:
                cp.wait_send()

        @pl.when(has_s)
        def _():
            for cp in so:
                cp.wait_send()

    def pack_flat(fields, src, pn, ps):
        lane = lax.broadcasted_iota(jnp.int32, (NI, NJ), 1) // HALO
        for a in range((fields + 3) // 4):
            top = jnp.zeros((NI, NJ), F32)
            bot = jnp.zeros((NI, NJ), F32)
            for q in range(min(4, fields - 4 * a)):
                x = src[4 * a + q]
                top = jnp.where(lane == q, rot(x, HALO * q + HALO), top)
                bot = jnp.where(lane == q, rot(x, HALO * q), bot)
            pn[a] = top
            ps[a] = bot

    pack_flat(5, st2, pk2n, pk2s)
    g2 = flat_messages(8, st2, ext2, pk2n, pk2s, hs2, hn2)
    start_all(*g2)
    for f in range(5):
        ext2[f, HALO:HALO + NI, :] = st2[f]

    lane8 = lax.broadcasted_iota(jnp.int32, (8, NJ), 1)
    slot8 = lane8 >> 1
    even8 = (lane8 & 1) == 0
    first8 = lane8 == 0
    last8 = lane8 == NJ - 1

    def rows(ib, off=0):
        return pl.ds(pl.multiple_of(ib * 8, 8) + off, 8)

    def pack_edges(f, ref):
        def body(ib, carry):
            acc = jnp.zeros((8, NJ), F32)
            for k in range(LEVELS):
                acc = jnp.where(slot8 == k, rot(ref[k, rows(ib, OFF), :], 2 * k + 1), acc)
            pack[f, rows(ib), :] = acc
            return carry
        lax.fori_loop(0, NI // 8, body, 0)

    loads3[0].wait()
    pack_edges(2, t3)
    loads3[1].wait()
    pack_edges(3, s3)
    loads3[2].wait()
    pack_edges(0, u3)
    loads3[3].wait()
    pack_edges(1, v3)

    def pair_body(ib, carry):
        for a in range(2):
            x = pack[2 * a, rows(ib), :]
            y = pack[2 * a + 1, rows(ib), :]
            mn[a, rows(ib), :] = jnp.where(even8, y, rot(x, 1))
            ms[a, rows(ib), :] = jnp.where(even8, rot(x, -1), y)
        return carry
    lax.fori_loop(0, NI // 8, pair_body, 0)

    g3n = [
        remote(16, mn, in_s.at[:, OFF:OFF + NI, :], c, up),
        remote(17, mn.at[0, 0:8, :], in_s.at[0, OFF + NI:IPAD, :], west, up),
    ]
    g3s = [
        remote(18, ms, in_n.at[:, OFF:OFF + NI, :], c, down),
        remote(19, ms.at[0, NI - 8:NI, :], in_n.at[0, 0:OFF, :], east, down),
    ]
    start_all((), g3n, g3s)

    wait_recv_all(*g2)
    has_nf = jnp.where(has_n, 1.0, 0.0).astype(F32)
    has_sf = jnp.where(has_s, 1.0, 0.0).astype(F32)
    big_n = jnp.full((NI, 1), has_nf) > 0.5
    big_s = jnp.full((NI, 1), has_sf) > 0.5
    kmt = st2[4]
    depth = st2[3]
    kmt_n = jnp.where(big_n, hn2[1, HALO:HALO + NI, 0:1], 0.0)
    dep_n = jnp.where(big_n, hn2[0, HALO:HALO + NI, 3 * HALO:3 * HALO + 1], 0.0)
    kmt_s = jnp.where(big_s, hs2[1, HALO:HALO + NI, HALO - 1:HALO], 0.0)
    lane64 = lax.broadcasted_iota(jnp.int32, (NI, NJ), 1)
    kmt_north = jnp.where(lane64 == NJ - 1, kmt_n, rot(kmt, -1))
    dep_north = jnp.where(lane64 == NJ - 1, dep_n, rot(depth, -1))
    kmt_east = ext2[4, HALO + 1:HALO + NI + 1, :]
    dep_east = ext2[3, HALO + 1:HALO + NI + 1, :]
    kmu_v = jnp.minimum(kmt, kmt_east)
    kmv_v = jnp.minimum(kmt, kmt_north)
    kmu[...] = kmu_v
    kmw[...] = jnp.minimum(kmt, ext2[4, HALO - 1:HALO + NI - 1, :])
    kmv[...] = kmv_v
    hu2[...] = jnp.where(kmu_v > 0, 0.5 * (depth + dep_east), 0.0)
    hv2[...] = jnp.where(kmv_v > 0, 0.5 * (depth + dep_north), 0.0)

    def pressure_body(ib, carry):
        km = st2[4, rows(ib), :]
        thick = st2[3, rows(ib), :] / jnp.maximum(km, 1.0)
        total = jnp.zeros((8, NJ), F32)
        for k in range(LEVELS):
            dens = BETA_S * s3[k, rows(ib, OFF), :] - ALPHA_T * t3[k, rows(ib, OFF), :]
            dens = jnp.where(km > k, dens, 0.0)
            total = total + dens
            p3[k, rows(ib, OFF), :] = (total - 0.5 * dens) * thick
        return carry
    lax.fori_loop(0, NI // 8, pressure_body, 0)

    wait_recv_all((), g3n, g3s)
    pad_even = (lax.broadcasted_iota(jnp.int32, (IPAD, NJ), 1) & 1) == 0
    keep_n = jnp.full((IPAD, NJ), has_nf) > 0.5
    keep_s = jnp.full((IPAD, NJ), has_sf) > 0.5
    halo = []
    for a in range(2):
        north = jnp.where(keep_n, in_n[a], 0.0)
        south = jnp.where(keep_s, in_s[a], 0.0)
        halo.append(jnp.where(pad_even, north, south))
        halo.append(jnp.where(pad_even, rot(north, -1), rot(south, 1)))
    slot64 = lane64 >> 1
    even64 = (lane64 & 1) == 0
    for f in range(4):
        rr[f] = halo[f]
    own = slice(OFF, OFF + NI)
    ru, rv, rt, rs = (rr[f, own, :] for f in range(4))
    mean_n = ru + rr[0, OFF - 1:OFF + NI - 1, :]
    mean_s = rv + rr[1, OFF + 1:OFF + NI + 1, :]
    rr[4, own, :] = jnp.where(even64, mean_n, mean_s)
    dens = jnp.where((kmt_n > slot64.astype(F32)) & even64, BETA_S * rs - ALPHA_T * rt, 0.0)
    total = dens
    step = 2
    while step < 2 * LEVELS:
        total = total + jnp.where(lane64 >= step, rot(total, step), 0.0)
        step *= 2
    rr[5, own, :] = (total - 0.5 * dens) * (dep_n / jnp.maximum(kmt_n, 1.0))
    face_s = jnp.minimum(kmt_s, kmt[:, 0:1]) > slot64.astype(F32)
    vs_pos = jnp.where(face_s, jnp.maximum(rv, 0.0), 0.0)
    vs_neg = jnp.where(face_s, jnp.minimum(rv, 0.0), 0.0)
    rr[6, own, :] = jnp.where(even64, rt, vs_pos * rt + vs_neg * pack[2])
    rr[7, own, :] = jnp.where(even64, rs, vs_pos * rs + vs_neg * pack[3])

    def momentum_body(ib):
        km_u = kmu[rows(ib), :]
        km_v = kmv[rows(ib), :]
        qu, qv, qm, qp = (rr[f, rows(ib, OFF), :] for f in (0, 1, 4, 5))
        zero = jnp.zeros((8, NJ), F32)
        du, dv, st_u, st_v, sr_u, sr_v = (zero,) * 6
        for k in range(LEVELS):
            sh = NJ - 1 - 2 * k
            hu, hv, hm, hp = rot(qu, sh), rot(qv, sh), rot(qm, sh), rot(qp, sh)
            u = u3[k, rows(ib, OFF), :]
            ue = u3[k, rows(ib, OFF + 1), :]
            uw = u3[k, rows(ib, OFF - 1), :]
            v = v3[k, rows(ib, OFF), :]
            ve = v3[k, rows(ib, OFF + 1), :]
            vw = v3[k, rows(ib, OFF - 1), :]
            p = p3[k, rows(ib, OFF), :]
            pe = p3[k, rows(ib, OFF + 1), :]
            un = jnp.where(last8, hu, rot(u, -1))
            us = jnp.where(first8, hu, rot(u, 1))
            vn = jnp.where(last8, hv, rot(v, -1))
            vs = jnp.where(first8, hv, rot(v, 1))
            a = v + ve
            b = u + uw
            vm4 = a + jnp.where(first8, hm, rot(a, 1))
            um4 = b + jnp.where(last8, hm, rot(b, -1))
            pn = jnp.where(last8, hp, rot(p, -1))
            tu = (p - pe) - 0.5 * (u * (ue - uw)) - 0.125 * (vm4 * (un - us))
            tv = (p - pn) - 0.125 * (um4 * (ve - vw)) - 0.5 * (v * (vn - vs))
            wu = km_u > k
            wv = km_v > k
            tu = jnp.where(wu, tu, 0.0)
            tv = jnp.where(wv, tv, 0.0)
            ru_k = jnp.where(wu, u, 0.0) + ADV_COURANT * tu
            rv_k = jnp.where(wv, v, 0.0) + ADV_COURANT * tv
            st_u = st_u + tu
            st_v = st_v + tv
            sr_u = sr_u + ru_k
            sr_v = sr_v + rv_k
            fu = jnp.where(km_u > k + 1, INNER_V[k], jnp.where(wu, LAST_V[k], 0.0))
            fv = jnp.where(km_v > k + 1, INNER_V[k], jnp.where(wv, LAST_V[k], 0.0))
            if k > 0:
                ru_k = ru_k + VISC_NUM * du
                rv_k = rv_k + VISC_NUM * dv
            du = ru_k * fu
            dv = rv_k * fv
            du_o[k, rows(ib), :] = du
            dv_o[k, rows(ib), :] = dv
        inv_u = 1.0 / jnp.maximum(km_u, 1.0)
        inv_v = 1.0 / jnp.maximum(km_v, 1.0)
        ff[0, rows(ib), :] = hu2[rows(ib), :] * inv_u * st_u
        ff[1, rows(ib), :] = hv2[rows(ib), :] * inv_v * st_v
        smr[0, rows(ib), :] = inv_u * sr_u
        smr[1, rows(ib), :] = inv_v * sr_v

    def loop_body(ib, carry):
        momentum_body(ib)
        return carry

    blocks = NI // 8
    lax.fori_loop(1, blocks - 1, loop_body, 0)
    for cp in g1:
        cp.wait_recv()
    thick_e = ext2[3, HALO + NI:HALO + NI + 1, :] / jnp.maximum(ext2[4, HALO + NI:HALO + NI + 1, :], 1.0)
    km_e = ext2[4, HALO + NI:HALO + NI + 1, :]
    tot_e = jnp.zeros((1, NJ), F32)
    edge = slice(OFF + NI, OFF + NI + 1)
    for k in range(LEVELS):
        dens_e = jnp.where(km_e > k, BETA_S * s3[k, edge, :] - ALPHA_T * t3[k, edge, :], 0.0)
        tot_e = tot_e + dens_e
        p3[k, edge, :] = (tot_e - 0.5 * dens_e) * thick_e

    def edge_body(n, carry):
        momentum_body(n * (blocks - 1))
        return carry
    lax.fori_loop(0, 2, edge_body, 0)

    pack_flat(2, ff, pkfn, pkfs)
    g4 = flat_messages(20, ff, extf, pkfn, pkfs, hsf, hnf)
    start_all(*g4)
    for f in range(2):
        extf[f, HALO:HALO + NI, :] = ff[f]

    def tracer_body(ib, carry):
        km_u = kmu[rows(ib), :]
        km_w = kmw[rows(ib), :]
        km_v = kmv[rows(ib), :]
        km = st2[4, rows(ib), :]
        qt = rr[6, rows(ib, OFF), :]
        qs = rr[7, rows(ib, OFF), :]
        zero = jnp.zeros((8, NJ), F32)
        prev = [zero, zero]
        for k in range(LEVELS):
            sh = NJ - 1 - 2 * k
            u = jnp.where(km_u > k, u3[k, rows(ib, OFF), :], 0.0)
            w = jnp.where(km_w > k, u3[k, rows(ib, OFF - 1), :], 0.0)
            v = jnp.where(km_v > k, v3[k, rows(ib, OFF), :], 0.0)
            u_pos, u_neg = jnp.maximum(u, 0.0), jnp.minimum(u, 0.0)
            w_pos, w_neg = jnp.maximum(w, 0.0), jnp.minimum(w, 0.0)
            v_pos, v_neg = jnp.maximum(v, 0.0), jnp.minimum(v, 0.0)
            fac = jnp.where(km > k + 1, INNER_D[k], jnp.where(km > k, LAST_D[k], 0.0))
            for n, (ref, q, out) in enumerate(((t3, qt, dt_o), (s3, qs, ds_o))):
                x = ref[k, rows(ib, OFF), :]
                xe = ref[k, rows(ib, OFF + 1), :]
                xw = ref[k, rows(ib, OFF - 1), :]
                h = rot(q, sh)
                xn = jnp.where(last8, h, rot(x, -1))
                fe = u_pos * x + u_neg * xe
                fw = w_pos * xw + w_neg * x
                fn = v_pos * x + v_neg * xn
                fs = jnp.where(first8, h, rot(fn, 1))
                rhs = x - ADV_COURANT * ((fe - fw) + (fn - fs))
                if k > 0:
                    rhs = rhs + DIFF_NUM * prev[n]
                prev[n] = rhs * fac
                out[k, rows(ib), :] = prev[n]
        return carry
    lax.fori_loop(0, blocks, tracer_body, 0)

    def window(f, ext, hs, hn):
        a, q = f // 4, f % 4
        low = jnp.where(jnp.full((HALO, IEXT), has_sf) > 0.5, hs[a][HALO * q:HALO * (q + 1)], 0.0)
        high = jnp.where(jnp.full((HALO, IEXT), has_nf) > 0.5, hn[a][HALO * q:HALO * (q + 1)], 0.0)
        return jnp.concatenate([low, ext[f].T, high], axis=0)

    hs_t = [hs2[a].T for a in range(2)]
    hn_t = [hn2[a].T for a in range(2)]
    win = pl.ds(8, JEXT)
    zpad = jnp.zeros((8, IEXT), F32)
    b_v[0:8, :] = zpad
    b_eta[8 + JEXT:16 + JEXT, :] = zpad
    b_mu[win, :] = window(4, ext2, hs_t, hn_t)
    b_mu[8 + JEXT:16 + JEXT, :] = zpad
    b_mv[win, :] = window(3, ext2, hs_t, hn_t)
    b_mv[8 + JEXT:16 + JEXT, :] = zpad
    km_w = b_mu[win, :]
    dp_w = b_mv[win, :]
    wet_u = jnp.minimum(km_w, rot(km_w, -1)) > 0
    wet_v = jnp.minimum(km_w, b_mu[pl.ds(9, JEXT), :]) > 0
    b_wu[...] = jnp.where(wet_u, (0.5 * WAVE_COURANT) * (dp_w + rot(dp_w, -1)), 0.0)
    b_wv[...] = jnp.where(wet_v, (0.5 * WAVE_COURANT) * (dp_w + b_mv[pl.ds(9, JEXT), :]), 0.0)
    b_eta[win, :] = jnp.where(km_w > 0, window(0, ext2, hs_t, hn_t), 0.0)
    b_u[...] = jnp.where(wet_u, window(1, ext2, hs_t, hn_t), 0.0)
    b_v[win, :] = jnp.where(wet_v, window(2, ext2, hs_t, hn_t), 0.0)

    wait_recv_all(*g4)
    hsf_t = [hsf[0].T]
    hnf_t = [hnf[0].T]
    push = ADV_COURANT / SUBCYCLES
    b_pu[...] = jnp.where(wet_u, push * window(0, extf, hsf_t, hnf_t), 0.0)
    b_pv[...] = jnp.where(wet_v, push * window(1, extf, hsf_t, hnf_t), 0.0)
    b_mu[...] = jnp.zeros_like(b_mu)
    b_mv[...] = jnp.zeros_like(b_mv)

    def subcycle(n, carry):
        s = (n + 1).astype(F32) * (1.0 / (SUBCYCLES + 1))
        weight = (s * s) * (1.0 - (s * s) * (s * s)) * W_NORM
        u = b_u[...]
        v = b_v[win, :]
        eta = b_eta[win, :] - WAVE_COURANT * ((u - rot(u, 1)) + (v - b_v[pl.ds(7, JEXT), :]))
        b_eta[win, :] = eta
        u = u - b_wu[...] * (rot(eta, -1) - eta) + b_pu[...]
        v = v - b_wv[...] * (b_eta[pl.ds(9, JEXT), :] - eta) + b_pv[...]
        b_u[...] = u
        b_v[win, :] = v
        b_mu[win, :] += weight * u
        b_mv[win, :] += weight * v
        return carry
    lax.fori_loop(0, SUBCYCLES, subcycle, 0)

    mid = pl.ds(8 + HALO, NJ)
    cols = slice(HALO, HALO + NI)
    flat_o[0] = b_eta[mid, :].T[cols]
    flat_o[1] = b_u[pl.ds(HALO, NJ), :].T[cols]
    flat_o[2] = b_v[mid, :].T[cols]
    for f, (mean, depth_ref, km_ref) in enumerate(((b_mu, hu2, kmu), (b_mv, hv2, kmv))):
        d = depth_ref[...]
        flat_o[3 + f] = mean[mid, :].T[cols] / jnp.where(d > 0, d, 1.0) - smr[f]
        flat_o[5 + f] = km_ref[...]

    for cp in g1:
        cp.wait_send()
    wait_send_all(*g2)
    wait_send_all((), g3n, g3s)
    wait_send_all(*g4)


CHUNKS = ((46, 62), (30, 46), (14, 30), (0, 14))


def back_kernel(du, dv, dt, ds, flat, eta_h, tu_h, tv_h, u_h, v_h, t_h, s_h, xu, xv, xt, xs, sem2, sem3):
    copies = [pltpu.make_async_copy(flat.at[f], out, sem2.at[f]) for f, out in enumerate((eta_h, tu_h, tv_h))]
    for cp in copies:
        cp.start()
    for n, (lo, hi) in enumerate(CHUNKS):
        def body(ib, carry):
            rows = pl.ds(pl.multiple_of(ib * 8, 8), 8)
            cu, cv, ku, kv = (flat[f, rows, :] for f in (3, 4, 5, 6))
            if hi == LEVELS:
                x = [jnp.zeros((8, NJ), F32) for _ in range(4)]
            else:
                x = [ref[rows, :] for ref in (carry_refs)]
            for k in range(hi - 1, lo - 1, -1):
                x[0] = du[k, rows, :] + RATIO_V[k] * x[0]
                x[1] = dv[k, rows, :] + RATIO_V[k] * x[1]
                x[2] = dt[k, rows, :] + RATIO_D[k] * x[2]
                x[3] = ds[k, rows, :] + RATIO_D[k] * x[3]
                xu[k, rows, :] = jnp.where(ku > k, x[0] + cu, 0.0)
                xv[k, rows, :] = jnp.where(kv > k, x[1] + cv, 0.0)
                xt[k, rows, :] = x[2]
                xs[k, rows, :] = x[3]
            for ref, val in zip(carry_refs, x):
                ref[rows, :] = val
            return carry
        carry_refs = (xu.at[LEVELS], xv.at[LEVELS], xt.at[LEVELS], xs.at[LEVELS])
        lax.fori_loop(0, NI // 8, body, 0)
        for f, (src, out) in enumerate(((xu, u_h), (xv, v_h), (xt, t_h), (xs, s_h))):
            cp = pltpu.make_async_copy(src.at[lo:hi], out.at[lo:hi], sem3.at[n, f])
            cp.start()
            copies.append(cp)
    for cp in copies:
        cp.wait()


def solution(mesh):
    col_count = mesh.shape['col']
    row_count = mesh.shape['row']

    def ocean_step(*args):
        flipped = [jnp.swapaxes(x, -1, -2) for x in args]
        cube = (LEVELS, NI, NJ)
        flat = (NI, NJ)
        dma = pltpu.SemaphoreType.DMA
        hbm = pl.BlockSpec(memory_space=pltpu.HBM)
        vmem = pl.BlockSpec(memory_space=VMEM)
        padded = VMEM((LEVELS, IPAD, NJ), F32)
        wide = VMEM((JEXT + 16, IEXT), F32)
        plain = VMEM((JEXT, IEXT), F32)
        inner = pl.pallas_call(
            functools.partial(exchange_kernel, col_count, row_count),
            out_shape=tuple(VMEM(cube, F32) for _ in range(4)) + (VMEM((7,) + flat, F32),),
            in_specs=[hbm] * 9,
            out_specs=(vmem,) * 5,
            scratch_shapes=[
                padded, padded, padded, padded, padded,
                VMEM((5,) + flat, F32), VMEM(flat, jnp.int32), VMEM((5, IEXT, NJ), F32),
                VMEM((2,) + flat, F32), VMEM((2,) + flat, F32),
                VMEM((2, IEXT, NJ), F32), VMEM((2, IEXT, NJ), F32),
                VMEM((4,) + flat, F32), VMEM((2,) + flat, F32), VMEM((2,) + flat, F32),
                VMEM((2, IPAD, NJ), F32), VMEM((2, IPAD, NJ), F32), VMEM((8, IPAD, NJ), F32),
                VMEM((2,) + flat, F32), VMEM((2, IEXT, NJ), F32),
                VMEM((1,) + flat, F32), VMEM((1,) + flat, F32),
                VMEM((1, IEXT, NJ), F32), VMEM((1, IEXT, NJ), F32),
                VMEM(flat, F32), VMEM(flat, F32), VMEM(flat, F32), VMEM(flat, F32),
                VMEM(flat, F32), VMEM(flat, F32), VMEM((2,) + flat, F32), VMEM((2,) + flat, F32),
                wide, plain, wide, plain, plain, plain, plain, wide, wide,
                dma((4,)), dma((5,)), dma((28,)), dma((28,)),
            ],
            compiler_params=pltpu.CompilerParams(
                collective_id=0, has_side_effects=True, vmem_limit_bytes=54 * 2 ** 20),
        )(*flipped)
        spare = VMEM((LEVELS + 1,) + flat, F32)
        outs = pl.pallas_call(
            back_kernel,
            out_shape=tuple(jax.ShapeDtypeStruct(flat, F32) for _ in range(3))
            + tuple(jax.ShapeDtypeStruct(cube, F32) for _ in range(4)),
            in_specs=[vmem] * 5,
            out_specs=(hbm,) * 7,
            scratch_shapes=[spare, spare, spare, spare, dma((3,)), dma((4, 4))],
            compiler_params=pltpu.CompilerParams(vmem_limit_bytes=40 * 2 ** 20),
        )(*inner)
        return tuple(jnp.swapaxes(x, -1, -2) for x in outs)

    spec_3d = P(None, 'row', 'col')
    spec_2d = P('row', 'col')
    return jax.shard_map(ocean_step, mesh=mesh, in_specs=(spec_3d,) * 4 + (spec_2d,) * 5, out_specs=(spec_2d,) * 3 + (spec_3d,) * 4, check_vma=False)
```

```python
import functools
import itertools

import jax
import jax.numpy as jnp
import numpy as np
from jax import lax
from jax.experimental import pallas as pl
from jax.experimental.pallas import tpu as pltpu
from jax.sharding import PartitionSpec as P

LEVELS = 62
NI = 64
NJ = 128
HALO = 32
SUBCYCLES = 30
ADV_COURANT = 0.25
WAVE_COURANT = 0.5
VISC_NUM = 4.0
DIFF_NUM = 1.0
ALPHA_T = 0.3
BETA_S = 0.6

F32 = jnp.float32
MESH = pl.DeviceIdType.MESH
VMEM = pltpu.VMEM
OFF = 8
IPAD = NI + 16
IEXT = NI + 2 * HALO
JEXT = NJ + 2 * HALO
EAST, WEST = slice(NI - 1, NI), slice(0, 1)
OWN = slice(OFF, OFF + NI)
WEST_HALO, EAST_HALO = slice(OFF - 1, OFF), slice(OFF + NI, OFF + NI + 1)
BEFORE, AFTER = slice(0, OFF), slice(OFF + NI, IPAD)
CORE = slice(HALO, HALO + NI)
LOW, HIGH = slice(0, HALO), slice(HALO + NI, IEXT)
FAR_EAST, FAR_WEST = slice(NI - HALO, NI), slice(0, HALO)


def solve_constants(diff):
    ratio, inner, last = [], [], []
    c_prev = 0.0
    for k in range(LEVELS):
        lower = diff if k > 0 else 0.0
        pivot = 1.0 + diff + lower - lower * c_prev
        inner.append(1.0 / pivot)
        last.append(1.0 / (1.0 + lower - lower * c_prev))
        c_prev = diff / pivot
        ratio.append(c_prev)
    return ratio, inner, last


RATIO_V, INNER_V, LAST_V = solve_constants(VISC_NUM)
RATIO_D, INNER_D, LAST_D = solve_constants(DIFF_NUM)


def sm_weights():
    s = np.arange(1, SUBCYCLES + 1, dtype=np.float64) / (SUBCYCLES + 1)
    raw = s ** 2 * (1.0 - s ** 4)
    return raw / np.sum(raw)


WEIGHTS = sm_weights()
TAIL_WEIGHTS = np.cumsum(WEIGHTS[::-1])[::-1]
MEAN_STEP = float(np.sum(WEIGHTS * np.arange(1, SUBCYCLES + 1)))
MESSAGES = 38
LAG = 7
CHUNK = 24


def rot(x, shift):
    shift = shift % x.shape[-1]
    return pltpu.roll(x, shift, 1) if shift else x


def back(x):
    return rot(x, 1)


def ahead(x):
    return rot(x, -1)


def keep(mask, x):
    return jnp.where(mask, x, 0.0)


def pos(x):
    return jnp.maximum(x, 0.0)


def neg(x):
    return jnp.minimum(x, 0.0)


def per_level(x, count):
    return x / jnp.maximum(count, 1.0)


ETA, TU, TV, DEP, KMT = range(5)
U, V, T, S, MEAN, PRES, T_FLUX, S_FLUX = range(8)
UV, TS = range(2)


def exchange_kernel(
    col_count, row_count,
    u_hbm, v_hbm, t_hbm, s_hbm, eta_hbm, tu_hbm, tv_hbm, dep_hbm, kmt_hbm,
    du_o, dv_o, dt_o, ds_o, flat_o,
    u3, v3, t3, s3, p3, un3, us3, vn3, vs3, tn3, sn3, st2, near_w, near_e, kmt_i, ext2, pk2n, pk2s, hs2, hn2,
    pack, mn, ms, in_s, in_n, rr,
    ff, extf, pkfn, pkfs, hsf, hnf,
    kmu, kmw, kmv, hu2, hv2, smr,
    b_e0, b_e1, b_d, b_p, b_wu, b_ww, b_wv, b_u, b_v, b_pu, b_pv, b_s, b_g,
    ld3, ld2, snd, rcv,
):
    c = lax.axis_index("col")
    r = lax.axis_index("row")
    has_n = r < row_count - 1
    has_s = r > 0
    label = itertools.count()
    east = lax.rem(c + 1, col_count)
    west = lax.rem(c + col_count - 1, col_count)
    up, down = r + 1, r - 1

    barrier = pltpu.get_barrier_semaphore()

    def greet(cc, row):
        pl.semaphore_signal(barrier, inc=1, device_id=(cc, row), device_id_type=MESH)

    greet(east, r)
    greet(west, r)

    @pl.when(has_n)
    def _():
        for cc in (west, c, east):
            greet(cc, up)

    @pl.when(has_s)
    def _():
        for cc in (west, c, east):
            greet(cc, down)

    loads2 = []
    for f, src in enumerate((eta_hbm, tu_hbm, tv_hbm, dep_hbm)):
        loads2.append(pltpu.make_async_copy(src, st2.at[f, :NI, :], ld2.at[f]))
    loads2.append(pltpu.make_async_copy(kmt_hbm, kmt_i, ld2.at[KMT]))
    loads3 = []
    for f, (src, dst) in enumerate(((t_hbm, t3), (s_hbm, s3), (u_hbm, u3), (v_hbm, v3))):
        loads3.append(pltpu.make_async_copy(src, dst.at[:, OWN, :], ld3.at[f]))
    for cp in loads2 + loads3[:2]:
        cp.start()

    def remote(src, dst, cc, row):
        n = next(label)
        return pltpu.make_async_remote_copy(
            src_ref=src, dst_ref=dst, send_sem=snd.at[n], recv_sem=rcv.at[n],
            device_id=(cc, row), device_id_type=MESH)

    def each(go_ew, ew, cond_n, go_n, no, cond_s, so):
        for cp in ew:
            go_ew(cp)
        if no:
            @pl.when(cond_n)
            def _():
                for cp in no:
                    go_n(cp)
        if so:
            @pl.when(cond_s)
            def _():
                for cp in so:
                    go_n(cp)

    def start(ew=(), no=(), so=()):
        go = lambda cp: cp.start()
        each(go, ew, has_n, go, no, has_s, so)

    def recv(ew=(), no=(), so=()):
        go = lambda cp: cp.wait_recv()
        each(go, ew, has_s, go, no, has_n, so)

    def sent(ew=(), no=(), so=()):
        go = lambda cp: cp.wait_send()
        each(go, ew, has_n, go, no, has_s, so)

    g1 = []
    for src, dst in ((u_hbm, u3), (v_hbm, v3), (t_hbm, t3), (s_hbm, s3)):
        g1.append(remote(src.at[:, EAST, :], dst.at[:, WEST_HALO, :], east, r))
        g1.append(remote(src.at[:, WEST, :], dst.at[:, EAST_HALO, :], west, r))

    def near_ns(pn, ps, hs, hn):
        if hs.shape[0] > NI:
            hs, hn = hs.at[CORE, :], hn.at[CORE, :]
        return [remote(pn, hs, c, up)], [remote(ps, hn, c, down)]

    def corners(pn, ps, hs, hn):
        no = [
            remote(pn.at[FAR_EAST, :], hs.at[LOW, :], east, up),
            remote(pn.at[FAR_WEST, :], hs.at[HIGH, :], west, up),
        ]
        so = [
            remote(ps.at[FAR_EAST, :], hn.at[LOW, :], east, down),
            remote(ps.at[FAR_WEST, :], hn.at[HIGH, :], west, down),
        ]
        return no, so

    def side_ew(own, ext):
        return [
            remote(own.at[:, FAR_EAST, :], ext.at[:, LOW, :], east, r),
            remote(own.at[:, FAR_WEST, :], ext.at[:, HIGH, :], west, r),
        ]

    lane64 = lax.broadcasted_iota(jnp.int32, (NI, NJ), 1)
    group64 = lane64 // HALO

    def pack_flat(fields, src, pn, ps):
        top = jnp.zeros((NI, NJ), F32)
        bot = jnp.zeros((NI, NJ), F32)
        for q, f in enumerate(fields):
            x = src[f, :NI, :]
            top = jnp.where(group64 == q, rot(x, HALO * q + HALO), top)
            bot = jnp.where(group64 == q, rot(x, HALO * q), bot)
        pn[...] = top
        ps[...] = bot

    for cp in loads2:
        cp.wait()
    for cp in loads3[2:]:
        cp.start()
    st2[KMT, :NI, :] = kmt_i[...].astype(F32)
    for f in (DEP, KMT):
        st2[f, NI:, :] = jnp.zeros((OFF, NJ), F32)
    near2 = pk2n.at[1], pk2s.at[1], hs2.at[1], hn2.at[1]
    far2 = pk2n.at[0], pk2s.at[0], hs2.at[0], hn2.at[0]
    pack_flat((DEP, KMT), st2, *near2[:2])
    pack_flat((ETA, TU, TV), st2, *far2[:2])
    for f in range(5):
        ext2[f, CORE, :] = st2[f, :NI, :]

    lane8 = lax.broadcasted_iota(jnp.int32, (8, NJ), 1)
    first8 = lane8 == 0
    last8 = lane8 == NJ - 1
    slot64 = lane64 >> 1
    even64 = (lane64 & 1) == 0

    def rows(ib, off=0):
        return pl.ds(pl.multiple_of(ib * 8, 8) + off, 8)

    def pack_edges(f, ref):
        acc = jnp.zeros((NI, NJ), F32)
        for k in range(LEVELS):
            acc = jnp.where(slot64 == k, rot(ref[k, OWN, :], 2 * k + 1), acc)
        pack[f] = acc

    def pack_pair(a):
        x, y = pack[2 * a], pack[2 * a + 1]
        mn[a] = jnp.where(even64, y, back(x))
        ms[a] = jnp.where(even64, ahead(x), y)

    loads3[0].wait()
    pack_edges(T, t3)

    pl.semaphore_wait(barrier, 2 + 3 * has_n.astype(jnp.int32) + 3 * has_s.astype(jnp.int32))
    g0 = [
        remote(st2.at[DEP:KMT + 1, EAST, :], near_w.at[:, WEST, :], east, r),
        remote(st2.at[DEP:KMT + 1, WEST, :], near_e.at[:, WEST, :], west, r),
    ]
    g2b_n, g2b_s = near_ns(*near2)
    start(g0 + g1, g2b_n, g2b_s)

    loads3[1].wait()
    pack_edges(S, s3)
    pack_pair(TS)
    g3n, g3s = near_ns(mn.at[TS], ms.at[TS], in_s.at[TS, OWN, :], in_n.at[TS, OWN, :])
    start((), g3n, g3s)
    loads3[2].wait()
    pack_edges(U, u3)
    loads3[3].wait()
    pack_edges(V, v3)
    pack_pair(UV)
    g5n, g5s = near_ns(mn.at[UV], ms.at[UV], in_s.at[UV, OWN, :], in_n.at[UV, OWN, :])
    g7n = [remote(mn.at[UV, :OFF, :], in_s.at[UV, AFTER, :], west, up)]
    g7s = [remote(ms.at[UV, NI - OFF:NI, :], in_n.at[UV, BEFORE, :], east, down)]
    start((), g5n + g7n, g5s + g7s)
    g2 = side_ew(st2, ext2)
    g2a_n, g2a_s = near_ns(*far2)
    gc_n, gc_s = corners(*near2)
    gd_n, gd_s = corners(*far2)
    start(g2, g2a_n + gc_n + gd_n, g2a_s + gc_s + gd_s)

    def local_body(ib, carry):
        mid, at = rows(ib, OFF), rows(ib)
        km = st2[KMT, at, :]
        thick = per_level(st2[DEP, at, :], km)
        total = jnp.zeros((8, NJ), F32)
        for k in range(LEVELS):
            u, v = u3[k, mid, :], v3[k, mid, :]
            un3[k, mid, :] = ahead(u)
            us3[k, at, :] = back(u)
            vn3[k, at, :] = ahead(v)
            vs3[k, mid, :] = back(v)
            dens = keep(km > k, BETA_S * s3[k, mid, :] - ALPHA_T * t3[k, mid, :])
            total = total + dens
            p3[k, mid, :] = (total - 0.5 * dens) * thick
        return carry
    blocks = NI // 8
    lax.fori_loop(0, blocks, local_body, 0)

    recv((), g2b_n, g2b_s)
    has_nf = keep(has_n, 1.0).astype(F32)
    has_sf = keep(has_s, 1.0).astype(F32)
    big_n = jnp.full((NI, 1), has_nf) > 0.5
    big_s = jnp.full((NI, 1), has_sf) > 0.5
    kmt = st2[KMT, :NI, :]
    depth = st2[DEP, :NI, :]
    dep_n = keep(big_n, hn2[1, CORE, 0:1])
    kmt_n = keep(big_n, hn2[1, CORE, HALO:HALO + 1])
    kmt_s = keep(big_s, hs2[1, CORE, 2 * HALO - 1:2 * HALO])
    last64 = lane64 == NJ - 1
    kmt_north = jnp.where(last64, kmt_n, ahead(kmt))
    dep_north = jnp.where(last64, dep_n, ahead(depth))
    kmv_v = jnp.minimum(kmt, kmt_north)
    kmv[...] = kmv_v
    hv2[...] = keep(kmv_v > 0, 0.5 * (depth + dep_north))

    def u_faces():
        kmu_v = jnp.minimum(st2[KMT, :NI, :], st2[KMT, 1:NI + 1, :])
        kmu[...] = kmu_v
        hu2[...] = keep(kmu_v > 0, 0.5 * (st2[DEP, :NI, :] + st2[DEP, 1:NI + 1, :]))

    u_faces()

    def unpack_pair(a, where):
        north = keep(has_nf > 0.5, in_n[a, where, :])
        south = keep(has_sf > 0.5, in_s[a, where, :])
        even = (lax.broadcasted_iota(jnp.int32, north.shape, 1) & 1) == 0
        rr[2 * a, where, :] = jnp.where(even, north, south)
        rr[2 * a + 1, where, :] = jnp.where(even, ahead(north), back(south))

    def mean_rows():
        mean_n = rr[U, OWN, :] + rr[U, OFF - 1:OFF + NI - 1, :]
        mean_s = rr[V, OWN, :] + rr[V, OFF + 1:OFF + NI + 1, :]
        rr[MEAN, OWN, :] = jnp.where(even64, mean_n, mean_s)

    recv((), g3n, g3s)
    unpack_pair(TS, OWN)
    rt, rs = rr[T, OWN, :], rr[S, OWN, :]
    dens = keep((kmt_n > slot64.astype(F32)) & even64, BETA_S * rs - ALPHA_T * rt)
    above = lax.broadcasted_iota(jnp.int32, (NJ, NJ), 0) <= lax.broadcasted_iota(jnp.int32, (NJ, NJ), 1)
    total = jnp.dot(dens, above.astype(F32), precision=lax.Precision.HIGHEST, preferred_element_type=F32)
    rr[PRES, OWN, :] = (total - 0.5 * dens) * per_level(dep_n, kmt_n)
    recv((), g5n, g5s)
    rr[U, BEFORE, :] = jnp.zeros((OFF, NJ), F32)
    rr[V, AFTER, :] = jnp.zeros((OFF, NJ), F32)
    unpack_pair(UV, OWN)
    mean_rows()
    rv = rr[V, OWN, :]
    face_s = jnp.minimum(kmt_s, kmt[:, 0:1]) > slot64.astype(F32)
    vs_pos = keep(face_s, pos(rv))
    vs_neg = keep(face_s, neg(rv))
    rr[T_FLUX, OWN, :] = jnp.where(even64, rt, vs_pos * rt + vs_neg * pack[T])
    rr[S_FLUX, OWN, :] = jnp.where(even64, rs, vs_pos * rs + vs_neg * pack[S])

    def momentum_body(ib):
        at, mid, below, above = rows(ib), rows(ib, OFF), rows(ib, OFF - 1), rows(ib, OFF + 1)
        km_u = kmu[at, :]
        km_v = kmv[at, :]
        qu, qv, qm, qp = (rr[f, mid, :] for f in (U, V, MEAN, PRES))
        zero = jnp.zeros((8, NJ), F32)
        du, dv, st_u, st_v, sr_u, sr_v = (zero,) * 6
        for k in range(LEVELS):
            sh = NJ - 1 - 2 * k
            hu, hv, hm, hp = rot(qu, sh), rot(qv, sh), rot(qm, sh), rot(qp, sh)
            u = u3[k, mid, :]
            ue = u3[k, above, :]
            uw = u3[k, below, :]
            v = v3[k, mid, :]
            ve = v3[k, above, :]
            vw = v3[k, below, :]
            p = p3[k, mid, :]
            pe = p3[k, above, :]
            un_k, vs_k = un3[k, mid, :], vs3[k, mid, :]
            un = jnp.where(last8, hu, un_k)
            us = jnp.where(first8, hu, us3[k, at, :])
            vn = jnp.where(last8, hv, vn3[k, at, :])
            vs = jnp.where(first8, hv, vs_k)
            vm4 = (v + ve) + jnp.where(first8, hm, vs_k + vs3[k, above, :])
            um4 = (u + uw) + jnp.where(last8, hm, un_k + un3[k, below, :])
            pn = jnp.where(last8, hp, ahead(p))
            tn3[k, at, :] = ahead(t3[k, mid, :])
            sn3[k, at, :] = ahead(s3[k, mid, :])
            tu = (p - pe) - 0.5 * (u * (ue - uw)) - 0.125 * (vm4 * (un - us))
            tv = (p - pn) - 0.125 * (um4 * (ve - vw)) - 0.5 * (v * (vn - vs))
            wu = km_u > k
            wv = km_v > k
            tu = keep(wu, tu)
            tv = keep(wv, tv)
            ru_k = keep(wu, u) + ADV_COURANT * tu
            rv_k = keep(wv, v) + ADV_COURANT * tv
            st_u = st_u + tu
            st_v = st_v + tv
            sr_u = sr_u + ru_k
            sr_v = sr_v + rv_k
            fu = jnp.where(km_u > k + 1, INNER_V[k], keep(wu, LAST_V[k]))
            fv = jnp.where(km_v > k + 1, INNER_V[k], keep(wv, LAST_V[k]))
            if k > 0:
                ru_k = ru_k + VISC_NUM * du
                rv_k = rv_k + VISC_NUM * dv
            du = ru_k * fu
            dv = rv_k * fv
            du_o[k, at, :] = du
            dv_o[k, at, :] = dv
        inv_u = per_level(1.0, km_u)
        inv_v = per_level(1.0, km_v)
        ff[0, at, :] = hu2[at, :] * inv_u * st_u
        ff[1, at, :] = hv2[at, :] * inv_v * st_v
        smr[0, at, :] = inv_u * sr_u
        smr[1, at, :] = inv_v * sr_v

    def beside():
        recv(g0 + g1, g7n, g7s)
        for n, f in enumerate((DEP, KMT)):
            st2[f, NI:NI + 1, :] = near_e[n, WEST, :]
        u_faces()
        kmt = st2[KMT, :NI, :]
        first_col = lax.broadcasted_iota(jnp.int32, (NI, NJ), 0) == 0
        kmw[...] = jnp.minimum(kmt, jnp.where(first_col, near_w[1, WEST, :], pltpu.roll(kmt, 1, 0)))
        unpack_pair(UV, BEFORE)
        unpack_pair(UV, AFTER)
        mean_rows()
        km_e = near_e[1, WEST, :]
        thick_e = per_level(near_e[0, WEST, :], km_e)
        tot_e = jnp.zeros((1, NJ), F32)
        for k in range(LEVELS):
            un3[k, WEST_HALO, :] = ahead(u3[k, WEST_HALO, :])
            vs3[k, EAST_HALO, :] = back(v3[k, EAST_HALO, :])
            dens_e = keep(km_e > k, BETA_S * s3[k, EAST_HALO, :] - ALPHA_T * t3[k, EAST_HALO, :])
            tot_e = tot_e + dens_e
            p3[k, EAST_HALO, :] = (tot_e - 0.5 * dens_e) * thick_e

    def loop_body(n, carry):
        pl.when(n == blocks - 2)(beside)
        momentum_body(lax.rem(n + 1, blocks))
        return carry
    lax.fori_loop(0, blocks, loop_body, 0)

    force = pkfn.at[0], pkfs.at[0], hsf.at[0], hnf.at[0]
    pack_flat((0, 1), ff, *force[:2])
    g4 = side_ew(ff, extf)
    g4_n, g4_s = near_ns(*force)
    g6_n, g6_s = corners(*force)
    start(g4, g6_n + g4_n, g6_s + g4_s)
    for f in range(2):
        extf[f, CORE, :] = ff[f]

    def tracer_body(ib, carry):
        at, mid, below, above = rows(ib), rows(ib, OFF), rows(ib, OFF - 1), rows(ib, OFF + 1)
        km_u = kmu[at, :]
        km_w = kmw[at, :]
        km_v = kmv[at, :]
        km = st2[KMT, at, :]
        fields = ((t3, tn3, rr[T_FLUX, mid, :], dt_o), (s3, sn3, rr[S_FLUX, mid, :], ds_o))
        prev = [None, None]
        turned, flux = {}, {}
        for step in range(LEVELS + 2 * LAG):
            k = step
            if k < LEVELS:
                sh = NJ - 1 - 2 * k
                turned[k] = [(rot(q, sh), rot(q, sh - 1)) for _, _, q, _ in fields]
            k = step - LAG
            if 0 <= k < LEVELS:
                v = keep(km_v > k, v3[k, mid, :])
                v_pos, v_neg = pos(v), neg(v)
                flux[k] = []
                for (ref, next_ref, _, _), (north, south) in zip(fields, turned.pop(k)):
                    xn = jnp.where(last8, north, next_ref[k, at, :])
                    fn = v_pos * ref[k, mid, :] + v_neg * xn
                    flux[k].append((fn, back(jnp.where(last8, south, fn))))
            k = step - 2 * LAG
            if k >= 0:
                u = keep(km_u > k, u3[k, mid, :])
                w = keep(km_w > k, u3[k, below, :])
                u_pos, u_neg = pos(u), neg(u)
                w_pos, w_neg = pos(w), neg(w)
                fac = jnp.where(km > k + 1, INNER_D[k], keep(km > k, LAST_D[k]))
                for n, ((ref, _, _, out), (fn, fs)) in enumerate(zip(fields, flux.pop(k))):
                    x = ref[k, mid, :]
                    fe = u_pos * x + u_neg * ref[k, above, :]
                    fw = w_pos * ref[k, below, :] + w_neg * x
                    rhs = x - ADV_COURANT * ((fe - fw) + (fn - fs))
                    if k > 0:
                        rhs = rhs + DIFF_NUM * prev[n]
                    prev[n] = rhs * fac
                    out[k, at, :] = prev[n]
        return carry
    lax.fori_loop(0, blocks, tracer_body, 0)

    recv(g2, g2a_n + gc_n + gd_n, g2a_s + gc_s + gd_s)
    low_ok = jnp.full((HALO, IEXT), has_sf) > 0.5
    high_ok = jnp.full((HALO, IEXT), has_nf) > 0.5

    def window(ext, hs, hn, q):
        low = keep(low_ok, hs[HALO * q:HALO * (q + 1)])
        high = keep(high_ok, hn[HALO * q:HALO * (q + 1)])
        return jnp.concatenate([low, ext.T, high], axis=0)

    hs_t = [hs2[a].T for a in range(2)]
    hn_t = [hn2[a].T for a in range(2)]
    win = pl.ds(8, JEXT)
    north_of = pl.ds(9, JEXT)
    south_of = pl.ds(7, JEXT)
    zpad = jnp.zeros((8, IEXT), F32)
    for ref in (b_e0, b_e1, b_wv, b_v, b_pv, b_s, b_g):
        ref[0:8, :] = zpad
        ref[8 + JEXT:16 + JEXT, :] = zpad
    b_s[win, :] = window(ext2[KMT], hs_t[1], hn_t[1], 1)
    b_g[win, :] = window(ext2[DEP], hs_t[1], hn_t[1], 0)
    km_w = b_s[win, :]
    dp_w = b_g[win, :]
    wet_u = jnp.minimum(km_w, ahead(km_w)) > 0
    wet_v = jnp.minimum(km_w, b_s[north_of, :]) > 0
    wu = keep(wet_u, (0.25 * WAVE_COURANT) * (dp_w + ahead(dp_w)))
    wv = keep(wet_v, (0.25 * WAVE_COURANT) * (dp_w + b_g[north_of, :]))
    b_wu[...] = wu
    b_ww[...] = back(wu)
    b_wv[win, :] = wv
    b_e0[win, :] = keep(km_w > 0, window(ext2[ETA], hs_t[0], hn_t[0], ETA))
    u0 = keep(wet_u, window(ext2[TU], hs_t[0], hn_t[0], TU))
    v0 = keep(wet_v, window(ext2[TV], hs_t[0], hn_t[0], TV))
    b_u[...] = u0
    b_v[win, :] = v0
    b_d[...] = -WAVE_COURANT * ((u0 - back(u0)) + (v0 - b_v[south_of, :]))

    recv(g4, g4_n + g6_n, g4_s + g6_s)
    hsf_t = hsf[0].T
    hnf_t = hnf[0].T
    push = ADV_COURANT / SUBCYCLES
    pu = keep(wet_u, push * window(extf[0], hsf_t, hnf_t, 0))
    pv = keep(wet_v, push * window(extf[1], hsf_t, hnf_t, 1))
    b_pu[...] = pu
    b_pv[win, :] = pv
    b_p[...] = -WAVE_COURANT * ((pu - back(pu)) + (pv - b_pv[south_of, :]))

    eta_bufs = (b_e0, b_e1)
    turned = {}
    for n in range(1, SUBCYCLES + 1):
        old, new = eta_bufs[(n - 1) % 2], eta_bufs[n % 2]
        fresh = {}
        for ch in range(JEXT // CHUNK):
            lo = CHUNK * ch
            if lo + CHUNK - 1 < HALO - (SUBCYCLES - n) or lo > HALO + NJ + (SUBCYCLES - n):
                continue
            here = pl.ds(lo, CHUNK)
            mid = pl.ds(8 + lo, CHUNK)
            e = old[mid, :]
            d = b_d[here, :]
            if n > 1:
                ee, ew = turned[ch]
                gain = b_wu[here, :] * (ee - e) - b_ww[here, :] * (e - ew)
                gain = gain + b_wv[mid, :] * (old[pl.ds(9 + lo, CHUNK), :] - e)
                gain = gain - b_wv[pl.ds(7 + lo, CHUNK), :] * (e - old[pl.ds(7 + lo, CHUNK), :])
                d = d + (gain + b_p[here, :])
                b_d[here, :] = d
            e = e + d
            new[mid, :] = e
            if n < SUBCYCLES:
                fresh[ch] = (ahead(e), back(e))
            if lo + CHUNK > HALO and lo <= HALO + NJ:
                tail = float(TAIL_WEIGHTS[n - 1])
                if n == 1:
                    b_s[mid, :] = e
                    b_g[mid, :] = tail * e
                else:
                    b_s[mid, :] = b_s[mid, :] + e
                    b_g[mid, :] = b_g[mid, :] + tail * e
        turned = fresh

    mid = pl.ds(8 + HALO, NJ)
    above = pl.ds(9 + HALO, NJ)
    core = pl.ds(HALO, NJ)
    last = eta_bufs[SUBCYCLES % 2]
    flat_o[0] = last[mid, :].T[CORE]
    wu = b_wu[core, :] * 2.0
    wv = b_wv[mid, :] * 2.0
    pu, pv, u0, v0 = b_pu[core, :], b_pv[mid, :], b_u[core, :], b_v[mid, :]
    s, g = b_s[mid, :], b_g[mid, :]
    flat_o[1] = (u0 + SUBCYCLES * pu - wu * (ahead(s) - s)).T[CORE]
    flat_o[2] = (v0 + SUBCYCLES * pv - wv * (b_s[above, :] - s)).T[CORE]
    mean_u = u0 + MEAN_STEP * pu - wu * (ahead(g) - g)
    mean_v = v0 + MEAN_STEP * pv - wv * (b_g[above, :] - g)
    for f, (mean, depth_ref, km_ref) in enumerate(((mean_u, hu2, kmu), (mean_v, hv2, kmv))):
        d = depth_ref[...]
        flat_o[3 + f] = mean.T[CORE] / jnp.where(d > 0, d, 1.0) - smr[f]
        flat_o[5 + f] = km_ref[...]

    sent(g0 + g1, g2b_n, g2b_s)
    sent(g2, g3n + g5n + g7n, g3s + g5s + g7s)
    sent((), g2a_n + gc_n + gd_n, g2a_s + gc_s + gd_s)
    sent(g4, g4_n + g6_n, g4_s + g6_s)


CHUNKS = ((46, 62), (30, 46), (14, 30), (0, 14))


def back_kernel(du, dv, dt, ds, flat, eta_h, tu_h, tv_h, u_h, v_h, t_h, s_h, xu, xv, xt, xs, sem2, sem3):
    copies = [pltpu.make_async_copy(flat.at[f], out, sem2.at[f]) for f, out in enumerate((eta_h, tu_h, tv_h))]
    for cp in copies:
        cp.start()
    for n, (lo, hi) in enumerate(CHUNKS):
        def body(ib, carry):
            rows = pl.ds(pl.multiple_of(ib * 8, 8), 8)
            cu, cv, ku, kv = (flat[f, rows, :] for f in (3, 4, 5, 6))
            if hi == LEVELS:
                x = [jnp.zeros((8, NJ), F32) for _ in range(4)]
            else:
                x = [ref[rows, :] for ref in (carry_refs)]
            for k in range(hi - 1, lo - 1, -1):
                x[0] = du[k, rows, :] + RATIO_V[k] * x[0]
                x[1] = dv[k, rows, :] + RATIO_V[k] * x[1]
                x[2] = dt[k, rows, :] + RATIO_D[k] * x[2]
                x[3] = ds[k, rows, :] + RATIO_D[k] * x[3]
                xu[k, rows, :] = jnp.where(ku > k, x[0] + cu, 0.0)
                xv[k, rows, :] = jnp.where(kv > k, x[1] + cv, 0.0)
                xt[k, rows, :] = x[2]
                xs[k, rows, :] = x[3]
            for ref, val in zip(carry_refs, x):
                ref[rows, :] = val
            return carry
        carry_refs = (xu.at[LEVELS], xv.at[LEVELS], xt.at[LEVELS], xs.at[LEVELS])
        lax.fori_loop(0, NI // 8, body, 0)
        for f, (src, out) in enumerate(((xu, u_h), (xv, v_h), (xt, t_h), (xs, s_h))):
            cp = pltpu.make_async_copy(src.at[lo:hi], out.at[lo:hi], sem3.at[n, f])
            cp.start()
            copies.append(cp)
    for cp in copies:
        cp.wait()


def solution(mesh):
    col_count = mesh.shape['col']
    row_count = mesh.shape['row']

    def ocean_step(*args):
        flipped = [jnp.swapaxes(x, -1, -2) for x in args]
        cube = (LEVELS, NI, NJ)
        flat = (NI, NJ)
        dma = pltpu.SemaphoreType.DMA
        hbm = pl.BlockSpec(memory_space=pltpu.HBM)
        vmem = pl.BlockSpec(memory_space=VMEM)
        padded = VMEM((LEVELS, IPAD, NJ), F32)
        pair = VMEM((2,) + flat, F32)
        block = VMEM(cube, F32)
        near = VMEM((2, OFF, NJ), F32)
        wide = VMEM((JEXT + 16, IEXT), F32)
        plain = VMEM((JEXT, IEXT), F32)
        inner = pl.pallas_call(
            functools.partial(exchange_kernel, col_count, row_count),
            out_shape=tuple(VMEM(cube, F32) for _ in range(4)) + (VMEM((7,) + flat, F32),),
            in_specs=[hbm] * 9,
            out_specs=(vmem,) * 5,
            scratch_shapes=[
                padded, padded, padded, padded, padded, padded, block, block, padded, block, block,
                VMEM((5, NI + OFF, NJ), F32), near, near, VMEM(flat, jnp.int32), VMEM((5, IEXT, NJ), F32),
                pair, pair, VMEM((2, IEXT, NJ), F32), VMEM((2, IEXT, NJ), F32),
                VMEM((4,) + flat, F32), pair, pair,
                VMEM((2, IPAD, NJ), F32), VMEM((2, IPAD, NJ), F32), VMEM((8, IPAD, NJ), F32),
                pair, VMEM((2, IEXT, NJ), F32),
                VMEM((1,) + flat, F32), VMEM((1,) + flat, F32),
                VMEM((1, IEXT, NJ), F32), VMEM((1, IEXT, NJ), F32),
                VMEM(flat, F32), VMEM(flat, F32), VMEM(flat, F32),
                VMEM(flat, F32), VMEM(flat, F32), pair,
                wide, wide, plain, plain, plain, plain, wide, plain, wide, plain, wide, wide, wide,
                dma((4,)), dma((5,)), dma((MESSAGES,)), dma((MESSAGES,)),
            ],
            compiler_params=pltpu.CompilerParams(
                collective_id=0, has_side_effects=True, vmem_limit_bytes=54 * 2 ** 20),
        )(*flipped)
        spare = VMEM((LEVELS + 1,) + flat, F32)
        outs = pl.pallas_call(
            back_kernel,
            out_shape=tuple(jax.ShapeDtypeStruct(flat, F32) for _ in range(3))
            + tuple(jax.ShapeDtypeStruct(cube, F32) for _ in range(4)),
            in_specs=[vmem] * 5,
            out_specs=(hbm,) * 7,
            scratch_shapes=[spare, spare, spare, spare, dma((3,)), dma((4, 4))],
            compiler_params=pltpu.CompilerParams(vmem_limit_bytes=40 * 2 ** 20),
        )(*inner)
        return tuple(jnp.swapaxes(x, -1, -2) for x in outs)

    spec_3d = P(None, 'row', 'col')
    spec_2d = P('row', 'col')
    return jax.shard_map(ocean_step, mesh=mesh, in_specs=(spec_3d,) * 4 + (spec_2d,) * 5, out_specs=(spec_2d,) * 3 + (spec_3d,) * 4, check_vma=False)
```

```python
import functools
import itertools

import jax
import jax.numpy as jnp
import numpy as np
from jax import lax
from jax.experimental import pallas as pl
from jax.experimental.pallas import tpu as pltpu
from jax.sharding import PartitionSpec as P

LEVELS = 62
NI = 64
NJ = 128
HALO = 32
SUBCYCLES = 30
ADV_COURANT = 0.25
WAVE_COURANT = 0.5
VISC_NUM = 4.0
DIFF_NUM = 1.0
ALPHA_T = 0.3
BETA_S = 0.6

F32 = jnp.float32
MESH = pl.DeviceIdType.MESH
VMEM = pltpu.VMEM
OFF = 8
IPAD = NI + 16
IEXT = NI + 2 * HALO
JEXT = NJ + 2 * HALO
EAST, WEST = slice(NI - 1, NI), slice(0, 1)
OWN = slice(OFF, OFF + NI)
WEST_HALO, EAST_HALO = slice(OFF - 1, OFF), slice(OFF + NI, OFF + NI + 1)
BEFORE, AFTER = slice(0, OFF), slice(OFF + NI, IPAD)
CORE = slice(HALO, HALO + NI)
LOW, HIGH = slice(0, HALO), slice(HALO + NI, IEXT)
FAR_EAST, FAR_WEST = slice(NI - HALO, NI), slice(0, HALO)


def solve_constants(diff):
    ratio, inner, last = [], [], []
    c_prev = 0.0
    for k in range(LEVELS):
        lower = diff if k > 0 else 0.0
        pivot = 1.0 + diff + lower - lower * c_prev
        inner.append(1.0 / pivot)
        last.append(1.0 / (1.0 + lower - lower * c_prev))
        c_prev = diff / pivot
        ratio.append(c_prev)
    return ratio, inner, last


RATIO_V, INNER_V, LAST_V = solve_constants(VISC_NUM)
RATIO_D, INNER_D, LAST_D = solve_constants(DIFF_NUM)


def sm_weights():
    s = np.arange(1, SUBCYCLES + 1, dtype=np.float64) / (SUBCYCLES + 1)
    raw = s ** 2 * (1.0 - s ** 4)
    return raw / np.sum(raw)


WEIGHTS = sm_weights()
TAIL_WEIGHTS = np.cumsum(WEIGHTS[::-1])[::-1]
MEAN_STEP = float(np.sum(WEIGHTS * np.arange(1, SUBCYCLES + 1)))
MESSAGES = 32
PARTS = ((0, 16), (16, 32), (32, 48), (48, LEVELS))
SPARE = 2 * LEVELS
LAG_M = 2
LAG = 7
CHUNK = 24


def rot(x, shift):
    shift = shift % x.shape[-1]
    return pltpu.roll(x, shift, 1) if shift else x


def back(x):
    return rot(x, 1)


def ahead(x):
    return rot(x, -1)


def keep(mask, x):
    return jnp.where(mask, x, 0.0)


def pos(x):
    return jnp.maximum(x, 0.0)


def neg(x):
    return jnp.minimum(x, 0.0)


def per_level(x, count):
    return x / jnp.maximum(count, 1.0)


ETA, TU, TV, WET_DEP = range(4)
DEP, KMT = range(2)
U, V, T, S, MEAN, PRES, T_FLUX, S_FLUX = range(8)
UV, TS = range(2)


def exchange_kernel(
    col_count, row_count,
    u_hbm, v_hbm, t_hbm, s_hbm, eta_hbm, tu_hbm, tv_hbm, dep_hbm, kmt_hbm,
    du_o, dv_o, dt_o, ds_o, flat_o,
    u3, v3, t3, s3, p3, un3, us3, vn3, vs3, tn3, sn3, st2, nd2, near_w, near_e, kmt_i, ext2, pk2n, pk2s, hs2, hn2,
    pack, mn, ms, in_s, in_n, rr,
    ff, extf, pkfn, pkfs, hsf, hnf,
    kmu, kmw, kmv, hu2, hv2, smr,
    b_e0, b_e1, b_d, b_p, b_wu, b_ww, b_wv, b_u, b_v, b_pu, b_pv, b_s, b_g,
    ld3, ld2, snd, rcv,
):
    c = lax.axis_index("col")
    r = lax.axis_index("row")
    has_n = r < row_count - 1
    has_s = r > 0
    label = itertools.count()
    east = lax.rem(c + 1, col_count)
    west = lax.rem(c + col_count - 1, col_count)
    up, down = r + 1, r - 1

    barrier = pltpu.get_barrier_semaphore()

    def greet(cc, row):
        pl.semaphore_signal(barrier, inc=1, device_id=(cc, row), device_id_type=MESH)

    greet(east, r)
    greet(west, r)

    @pl.when(has_n)
    def _():
        for cc in (west, c, east):
            greet(cc, up)

    @pl.when(has_s)
    def _():
        for cc in (west, c, east):
            greet(cc, down)

    loads2 = []
    for f, (src, dst) in enumerate((
            (eta_hbm, st2.at[ETA]), (tu_hbm, st2.at[TU]), (tv_hbm, st2.at[TV]),
            (dep_hbm, nd2.at[DEP, :NI, :]), (kmt_hbm, kmt_i))):
        loads2.append(pltpu.make_async_copy(src, dst, ld2.at[f]))
    loads3 = []
    for f, (src, dst) in enumerate(((t_hbm, t3), (s_hbm, s3), (u_hbm, u3), (v_hbm, v3))):
        loads3.append([
            pltpu.make_async_copy(src.at[lo:hi], dst.at[lo:hi, OWN, :], ld3.at[f, n])
            for n, (lo, hi) in enumerate(PARTS)])
    for cp in loads3[0] + loads2 + sum(loads3[1:], []):
        cp.start()

    def landed(f):
        for cp in loads3[f]:
            cp.wait()

    def remote(src, dst, cc, row):
        n = next(label)
        return pltpu.make_async_remote_copy(
            src_ref=src, dst_ref=dst, send_sem=snd.at[n], recv_sem=rcv.at[n],
            device_id=(cc, row), device_id_type=MESH)

    def each(go_ew, ew, cond_n, go_n, no, cond_s, so):
        for cp in ew:
            go_ew(cp)
        if no:
            @pl.when(cond_n)
            def _():
                for cp in no:
                    go_n(cp)
        if so:
            @pl.when(cond_s)
            def _():
                for cp in so:
                    go_n(cp)

    def start(ew=(), no=(), so=()):
        go = lambda cp: cp.start()
        each(go, ew, has_n, go, no, has_s, so)

    def recv(ew=(), no=(), so=()):
        go = lambda cp: cp.wait_recv()
        each(go, ew, has_s, go, no, has_n, so)

    def sent(ew=(), no=(), so=()):
        go = lambda cp: cp.wait_send()
        each(go, ew, has_n, go, no, has_s, so)

    g1 = []
    for src, dst in ((u_hbm, u3), (v_hbm, v3), (t_hbm, t3), (s_hbm, s3)):
        g1.append(remote(src.at[:, EAST, :], dst.at[:, WEST_HALO, :], east, r))
        g1.append(remote(src.at[:, WEST, :], dst.at[:, EAST_HALO, :], west, r))

    def near_ns(pn, ps, hs, hn):
        if hs.shape[0] > NI:
            hs, hn = hs.at[CORE, :], hn.at[CORE, :]
        return [remote(pn, hs, c, up)], [remote(ps, hn, c, down)]

    def corners(pn, ps, hs, hn):
        no = [
            remote(pn.at[FAR_EAST, :], hs.at[LOW, :], east, up),
            remote(pn.at[FAR_WEST, :], hs.at[HIGH, :], west, up),
        ]
        so = [
            remote(ps.at[FAR_EAST, :], hn.at[LOW, :], east, down),
            remote(ps.at[FAR_WEST, :], hn.at[HIGH, :], west, down),
        ]
        return no, so

    def side_ew(own, ext):
        return [
            remote(own.at[:, FAR_EAST, :], ext.at[:, LOW, :], east, r),
            remote(own.at[:, FAR_WEST, :], ext.at[:, HIGH, :], west, r),
        ]

    lane64 = lax.broadcasted_iota(jnp.int32, (NI, NJ), 1)
    group64 = lane64 // HALO

    def pack_flat(fields, src, pn, ps):
        top = jnp.zeros((NI, NJ), F32)
        bot = jnp.zeros((NI, NJ), F32)
        for q, f in enumerate(fields):
            x = src[f]
            top = jnp.where(group64 == q, rot(x, HALO * q + HALO), top)
            bot = jnp.where(group64 == q, rot(x, HALO * q), bot)
        pn[...] = top
        ps[...] = bot

    lane8 = lax.broadcasted_iota(jnp.int32, (8, NJ), 1)
    first8 = lane8 == 0
    last8 = lane8 == NJ - 1
    slot64 = lane64 >> 1
    even64 = (lane64 & 1) == 0

    def rows(ib, off=0):
        return pl.ds(pl.multiple_of(ib * 8, 8) + off, 8)

    def pack_edges(f, ref):
        acc = jnp.zeros((NI, NJ), F32)
        for k in range(LEVELS):
            acc = jnp.where(slot64 == k, rot(ref[k, OWN, :], 2 * k + 1), acc)
        pack[f] = acc

    def pack_pair(a):
        x, y = pack[2 * a], pack[2 * a + 1]
        return jnp.where(even64, y, back(x)), jnp.where(even64, ahead(x), y)

    def with_near(top, bottom):
        for f in (DEP, KMT):
            x = nd2[f, :NI, :]
            spare = lane64 == SPARE + f
            top = jnp.where(spare, rot(x, SPARE + f + 1), top)
            bottom = jnp.where(spare, rot(x, SPARE + f), bottom)
        return top, bottom

    landed(0)
    pack_edges(T, t3)
    for cp in loads2:
        cp.wait()
    kmt = kmt_i[...].astype(F32)
    nd2[KMT, :NI, :] = kmt
    nd2[:, NI:, :] = jnp.zeros((2, OFF, NJ), F32)
    st2[WET_DEP] = keep(kmt > 0, nd2[DEP, :NI, :])

    pl.semaphore_wait(barrier, 2 + 3 * has_n.astype(jnp.int32) + 3 * has_s.astype(jnp.int32))
    g0 = [
        remote(nd2.at[:, EAST, :], near_w.at[:, WEST, :], east, r),
        remote(nd2.at[:, WEST, :], near_e.at[:, WEST, :], west, r),
    ]
    start(g0 + g1)

    landed(1)
    pack_edges(S, s3)
    mn[TS], ms[TS] = with_near(*pack_pair(TS))
    g3n, g3s = near_ns(mn.at[TS], ms.at[TS], in_s.at[TS, OWN, :], in_n.at[TS, OWN, :])
    start((), g3n, g3s)
    landed(2)
    pack_edges(U, u3)
    landed(3)
    pack_edges(V, v3)
    mn[UV], ms[UV] = pack_pair(UV)
    g5n, g5s = near_ns(mn.at[UV], ms.at[UV], in_s.at[UV, OWN, :], in_n.at[UV, OWN, :])
    g7n = [remote(mn.at[UV, :OFF, :], in_s.at[UV, AFTER, :], west, up)]
    g7s = [remote(ms.at[UV, NI - OFF:NI, :], in_n.at[UV, BEFORE, :], east, down)]
    start((), g5n + g7n, g5s + g7s)
    wide2 = pk2n.at[0], pk2s.at[0], hs2.at[0], hn2.at[0]
    pack_flat(range(4), st2, *wide2[:2])
    g2 = side_ew(st2, ext2)
    g2a_n, g2a_s = near_ns(*wide2)
    gc_n, gc_s = corners(*wide2)
    start(g2, g2a_n + gc_n, g2a_s + gc_s)
    for f in range(4):
        ext2[f, CORE, :] = st2[f]

    def local_body(ib, carry):
        mid, at = rows(ib, OFF), rows(ib)
        km = nd2[KMT, at, :]
        thick = 2.0 * per_level(nd2[DEP, at, :], km)
        total = jnp.zeros((8, NJ), F32)
        for k in range(LEVELS):
            u, v = u3[k, mid, :], v3[k, mid, :]
            u = 0.25 * u
            un3[k, mid, :] = ahead(u)
            us3[k, at, :] = back(u)
            vn3[k, at, :] = ahead(v)
            vs3[k, mid, :] = back(v)
            dens = keep(km > k, BETA_S * s3[k, mid, :] - ALPHA_T * t3[k, mid, :])
            total = total + dens
            p3[k, mid, :] = (total - 0.5 * dens) * thick
        return carry
    blocks = NI // 8
    lax.fori_loop(0, blocks, local_body, 0)

    recv((), g3n, g3s)
    has_nf = keep(has_n, 1.0).astype(F32)
    has_sf = keep(has_s, 1.0).astype(F32)
    big_n = jnp.full((NI, 1), has_nf) > 0.5
    big_s = jnp.full((NI, 1), has_sf) > 0.5
    depth = nd2[DEP, :NI, :]
    dep_n = keep(big_n, in_n[TS, OWN, SPARE + DEP:SPARE + DEP + 1])
    kmt_n = keep(big_n, in_n[TS, OWN, SPARE + KMT:SPARE + KMT + 1])
    kmt_s = keep(big_s, in_s[TS, OWN, SPARE + KMT:SPARE + KMT + 1])
    last64 = lane64 == NJ - 1
    kmt_north = jnp.where(last64, kmt_n, ahead(kmt))
    dep_north = jnp.where(last64, dep_n, ahead(depth))
    kmv_v = jnp.minimum(kmt, kmt_north)
    kmv[...] = kmv_v
    hv2[...] = keep(kmv_v > 0, 0.5 * (depth + dep_north))

    def u_faces():
        kmu_v = jnp.minimum(nd2[KMT, :NI, :], nd2[KMT, 1:NI + 1, :])
        kmu[...] = kmu_v
        hu2[...] = keep(kmu_v > 0, 0.5 * (nd2[DEP, :NI, :] + nd2[DEP, 1:NI + 1, :]))

    u_faces()

    def unpack_pair(a, where):
        north = keep(has_nf > 0.5, in_n[a, where, :])
        south = keep(has_sf > 0.5, in_s[a, where, :])
        even = (lax.broadcasted_iota(jnp.int32, north.shape, 1) & 1) == 0
        first = jnp.where(even, north, south)
        rr[2 * a, where, :] = 0.25 * first if a == UV else first
        rr[2 * a + 1, where, :] = jnp.where(even, ahead(north), back(south))

    def mean_rows():
        mean_n = rr[U, OWN, :] + rr[U, OFF - 1:OFF + NI - 1, :]
        mean_s = rr[V, OWN, :] + rr[V, OFF + 1:OFF + NI + 1, :]
        rr[MEAN, OWN, :] = jnp.where(even64, mean_n, mean_s)

    unpack_pair(TS, OWN)
    rt, rs = rr[T, OWN, :], rr[S, OWN, :]
    dens = keep((kmt_n > slot64.astype(F32)) & even64, BETA_S * rs - ALPHA_T * rt)
    above = lax.broadcasted_iota(jnp.int32, (NJ, NJ), 0) <= lax.broadcasted_iota(jnp.int32, (NJ, NJ), 1)
    total = jnp.dot(dens, above.astype(F32), precision=lax.Precision.HIGHEST, preferred_element_type=F32)
    rr[PRES, OWN, :] = (total - 0.5 * dens) * (2.0 * per_level(dep_n, kmt_n))
    recv((), g5n, g5s)
    rr[U, BEFORE, :] = jnp.zeros((OFF, NJ), F32)
    rr[V, AFTER, :] = jnp.zeros((OFF, NJ), F32)
    unpack_pair(UV, OWN)
    mean_rows()
    rv = rr[V, OWN, :]
    face_s = jnp.minimum(kmt_s, kmt[:, 0:1]) > slot64.astype(F32)
    vs_pos = keep(face_s, pos(rv))
    vs_neg = keep(face_s, neg(rv))
    rr[T_FLUX, OWN, :] = jnp.where(even64, rt, vs_pos * rt + vs_neg * pack[T])
    rr[S_FLUX, OWN, :] = jnp.where(even64, rs, vs_pos * rs + vs_neg * pack[S])

    def momentum_body(ib):
        at, mid, below, above = rows(ib), rows(ib, OFF), rows(ib, OFF - 1), rows(ib, OFF + 1)
        km_u = kmu[at, :]
        km_v = kmv[at, :]
        qu, qv, qm, qp = (rr[f, mid, :] for f in (U, V, MEAN, PRES))
        zero = jnp.zeros((8, NJ), F32)
        du, dv, st_u, st_v, sr_u, sr_v = (zero,) * 6
        turned = {}
        for step in range(LEVELS + LAG_M):
            k = step
            if k < LEVELS:
                sh = NJ - 1 - 2 * k
                turned[k] = (
                    rot(qu, sh), rot(qv, sh), rot(qm, sh), rot(qp, sh),
                    ahead(p3[k, mid, :]), ahead(t3[k, mid, :]), ahead(s3[k, mid, :]))
            k = step - LAG_M
            if k < 0:
                continue
            hu, hv, hm, hp, p_next, t_next, s_next = turned.pop(k)
            tn3[k, at, :] = t_next
            sn3[k, at, :] = s_next
            u = u3[k, mid, :]
            ue = u3[k, above, :]
            uw = u3[k, below, :]
            v = v3[k, mid, :]
            ve = v3[k, above, :]
            vw = v3[k, below, :]
            p = p3[k, mid, :]
            pe = p3[k, above, :]
            un_k, vs_k = un3[k, mid, :], vs3[k, mid, :]
            un = jnp.where(last8, hu, un_k)
            us = jnp.where(first8, hu, us3[k, at, :])
            vn = jnp.where(last8, hv, vn3[k, at, :])
            vs = jnp.where(first8, hv, vs_k)
            vm4 = (v + ve) + jnp.where(first8, hm, vs_k + vs3[k, above, :])
            um = 0.25 * (u + uw) + jnp.where(last8, hm, un_k + un3[k, below, :])
            pn = jnp.where(last8, hp, p_next)
            tu = (p - pe) - u * (ue - uw) - vm4 * (un - us)
            tv = (p - pn) - um * (ve - vw) - v * (vn - vs)
            wu = km_u > k
            wv = km_v > k
            st_u = st_u + keep(wu, tu)
            st_v = st_v + keep(wv, tv)
            ru_k = u + (0.5 * ADV_COURANT) * tu
            rv_k = v + (0.5 * ADV_COURANT) * tv
            sr_u = sr_u + keep(wu, ru_k)
            sr_v = sr_v + keep(wv, rv_k)
            du = ru_k + RATIO_V[k - 1] * du if k else ru_k
            dv = rv_k + RATIO_V[k - 1] * dv if k else rv_k
            du_o[k, at, :] = du
            dv_o[k, at, :] = dv
        inv_u = per_level(1.0, km_u)
        inv_v = per_level(1.0, km_v)
        ff[0, at, :] = hu2[at, :] * inv_u * (0.5 * st_u)
        ff[1, at, :] = hv2[at, :] * inv_v * (0.5 * st_v)
        smr[0, at, :] = inv_u * sr_u
        smr[1, at, :] = inv_v * sr_v

    def beside():
        recv(g0 + g1, g7n, g7s)
        for f in (DEP, KMT):
            nd2[f, NI:NI + 1, :] = near_e[f, WEST, :]
        u_faces()
        kmt = nd2[KMT, :NI, :]
        first_col = lax.broadcasted_iota(jnp.int32, (NI, NJ), 0) == 0
        kmw[...] = jnp.minimum(kmt, jnp.where(first_col, near_w[KMT, WEST, :], pltpu.roll(kmt, 1, 0)))
        unpack_pair(UV, BEFORE)
        unpack_pair(UV, AFTER)
        mean_rows()
        km_e = near_e[KMT, WEST, :]
        thick_e = 2.0 * per_level(near_e[DEP, WEST, :], km_e)
        tot_e = jnp.zeros((1, NJ), F32)
        for k in range(LEVELS):
            un3[k, WEST_HALO, :] = ahead(0.25 * u3[k, WEST_HALO, :])
            vs3[k, EAST_HALO, :] = back(v3[k, EAST_HALO, :])
            dens_e = keep(km_e > k, BETA_S * s3[k, EAST_HALO, :] - ALPHA_T * t3[k, EAST_HALO, :])
            tot_e = tot_e + dens_e
            p3[k, EAST_HALO, :] = (tot_e - 0.5 * dens_e) * thick_e

    def loop_body(n, carry):
        pl.when(n == blocks - 2)(beside)
        momentum_body(lax.rem(n + 1, blocks))
        return carry
    lax.fori_loop(0, blocks, loop_body, 0)

    force = pkfn.at[0], pkfs.at[0], hsf.at[0], hnf.at[0]
    pack_flat((0, 1), ff, *force[:2])
    g4 = side_ew(ff, extf)
    g4_n, g4_s = near_ns(*force)
    g6_n, g6_s = corners(*force)
    start(g4, g6_n + g4_n, g6_s + g4_s)
    for f in range(2):
        extf[f, CORE, :] = ff[f]

    def tracer_body(ib, carry):
        at, mid, below, above = rows(ib), rows(ib, OFF), rows(ib, OFF - 1), rows(ib, OFF + 1)
        km_u = kmu[at, :]
        km_w = kmw[at, :]
        km_v = kmv[at, :]
        fields = ((t3, tn3, rr[T_FLUX, mid, :], dt_o), (s3, sn3, rr[S_FLUX, mid, :], ds_o))
        prev = [None, None]
        turned, flux = {}, {}
        for step in range(LEVELS + 2 * LAG):
            k = step
            if k < LEVELS:
                sh = NJ - 1 - 2 * k
                turned[k] = [(rot(q, sh), rot(q, sh - 1)) for _, _, q, _ in fields]
            k = step - LAG
            if 0 <= k < LEVELS:
                v = keep(km_v > k, v3[k, mid, :])
                northward = v > 0
                flux[k] = []
                for (ref, next_ref, _, _), (north, south) in zip(fields, turned.pop(k)):
                    xn = jnp.where(last8, north, next_ref[k, at, :])
                    fn = v * jnp.where(northward, ref[k, mid, :], xn)
                    flux[k].append((fn, back(jnp.where(last8, south, fn))))
            k = step - 2 * LAG
            if k >= 0:
                u = keep(km_u > k, u3[k, mid, :])
                w = keep(km_w > k, u3[k, below, :])
                eastward, from_west = u > 0, w > 0
                for n, ((ref, _, _, out), (fn, fs)) in enumerate(zip(fields, flux.pop(k))):
                    x = ref[k, mid, :]
                    fe = u * jnp.where(eastward, x, ref[k, above, :])
                    fw = w * jnp.where(from_west, ref[k, below, :], x)
                    rhs = x - ADV_COURANT * ((fe - fw) + (fn - fs))
                    prev[n] = rhs + RATIO_D[k - 1] * prev[n] if k else rhs
                    out[k, at, :] = prev[n]
        return carry
    lax.fori_loop(0, blocks, tracer_body, 0)

    recv(g2, g2a_n + gc_n, g2a_s + gc_s)
    low_ok = jnp.full((HALO, IEXT), has_sf) > 0.5
    high_ok = jnp.full((HALO, IEXT), has_nf) > 0.5

    def window(ext, hs, hn, q):
        low = keep(low_ok, hs[HALO * q:HALO * (q + 1)])
        high = keep(high_ok, hn[HALO * q:HALO * (q + 1)])
        return jnp.concatenate([low, ext.T, high], axis=0)

    hs_t, hn_t = hs2[0].T, hn2[0].T
    win = pl.ds(8, JEXT)
    north_of = pl.ds(9, JEXT)
    south_of = pl.ds(7, JEXT)
    zpad = jnp.zeros((8, IEXT), F32)
    for ref in (b_e0, b_e1, b_wv, b_v, b_pv, b_s, b_g):
        ref[0:8, :] = zpad
        ref[8 + JEXT:16 + JEXT, :] = zpad
    dp_w = window(ext2[WET_DEP], hs_t, hn_t, WET_DEP)
    b_s[win, :] = dp_w
    dp_n, dp_e = b_s[north_of, :], ahead(dp_w)
    wet_u = (dp_w > 0) & (dp_e > 0)
    wet_v = (dp_w > 0) & (dp_n > 0)
    wu = keep(wet_u, (0.25 * WAVE_COURANT) * (dp_w + dp_e))
    wv = keep(wet_v, (0.25 * WAVE_COURANT) * (dp_w + dp_n))
    b_wu[...] = wu
    b_ww[...] = back(wu)
    b_wv[win, :] = wv
    b_e0[win, :] = keep(dp_w > 0, window(ext2[ETA], hs_t, hn_t, ETA))
    u0 = keep(wet_u, window(ext2[TU], hs_t, hn_t, TU))
    v0 = keep(wet_v, window(ext2[TV], hs_t, hn_t, TV))
    b_u[...] = u0
    b_v[win, :] = v0
    b_d[...] = -WAVE_COURANT * ((u0 - back(u0)) + (v0 - b_v[south_of, :]))

    recv(g4, g4_n + g6_n, g4_s + g6_s)
    hsf_t = hsf[0].T
    hnf_t = hnf[0].T
    push = ADV_COURANT / SUBCYCLES
    pu = keep(wet_u, push * window(extf[0], hsf_t, hnf_t, 0))
    pv = keep(wet_v, push * window(extf[1], hsf_t, hnf_t, 1))
    b_pu[...] = pu
    b_pv[win, :] = pv
    b_p[...] = -WAVE_COURANT * ((pu - back(pu)) + (pv - b_pv[south_of, :]))

    eta_bufs = (b_e0, b_e1)
    turned = {}
    for n in range(1, SUBCYCLES + 1):
        old, new = eta_bufs[(n - 1) % 2], eta_bufs[n % 2]
        fresh = {}
        for ch in range(JEXT // CHUNK):
            lo = CHUNK * ch
            if lo + CHUNK - 1 < HALO - (SUBCYCLES - n) or lo > HALO + NJ + (SUBCYCLES - n):
                continue
            here = pl.ds(lo, CHUNK)
            mid = pl.ds(8 + lo, CHUNK)
            e = old[mid, :]
            d = b_d[here, :]
            if n > 1:
                ee, ew = turned[ch]
                gain = b_wu[here, :] * (ee - e) - b_ww[here, :] * (e - ew)
                gain = gain + b_wv[mid, :] * (old[pl.ds(9 + lo, CHUNK), :] - e)
                gain = gain - b_wv[pl.ds(7 + lo, CHUNK), :] * (e - old[pl.ds(7 + lo, CHUNK), :])
                d = d + (gain + b_p[here, :])
                b_d[here, :] = d
            e = e + d
            new[mid, :] = e
            if n < SUBCYCLES:
                fresh[ch] = (ahead(e), back(e))
            if lo + CHUNK > HALO and lo <= HALO + NJ:
                tail = float(TAIL_WEIGHTS[n - 1])
                if n == 1:
                    b_s[mid, :] = e
                    b_g[mid, :] = tail * e
                else:
                    b_s[mid, :] = b_s[mid, :] + e
                    b_g[mid, :] = b_g[mid, :] + tail * e
        turned = fresh

    mid = pl.ds(8 + HALO, NJ)
    above = pl.ds(9 + HALO, NJ)
    core = pl.ds(HALO, NJ)
    last = eta_bufs[SUBCYCLES % 2]
    flat_o[0] = last[mid, :].T[CORE]
    wu = b_wu[core, :] * 2.0
    wv = b_wv[mid, :] * 2.0
    pu, pv, u0, v0 = b_pu[core, :], b_pv[mid, :], b_u[core, :], b_v[mid, :]
    s, g = b_s[mid, :], b_g[mid, :]
    flat_o[1] = (u0 + SUBCYCLES * pu - wu * (ahead(s) - s)).T[CORE]
    flat_o[2] = (v0 + SUBCYCLES * pv - wv * (b_s[above, :] - s)).T[CORE]
    mean_u = u0 + MEAN_STEP * pu - wu * (ahead(g) - g)
    mean_v = v0 + MEAN_STEP * pv - wv * (b_g[above, :] - g)
    for f, (mean, depth_ref, km_ref) in enumerate(((mean_u, hu2, kmu), (mean_v, hv2, kmv))):
        d = depth_ref[...]
        flat_o[3 + f] = mean.T[CORE] / jnp.where(d > 0, d, 1.0) - smr[f]
        flat_o[5 + f] = km_ref[...]
    flat_o[7] = nd2[KMT, :NI, :]

    sent(g0 + g1)
    sent(g2, g3n + g5n + g7n, g3s + g5s + g7s)
    sent((), g2a_n + gc_n, g2a_s + gc_s)
    sent(g4, g4_n + g6_n, g4_s + g6_s)


CHUNKS = ((54, 62), (42, 54), (28, 42), (14, 28), (0, 14))


def back_kernel(du, dv, dt, ds, flat, eta_h, tu_h, tv_h, u_h, v_h, t_h, s_h, xu, xv, xt, xs, sem2, sem3):
    copies = [pltpu.make_async_copy(flat.at[f], out, sem2.at[f]) for f, out in enumerate((eta_h, tu_h, tv_h))]
    for cp in copies:
        cp.start()
    results = ((xu, u_h), (xv, v_h), (xt, t_h), (xs, s_h))
    for n, (lo, hi) in enumerate(CHUNKS):
        def body(ib, carry):
            rows = pl.ds(pl.multiple_of(ib * 8, 8), 8)
            cu, cv, ku, kv, kt = (flat[f, rows, :] for f in range(3, 8))
            x = [jnp.zeros((8, NJ), F32) if hi == LEVELS else ref[LEVELS, rows, :] for ref, _ in results]
            for k in range(hi - 1, lo - 1, -1):
                wu, wv = ku > k, kv > k
                fu = jnp.where(ku > k + 1, INNER_V[k], keep(wu, LAST_V[k]))
                fv = jnp.where(kv > k + 1, INNER_V[k], keep(wv, LAST_V[k]))
                ft = jnp.where(kt > k + 1, INNER_D[k], keep(kt > k, LAST_D[k]))
                x[0] = fu * du[k, rows, :] + RATIO_V[k] * x[0]
                x[1] = fv * dv[k, rows, :] + RATIO_V[k] * x[1]
                x[2] = ft * dt[k, rows, :] + RATIO_D[k] * x[2]
                x[3] = ft * ds[k, rows, :] + RATIO_D[k] * x[3]
                xu[k, rows, :] = keep(wu, x[0] + cu)
                xv[k, rows, :] = keep(wv, x[1] + cv)
                xt[k, rows, :] = x[2]
                xs[k, rows, :] = x[3]
            for (ref, _), val in zip(results, x):
                ref[LEVELS, rows, :] = val
            return carry
        lax.fori_loop(0, NI // 8, body, 0)
        for f, (src, out) in enumerate(results):
            cp = pltpu.make_async_copy(src.at[lo:hi], out.at[lo:hi], sem3.at[n, f])
            cp.start()
            copies.append(cp)
    for cp in copies:
        cp.wait()


def solution(mesh):
    col_count = mesh.shape['col']
    row_count = mesh.shape['row']

    def ocean_step(*args):
        flipped = [jnp.swapaxes(x, -1, -2) for x in args]
        cube = (LEVELS, NI, NJ)
        flat = (NI, NJ)
        dma = pltpu.SemaphoreType.DMA
        hbm = pl.BlockSpec(memory_space=pltpu.HBM)
        vmem = pl.BlockSpec(memory_space=VMEM)
        padded = VMEM((LEVELS, IPAD, NJ), F32)
        pair = VMEM((2,) + flat, F32)
        block = VMEM(cube, F32)
        single = VMEM((1,) + flat, F32)
        near = VMEM((2, OFF, NJ), F32)
        wide = VMEM((JEXT + 16, IEXT), F32)
        plain = VMEM((JEXT, IEXT), F32)
        inner = pl.pallas_call(
            functools.partial(exchange_kernel, col_count, row_count),
            out_shape=tuple(VMEM(cube, F32) for _ in range(4)) + (VMEM((8,) + flat, F32),),
            in_specs=[hbm] * 9,
            out_specs=(vmem,) * 5,
            scratch_shapes=[
                padded, padded, padded, padded, padded, padded, block, block, padded, block, block,
                VMEM((4,) + flat, F32), VMEM((2, NI + OFF, NJ), F32), near, near, VMEM(flat, jnp.int32),
                VMEM((4, IEXT, NJ), F32), single, single, VMEM((1, IEXT, NJ), F32), VMEM((1, IEXT, NJ), F32),
                VMEM((4,) + flat, F32), pair, pair,
                VMEM((2, IPAD, NJ), F32), VMEM((2, IPAD, NJ), F32), VMEM((8, IPAD, NJ), F32),
                pair, VMEM((2, IEXT, NJ), F32),
                single, single,
                VMEM((1, IEXT, NJ), F32), VMEM((1, IEXT, NJ), F32),
                VMEM(flat, F32), VMEM(flat, F32), VMEM(flat, F32),
                VMEM(flat, F32), VMEM(flat, F32), pair,
                wide, wide, plain, plain, plain, plain, wide, plain, wide, plain, wide, wide, wide,
                dma((4, len(PARTS))), dma((5,)), dma((MESSAGES,)), dma((MESSAGES,)),
            ],
            compiler_params=pltpu.CompilerParams(
                collective_id=0, has_side_effects=True, vmem_limit_bytes=54 * 2 ** 20),
        )(*flipped)
        spare = VMEM((LEVELS + 1,) + flat, F32)
        outs = pl.pallas_call(
            back_kernel,
            out_shape=tuple(jax.ShapeDtypeStruct(flat, F32) for _ in range(3))
            + tuple(jax.ShapeDtypeStruct(cube, F32) for _ in range(4)),
            in_specs=[vmem] * 5,
            out_specs=(hbm,) * 7,
            scratch_shapes=[spare, spare, spare, spare, dma((3,)), dma((len(CHUNKS), 4))],
            compiler_params=pltpu.CompilerParams(vmem_limit_bytes=40 * 2 ** 20),
        )(*inner)
        return tuple(jnp.swapaxes(x, -1, -2) for x in outs)

    spec_3d = P(None, 'row', 'col')
    spec_2d = P('row', 'col')
    return jax.shard_map(ocean_step, mesh=mesh, in_specs=(spec_3d,) * 4 + (spec_2d,) * 5, out_specs=(spec_2d,) * 3 + (spec_3d,) * 4, check_vma=False)
```

```python
import functools
import itertools

import jax
import jax.numpy as jnp
import numpy as np
from jax import lax
from jax.experimental import pallas as pl
from jax.experimental.pallas import tpu as pltpu
from jax.sharding import PartitionSpec as P

LEVELS = 62
NI = 64
NJ = 128
HALO = 32
SUBCYCLES = 30
ADV_COURANT = 0.25
WAVE_COURANT = 0.5
VISC_NUM = 4.0
DIFF_NUM = 1.0
ALPHA_T = 0.3
BETA_S = 0.6

F32 = jnp.float32
MESH = pl.DeviceIdType.MESH
VMEM = pltpu.VMEM
OFF = 8
IPAD = NI + 16
IEXT = NI + 2 * HALO
JEXT = NJ + 2 * HALO
EAST, WEST = slice(NI - 1, NI), slice(0, 1)
OWN = slice(OFF, OFF + NI)
WEST_HALO, EAST_HALO = slice(OFF - 1, OFF), slice(OFF + NI, OFF + NI + 1)
BEFORE, AFTER = slice(0, OFF), slice(OFF + NI, IPAD)
CORE = slice(HALO, HALO + NI)
LOW, HIGH = slice(0, HALO), slice(HALO + NI, IEXT)
FAR_EAST, FAR_WEST = slice(NI - HALO, NI), slice(0, HALO)


def solve_constants(diff):
    ratio, inner, last = [], [], []
    c_prev = 0.0
    for k in range(LEVELS):
        lower = diff if k > 0 else 0.0
        pivot = 1.0 + diff + lower - lower * c_prev
        inner.append(1.0 / pivot)
        last.append(1.0 / (1.0 + lower - lower * c_prev))
        c_prev = diff / pivot
        ratio.append(c_prev)
    return ratio, inner, last


RATIO_V, INNER_V, LAST_V = solve_constants(VISC_NUM)
RATIO_D, INNER_D, LAST_D = solve_constants(DIFF_NUM)


def sm_weights():
    s = np.arange(1, SUBCYCLES + 1, dtype=np.float64) / (SUBCYCLES + 1)
    raw = s ** 2 * (1.0 - s ** 4)
    return raw / np.sum(raw)


WEIGHTS = sm_weights()
TAIL_WEIGHTS = np.cumsum(WEIGHTS[::-1])[::-1]
MEAN_STEP = float(np.sum(WEIGHTS * np.arange(1, SUBCYCLES + 1)))
MESSAGES = 32
STAGGER = 500
TALL = 16
PARTS = ((0, 16), (16, 32), (32, 48), (48, LEVELS))
SPARE = 2 * LEVELS
LAG_M = 2
LAG = 4
CHUNK = 24


def rot(x, shift):
    shift = shift % x.shape[-1]
    return pltpu.roll(x, shift, 1) if shift else x


def back(x):
    return rot(x, 1)


def ahead(x):
    return rot(x, -1)


def keep(mask, x):
    return jnp.where(mask, x, 0.0)


def pos(x):
    return jnp.maximum(x, 0.0)


def neg(x):
    return jnp.minimum(x, 0.0)


def per_level(x, count):
    return x / jnp.maximum(count, 1.0)


ETA, TU, TV, WET_DEP = range(4)
DEP, KMT = range(2)
U, V, T, S, MEAN, PRES, T_FLUX, S_FLUX = range(8)
UV, TS = range(2)


def exchange_kernel(
    col_count, row_count,
    u_hbm, v_hbm, t_hbm, s_hbm, eta_hbm, tu_hbm, tv_hbm, dep_hbm, kmt_hbm,
    du_o, dv_o, dt_o, ds_o, flat_o,
    u3, v3, t3, s3, p3, un3, us3, vn3, vs3, tn3, sn3, st2, nd2, near_w, near_e, kmt_i, ext2, pk2n, pk2s, hs2, hn2,
    pack, mn, ms, in_s, in_n, rr,
    ff, extf, pkfn, pkfs, hsf, hnf,
    kmu, kmw, kmv, hu2, hv2, smr,
    b_e0, b_e1, b_d, b_p, b_wu, b_ww, b_wv, b_u, b_v, b_pu, b_pv, b_s, b_g,
    ld3, ld2, snd, rcv,
):
    c = lax.axis_index("col")
    r = lax.axis_index("row")
    has_n = r < row_count - 1
    has_s = r > 0
    label = itertools.count()
    east = lax.rem(c + 1, col_count)
    west = lax.rem(c + col_count - 1, col_count)
    up, down = r + 1, r - 1

    barrier = pltpu.get_barrier_semaphore()

    def greet(cc, row):
        pl.semaphore_signal(barrier, inc=1, device_id=(cc, row), device_id_type=MESH)

    greet(east, r)
    greet(west, r)

    @pl.when(has_n)
    def _():
        for cc in (west, c, east):
            greet(cc, up)

    @pl.when(has_s)
    def _():
        for cc in (west, c, east):
            greet(cc, down)

    loads2 = []
    for f, (src, dst) in enumerate((
            (eta_hbm, st2.at[ETA]), (tu_hbm, st2.at[TU]), (tv_hbm, st2.at[TV]),
            (dep_hbm, nd2.at[DEP, :NI, :]), (kmt_hbm, kmt_i))):
        loads2.append(pltpu.make_async_copy(src, dst, ld2.at[f]))
    loads3 = []
    for f, (src, dst) in enumerate(((t_hbm, t3), (s_hbm, s3), (u_hbm, u3), (v_hbm, v3))):
        loads3.append([
            pltpu.make_async_copy(src.at[lo:hi], dst.at[lo:hi, OWN, :], ld3.at[f, n])
            for n, (lo, hi) in enumerate(PARTS)])

    def fetch(f):
        for cp in loads3[f]:
            cp.start()

    def landed(f):
        for cp in loads3[f]:
            cp.wait()

    fetch(0)
    for cp in loads2:
        cp.start()
    pl.delay(STAGGER)
    fetch(1)
    pl.delay(STAGGER)
    fetch(2)

    def remote(src, dst, cc, row):
        n = next(label)
        return pltpu.make_async_remote_copy(
            src_ref=src, dst_ref=dst, send_sem=snd.at[n], recv_sem=rcv.at[n],
            device_id=(cc, row), device_id_type=MESH)

    def each(go_ew, ew, cond_n, go_n, no, cond_s, so):
        for cp in ew:
            go_ew(cp)
        if no:
            @pl.when(cond_n)
            def _():
                for cp in no:
                    go_n(cp)
        if so:
            @pl.when(cond_s)
            def _():
                for cp in so:
                    go_n(cp)

    def start(ew=(), no=(), so=()):
        go = lambda cp: cp.start()
        each(go, ew, has_n, go, no, has_s, so)

    def recv(ew=(), no=(), so=()):
        go = lambda cp: cp.wait_recv()
        each(go, ew, has_s, go, no, has_n, so)

    def sent(ew=(), no=(), so=()):
        go = lambda cp: cp.wait_send()
        each(go, ew, has_n, go, no, has_s, so)

    g1 = []
    for src, dst in ((u_hbm, u3), (v_hbm, v3), (t_hbm, t3), (s_hbm, s3)):
        g1.append(remote(src.at[:, EAST, :], dst.at[:, WEST_HALO, :], east, r))
        g1.append(remote(src.at[:, WEST, :], dst.at[:, EAST_HALO, :], west, r))

    def near_ns(pn, ps, hs, hn):
        if hs.shape[0] > NI:
            hs, hn = hs.at[CORE, :], hn.at[CORE, :]
        return [remote(pn, hs, c, up)], [remote(ps, hn, c, down)]

    def corners(pn, ps, hs, hn):
        no = [
            remote(pn.at[FAR_EAST, :], hs.at[LOW, :], east, up),
            remote(pn.at[FAR_WEST, :], hs.at[HIGH, :], west, up),
        ]
        so = [
            remote(ps.at[FAR_EAST, :], hn.at[LOW, :], east, down),
            remote(ps.at[FAR_WEST, :], hn.at[HIGH, :], west, down),
        ]
        return no, so

    def side_ew(own, ext):
        return [
            remote(own.at[:, FAR_EAST, :], ext.at[:, LOW, :], east, r),
            remote(own.at[:, FAR_WEST, :], ext.at[:, HIGH, :], west, r),
        ]

    lane64 = lax.broadcasted_iota(jnp.int32, (NI, NJ), 1)
    group64 = lane64 // HALO

    def pack_flat(fields, src, pn, ps):
        top = jnp.zeros((NI, NJ), F32)
        bot = jnp.zeros((NI, NJ), F32)
        for q, f in enumerate(fields):
            x = src[f]
            top = jnp.where(group64 == q, rot(x, HALO * q + HALO), top)
            bot = jnp.where(group64 == q, rot(x, HALO * q), bot)
        pn[...] = top
        ps[...] = bot

    lane8 = lax.broadcasted_iota(jnp.int32, (8, NJ), 1)
    first8 = lane8 == 0
    last8 = lane8 == NJ - 1
    slot64 = lane64 >> 1
    even64 = (lane64 & 1) == 0

    def rows(ib, off=0, size=8):
        return pl.ds(pl.multiple_of(ib * size, 8) + off, size)

    def edge_lanes(size):
        lane = lax.broadcasted_iota(jnp.int32, (size, NJ), 1)
        return lane == 0, lane == NJ - 1

    def pack_edges(f, ref):
        acc = jnp.zeros((NI, NJ), F32)
        for k in range(LEVELS):
            acc = jnp.where(slot64 == k, rot(ref[k, OWN, :], 2 * k + 1), acc)
        pack[f] = acc

    def pack_pair(a):
        x, y = pack[2 * a], pack[2 * a + 1]
        return jnp.where(even64, y, back(x)), jnp.where(even64, ahead(x), y)

    def with_near(top, bottom):
        for f in (DEP, KMT):
            x = nd2[f, :NI, :]
            spare = lane64 == SPARE + f
            top = jnp.where(spare, rot(x, SPARE + f + 1), top)
            bottom = jnp.where(spare, rot(x, SPARE + f), bottom)
        return top, bottom

    landed(0)
    pack_edges(T, t3)
    fetch(3)
    for cp in loads2:
        cp.wait()
    kmt = kmt_i[...].astype(F32)
    nd2[KMT, :NI, :] = kmt
    nd2[:, NI:, :] = jnp.zeros((2, OFF, NJ), F32)
    st2[WET_DEP] = keep(kmt > 0, nd2[DEP, :NI, :])

    pl.semaphore_wait(barrier, 2 + 3 * has_n.astype(jnp.int32) + 3 * has_s.astype(jnp.int32))
    g0 = [
        remote(nd2.at[:, EAST, :], near_w.at[:, WEST, :], east, r),
        remote(nd2.at[:, WEST, :], near_e.at[:, WEST, :], west, r),
    ]
    start(g0 + g1)

    landed(1)
    pack_edges(S, s3)
    mn[TS], ms[TS] = with_near(*pack_pair(TS))
    g3n, g3s = near_ns(mn.at[TS], ms.at[TS], in_s.at[TS, OWN, :], in_n.at[TS, OWN, :])
    start((), g3n, g3s)
    landed(2)
    pack_edges(U, u3)
    landed(3)
    pack_edges(V, v3)
    mn[UV], ms[UV] = pack_pair(UV)
    g5n, g5s = near_ns(mn.at[UV], ms.at[UV], in_s.at[UV, OWN, :], in_n.at[UV, OWN, :])
    g7n = [remote(mn.at[UV, :OFF, :], in_s.at[UV, AFTER, :], west, up)]
    g7s = [remote(ms.at[UV, NI - OFF:NI, :], in_n.at[UV, BEFORE, :], east, down)]
    start((), g5n + g7n, g5s + g7s)
    wide2 = pk2n.at[0], pk2s.at[0], hs2.at[0], hn2.at[0]
    pack_flat(range(4), st2, *wide2[:2])
    g2 = side_ew(st2, ext2)
    g2a_n, g2a_s = near_ns(*wide2)
    gc_n, gc_s = corners(*wide2)
    start(g2, g2a_n + gc_n, g2a_s + gc_s)
    for f in range(4):
        ext2[f, CORE, :] = st2[f]

    def local_body(ib, carry):
        mid, at = rows(ib, OFF, TALL), rows(ib, 0, TALL)
        km = nd2[KMT, at, :]
        thick = 2.0 * per_level(nd2[DEP, at, :], km)
        total = jnp.zeros((TALL, NJ), F32)
        for k in range(LEVELS):
            u, v = u3[k, mid, :], v3[k, mid, :]
            u = 0.25 * u
            un3[k, mid, :] = ahead(u)
            us3[k, at, :] = back(u)
            vn3[k, at, :] = ahead(v)
            vs3[k, mid, :] = back(v)
            dens = keep(km > k, BETA_S * s3[k, mid, :] - ALPHA_T * t3[k, mid, :])
            total = total + dens
            p3[k, mid, :] = (total - 0.5 * dens) * thick
        return carry
    blocks = NI // 8
    lax.fori_loop(0, NI // TALL, local_body, 0)

    recv((), g3n, g3s)
    has_nf = keep(has_n, 1.0).astype(F32)
    has_sf = keep(has_s, 1.0).astype(F32)
    big_n = jnp.full((NI, 1), has_nf) > 0.5
    big_s = jnp.full((NI, 1), has_sf) > 0.5
    depth = nd2[DEP, :NI, :]
    dep_n = keep(big_n, in_n[TS, OWN, SPARE + DEP:SPARE + DEP + 1])
    kmt_n = keep(big_n, in_n[TS, OWN, SPARE + KMT:SPARE + KMT + 1])
    kmt_s = keep(big_s, in_s[TS, OWN, SPARE + KMT:SPARE + KMT + 1])
    last64 = lane64 == NJ - 1
    kmt_north = jnp.where(last64, kmt_n, ahead(kmt))
    dep_north = jnp.where(last64, dep_n, ahead(depth))
    kmv_v = jnp.minimum(kmt, kmt_north)
    kmv[...] = kmv_v
    hv2[...] = keep(kmv_v > 0, 0.5 * (depth + dep_north))

    def u_faces():
        kmu_v = jnp.minimum(nd2[KMT, :NI, :], nd2[KMT, 1:NI + 1, :])
        kmu[...] = kmu_v
        hu2[...] = keep(kmu_v > 0, 0.5 * (nd2[DEP, :NI, :] + nd2[DEP, 1:NI + 1, :]))

    u_faces()

    def unpack_pair(a, where):
        north = keep(has_nf > 0.5, in_n[a, where, :])
        south = keep(has_sf > 0.5, in_s[a, where, :])
        even = (lax.broadcasted_iota(jnp.int32, north.shape, 1) & 1) == 0
        first = jnp.where(even, north, south)
        rr[2 * a, where, :] = 0.25 * first if a == UV else first
        rr[2 * a + 1, where, :] = jnp.where(even, ahead(north), back(south))

    def mean_rows():
        mean_n = rr[U, OWN, :] + rr[U, OFF - 1:OFF + NI - 1, :]
        mean_s = rr[V, OWN, :] + rr[V, OFF + 1:OFF + NI + 1, :]
        rr[MEAN, OWN, :] = jnp.where(even64, mean_n, mean_s)

    unpack_pair(TS, OWN)
    rt, rs = rr[T, OWN, :], rr[S, OWN, :]
    dens = keep((kmt_n > slot64.astype(F32)) & even64, BETA_S * rs - ALPHA_T * rt)
    above = lax.broadcasted_iota(jnp.int32, (NJ, NJ), 0) <= lax.broadcasted_iota(jnp.int32, (NJ, NJ), 1)
    total = jnp.dot(dens, above.astype(F32), precision=lax.Precision.HIGHEST, preferred_element_type=F32)
    rr[PRES, OWN, :] = (total - 0.5 * dens) * (2.0 * per_level(dep_n, kmt_n))
    recv((), g5n, g5s)
    rr[U, BEFORE, :] = jnp.zeros((OFF, NJ), F32)
    rr[V, AFTER, :] = jnp.zeros((OFF, NJ), F32)
    unpack_pair(UV, OWN)
    mean_rows()
    rv = rr[V, OWN, :]
    face_s = jnp.minimum(kmt_s, kmt[:, 0:1]) > slot64.astype(F32)
    vs_pos = keep(face_s, pos(rv))
    vs_neg = keep(face_s, neg(rv))
    rr[T_FLUX, OWN, :] = jnp.where(even64, rt, vs_pos * rt + vs_neg * pack[T])
    rr[S_FLUX, OWN, :] = jnp.where(even64, rs, vs_pos * rs + vs_neg * pack[S])

    def momentum_body(ib):
        at, mid, below, above = rows(ib), rows(ib, OFF), rows(ib, OFF - 1), rows(ib, OFF + 1)
        km_u = kmu[at, :]
        km_v = kmv[at, :]
        qu, qv, qm, qp = (rr[f, mid, :] for f in (U, V, MEAN, PRES))
        zero = jnp.zeros((8, NJ), F32)
        du, dv, st_u, st_v, sr_u, sr_v = (zero,) * 6
        turned = {}
        for step in range(LEVELS + LAG_M):
            k = step
            if k < LEVELS:
                sh = NJ - 1 - 2 * k
                turned[k] = (
                    rot(qu, sh), rot(qv, sh), rot(qm, sh), rot(qp, sh),
                    ahead(p3[k, mid, :]), ahead(t3[k, mid, :]), ahead(s3[k, mid, :]))
            k = step - LAG_M
            if k < 0:
                continue
            hu, hv, hm, hp, p_next, t_next, s_next = turned.pop(k)
            tn3[k, at, :] = t_next
            sn3[k, at, :] = s_next
            u = u3[k, mid, :]
            ue = u3[k, above, :]
            uw = u3[k, below, :]
            v = v3[k, mid, :]
            ve = v3[k, above, :]
            vw = v3[k, below, :]
            p = p3[k, mid, :]
            pe = p3[k, above, :]
            un_k, vs_k = un3[k, mid, :], vs3[k, mid, :]
            un = jnp.where(last8, hu, un_k)
            us = jnp.where(first8, hu, us3[k, at, :])
            vn = jnp.where(last8, hv, vn3[k, at, :])
            vs = jnp.where(first8, hv, vs_k)
            vm4 = (v + ve) + jnp.where(first8, hm, vs_k + vs3[k, above, :])
            um = 0.25 * (u + uw) + jnp.where(last8, hm, un_k + un3[k, below, :])
            pn = jnp.where(last8, hp, p_next)
            tu = (p - pe) - u * (ue - uw) - vm4 * (un - us)
            tv = (p - pn) - um * (ve - vw) - v * (vn - vs)
            wu = km_u > k
            wv = km_v > k
            st_u = st_u + keep(wu, tu)
            st_v = st_v + keep(wv, tv)
            ru_k = u + (0.5 * ADV_COURANT) * tu
            rv_k = v + (0.5 * ADV_COURANT) * tv
            sr_u = sr_u + keep(wu, ru_k)
            sr_v = sr_v + keep(wv, rv_k)
            du = ru_k + RATIO_V[k - 1] * du if k else ru_k
            dv = rv_k + RATIO_V[k - 1] * dv if k else rv_k
            du_o[k, at, :] = du
            dv_o[k, at, :] = dv
        inv_u = per_level(1.0, km_u)
        inv_v = per_level(1.0, km_v)
        ff[0, at, :] = hu2[at, :] * inv_u * (0.5 * st_u)
        ff[1, at, :] = hv2[at, :] * inv_v * (0.5 * st_v)
        smr[0, at, :] = inv_u * sr_u
        smr[1, at, :] = inv_v * sr_v

    def beside():
        recv(g0 + g1, g7n, g7s)
        for f in (DEP, KMT):
            nd2[f, NI:NI + 1, :] = near_e[f, WEST, :]
        u_faces()
        kmt = nd2[KMT, :NI, :]
        first_col = lax.broadcasted_iota(jnp.int32, (NI, NJ), 0) == 0
        kmw[...] = jnp.minimum(kmt, jnp.where(first_col, near_w[KMT, WEST, :], pltpu.roll(kmt, 1, 0)))
        unpack_pair(UV, BEFORE)
        unpack_pair(UV, AFTER)
        mean_rows()
        km_e = near_e[KMT, WEST, :]
        thick_e = 2.0 * per_level(near_e[DEP, WEST, :], km_e)
        tot_e = jnp.zeros((1, NJ), F32)
        for k in range(LEVELS):
            un3[k, WEST_HALO, :] = ahead(0.25 * u3[k, WEST_HALO, :])
            vs3[k, EAST_HALO, :] = back(v3[k, EAST_HALO, :])
            dens_e = keep(km_e > k, BETA_S * s3[k, EAST_HALO, :] - ALPHA_T * t3[k, EAST_HALO, :])
            tot_e = tot_e + dens_e
            p3[k, EAST_HALO, :] = (tot_e - 0.5 * dens_e) * thick_e

    def loop_body(n, carry):
        pl.when(n == blocks - 2)(beside)
        momentum_body(lax.rem(n + 1, blocks))
        return carry
    lax.fori_loop(0, blocks, loop_body, 0)

    force = pkfn.at[0], pkfs.at[0], hsf.at[0], hnf.at[0]
    pack_flat((0, 1), ff, *force[:2])
    g4 = side_ew(ff, extf)
    g4_n, g4_s = near_ns(*force)
    g6_n, g6_s = corners(*force)
    start(g4, g6_n + g4_n, g6_s + g4_s)
    for f in range(2):
        extf[f, CORE, :] = ff[f]

    def tracer_body(ib, carry):
        first, last = edge_lanes(TALL)
        at, mid = rows(ib, 0, TALL), rows(ib, OFF, TALL)
        below, above = rows(ib, OFF - 1, TALL), rows(ib, OFF + 1, TALL)
        km_u = kmu[at, :]
        km_w = kmw[at, :]
        km_v = kmv[at, :]
        fields = ((t3, tn3, rr[T_FLUX, mid, :], dt_o), (s3, sn3, rr[S_FLUX, mid, :], ds_o))
        prev = [None, None]
        turned, flux = {}, {}
        for step in range(LEVELS + 2 * LAG):
            k = step
            if k < LEVELS:
                sh = NJ - 1 - 2 * k
                turned[k] = [rot(q, sh) for _, _, q, _ in fields]
            k = step - LAG
            if 0 <= k < LEVELS:
                v = keep(km_v > k, v3[k, mid, :])
                northward = v > 0
                flux[k] = []
                for (ref, next_ref, _, _), halo in zip(fields, turned.pop(k)):
                    xn = jnp.where(last, halo, next_ref[k, at, :])
                    fn = v * jnp.where(northward, ref[k, mid, :], xn)
                    flux[k].append((fn, back(fn), halo))
            k = step - 2 * LAG
            if k >= 0:
                u = keep(km_u > k, u3[k, mid, :])
                w = keep(km_w > k, u3[k, below, :])
                eastward, from_west = u > 0, w > 0
                for n, ((ref, _, _, out), (fn, fs, halo)) in enumerate(zip(fields, flux.pop(k))):
                    fs = jnp.where(first, halo, fs)
                    x = ref[k, mid, :]
                    fe = u * jnp.where(eastward, x, ref[k, above, :])
                    fw = w * jnp.where(from_west, ref[k, below, :], x)
                    rhs = x - ADV_COURANT * ((fe - fw) + (fn - fs))
                    prev[n] = rhs + RATIO_D[k - 1] * prev[n] if k else rhs
                    out[k, at, :] = prev[n]
        return carry
    lax.fori_loop(0, NI // TALL, tracer_body, 0)

    recv(g2, g2a_n + gc_n, g2a_s + gc_s)
    low_ok = jnp.full((HALO, IEXT), has_sf) > 0.5
    high_ok = jnp.full((HALO, IEXT), has_nf) > 0.5

    def window(ext, hs, hn, q):
        low = keep(low_ok, hs[HALO * q:HALO * (q + 1)])
        high = keep(high_ok, hn[HALO * q:HALO * (q + 1)])
        return jnp.concatenate([low, ext.T, high], axis=0)

    hs_t, hn_t = hs2[0].T, hn2[0].T
    win = pl.ds(8, JEXT)
    north_of = pl.ds(9, JEXT)
    south_of = pl.ds(7, JEXT)
    zpad = jnp.zeros((8, IEXT), F32)
    for ref in (b_e0, b_e1, b_wv, b_v, b_pv, b_s, b_g):
        ref[0:8, :] = zpad
        ref[8 + JEXT:16 + JEXT, :] = zpad
    dp_w = window(ext2[WET_DEP], hs_t, hn_t, WET_DEP)
    b_s[win, :] = dp_w
    dp_n, dp_e = b_s[north_of, :], ahead(dp_w)
    wet_u = (dp_w > 0) & (dp_e > 0)
    wet_v = (dp_w > 0) & (dp_n > 0)
    wu = keep(wet_u, (0.25 * WAVE_COURANT) * (dp_w + dp_e))
    wv = keep(wet_v, (0.25 * WAVE_COURANT) * (dp_w + dp_n))
    b_wu[...] = wu
    b_ww[...] = back(wu)
    b_wv[win, :] = wv
    b_e0[win, :] = keep(dp_w > 0, window(ext2[ETA], hs_t, hn_t, ETA))
    u0 = keep(wet_u, window(ext2[TU], hs_t, hn_t, TU))
    v0 = keep(wet_v, window(ext2[TV], hs_t, hn_t, TV))
    b_u[...] = u0
    b_v[win, :] = v0
    b_d[...] = -WAVE_COURANT * ((u0 - back(u0)) + (v0 - b_v[south_of, :]))

    recv(g4, g4_n + g6_n, g4_s + g6_s)
    hsf_t = hsf[0].T
    hnf_t = hnf[0].T
    push = ADV_COURANT / SUBCYCLES
    pu = keep(wet_u, push * window(extf[0], hsf_t, hnf_t, 0))
    pv = keep(wet_v, push * window(extf[1], hsf_t, hnf_t, 1))
    b_pu[...] = pu
    b_pv[win, :] = pv
    b_p[...] = -WAVE_COURANT * ((pu - back(pu)) + (pv - b_pv[south_of, :]))

    eta_bufs = (b_e0, b_e1)
    turned = {}
    for n in range(1, SUBCYCLES + 1):
        old, new = eta_bufs[(n - 1) % 2], eta_bufs[n % 2]
        fresh = {}
        for ch in range(JEXT // CHUNK):
            lo = CHUNK * ch
            if lo + CHUNK - 1 < HALO - (SUBCYCLES - n) or lo > HALO + NJ + (SUBCYCLES - n):
                continue
            here = pl.ds(lo, CHUNK)
            mid = pl.ds(8 + lo, CHUNK)
            e = old[mid, :]
            d = b_d[here, :]
            if n > 1:
                ee, ew = turned[ch]
                gain = b_wu[here, :] * (ee - e) - b_ww[here, :] * (e - ew)
                gain = gain + b_wv[mid, :] * (old[pl.ds(9 + lo, CHUNK), :] - e)
                gain = gain - b_wv[pl.ds(7 + lo, CHUNK), :] * (e - old[pl.ds(7 + lo, CHUNK), :])
                d = d + (gain + b_p[here, :])
                b_d[here, :] = d
            e = e + d
            new[mid, :] = e
            if n < SUBCYCLES:
                fresh[ch] = (ahead(e), back(e))
            if lo + CHUNK > HALO and lo <= HALO + NJ:
                tail = float(TAIL_WEIGHTS[n - 1])
                if n == 1:
                    b_s[mid, :] = e
                    b_g[mid, :] = tail * e
                else:
                    b_s[mid, :] = b_s[mid, :] + e
                    b_g[mid, :] = b_g[mid, :] + tail * e
        turned = fresh

    mid = pl.ds(8 + HALO, NJ)
    above = pl.ds(9 + HALO, NJ)
    core = pl.ds(HALO, NJ)
    last = eta_bufs[SUBCYCLES % 2]
    flat_o[0] = last[mid, :].T[CORE]
    wu = b_wu[core, :] * 2.0
    wv = b_wv[mid, :] * 2.0
    pu, pv, u0, v0 = b_pu[core, :], b_pv[mid, :], b_u[core, :], b_v[mid, :]
    s, g = b_s[mid, :], b_g[mid, :]
    flat_o[1] = (u0 + SUBCYCLES * pu - wu * (ahead(s) - s)).T[CORE]
    flat_o[2] = (v0 + SUBCYCLES * pv - wv * (b_s[above, :] - s)).T[CORE]
    mean_u = u0 + MEAN_STEP * pu - wu * (ahead(g) - g)
    mean_v = v0 + MEAN_STEP * pv - wv * (b_g[above, :] - g)
    for f, (mean, depth_ref, km_ref) in enumerate(((mean_u, hu2, kmu), (mean_v, hv2, kmv))):
        d = depth_ref[...]
        flat_o[3 + f] = mean.T[CORE] / jnp.where(d > 0, d, 1.0) - smr[f]
        flat_o[5 + f] = km_ref[...]
    flat_o[7] = nd2[KMT, :NI, :]

    sent(g0 + g1)
    sent(g2, g3n + g5n + g7n, g3s + g5s + g7s)
    sent((), g2a_n + gc_n, g2a_s + gc_s)
    sent(g4, g4_n + g6_n, g4_s + g6_s)


CHUNKS = ((54, 62), (42, 54), (28, 42), (14, 28), (0, 14))


def back_kernel(du, dv, dt, ds, flat, eta_h, tu_h, tv_h, u_h, v_h, t_h, s_h, xu, xv, xt, xs, sem2, sem3):
    copies = [pltpu.make_async_copy(flat.at[f], out, sem2.at[f]) for f, out in enumerate((eta_h, tu_h, tv_h))]
    for cp in copies:
        cp.start()
    results = ((xu, u_h), (xv, v_h), (xt, t_h), (xs, s_h))
    for n, (lo, hi) in enumerate(CHUNKS):
        def body(ib, carry):
            rows = pl.ds(pl.multiple_of(ib * 8, 8), 8)
            cu, cv, ku, kv, kt = (flat[f, rows, :] for f in range(3, 8))
            x = [jnp.zeros((8, NJ), F32) if hi == LEVELS else ref[LEVELS, rows, :] for ref, _ in results]
            for k in range(hi - 1, lo - 1, -1):
                wu, wv = ku > k, kv > k
                fu = jnp.where(ku > k + 1, INNER_V[k], keep(wu, LAST_V[k]))
                fv = jnp.where(kv > k + 1, INNER_V[k], keep(wv, LAST_V[k]))
                ft = jnp.where(kt > k + 1, INNER_D[k], keep(kt > k, LAST_D[k]))
                x[0] = fu * du[k, rows, :] + RATIO_V[k] * x[0]
                x[1] = fv * dv[k, rows, :] + RATIO_V[k] * x[1]
                x[2] = ft * dt[k, rows, :] + RATIO_D[k] * x[2]
                x[3] = ft * ds[k, rows, :] + RATIO_D[k] * x[3]
                xu[k, rows, :] = keep(wu, x[0] + cu)
                xv[k, rows, :] = keep(wv, x[1] + cv)
                xt[k, rows, :] = x[2]
                xs[k, rows, :] = x[3]
            for (ref, _), val in zip(results, x):
                ref[LEVELS, rows, :] = val
            return carry
        lax.fori_loop(0, NI // 8, body, 0)
        for f, (src, out) in enumerate(results):
            cp = pltpu.make_async_copy(src.at[lo:hi], out.at[lo:hi], sem3.at[n, f])
            cp.start()
            copies.append(cp)
    for cp in copies:
        cp.wait()


def solution(mesh):
    col_count = mesh.shape['col']
    row_count = mesh.shape['row']

    def ocean_step(*args):
        flipped = [jnp.swapaxes(x, -1, -2) for x in args]
        cube = (LEVELS, NI, NJ)
        flat = (NI, NJ)
        dma = pltpu.SemaphoreType.DMA
        hbm = pl.BlockSpec(memory_space=pltpu.HBM)
        vmem = pl.BlockSpec(memory_space=VMEM)
        padded = VMEM((LEVELS, IPAD, NJ), F32)
        pair = VMEM((2,) + flat, F32)
        block = VMEM(cube, F32)
        single = VMEM((1,) + flat, F32)
        near = VMEM((2, OFF, NJ), F32)
        wide = VMEM((JEXT + 16, IEXT), F32)
        plain = VMEM((JEXT, IEXT), F32)
        inner = pl.pallas_call(
            functools.partial(exchange_kernel, col_count, row_count),
            out_shape=tuple(VMEM(cube, F32) for _ in range(4)) + (VMEM((8,) + flat, F32),),
            in_specs=[hbm] * 9,
            out_specs=(vmem,) * 5,
            scratch_shapes=[
                padded, padded, padded, padded, padded, padded, block, block, padded, block, block,
                VMEM((4,) + flat, F32), VMEM((2, NI + OFF, NJ), F32), near, near, VMEM(flat, jnp.int32),
                VMEM((4, IEXT, NJ), F32), single, single, VMEM((1, IEXT, NJ), F32), VMEM((1, IEXT, NJ), F32),
                VMEM((4,) + flat, F32), pair, pair,
                VMEM((2, IPAD, NJ), F32), VMEM((2, IPAD, NJ), F32), VMEM((8, IPAD, NJ), F32),
                pair, VMEM((2, IEXT, NJ), F32),
                single, single,
                VMEM((1, IEXT, NJ), F32), VMEM((1, IEXT, NJ), F32),
                VMEM(flat, F32), VMEM(flat, F32), VMEM(flat, F32),
                VMEM(flat, F32), VMEM(flat, F32), pair,
                wide, wide, plain, plain, plain, plain, wide, plain, wide, plain, wide, wide, wide,
                dma((4, len(PARTS))), dma((5,)), dma((MESSAGES,)), dma((MESSAGES,)),
            ],
            compiler_params=pltpu.CompilerParams(
                collective_id=0, has_side_effects=True, vmem_limit_bytes=54 * 2 ** 20),
        )(*flipped)
        spare = VMEM((LEVELS + 1,) + flat, F32)
        outs = pl.pallas_call(
            back_kernel,
            out_shape=tuple(jax.ShapeDtypeStruct(flat, F32) for _ in range(3))
            + tuple(jax.ShapeDtypeStruct(cube, F32) for _ in range(4)),
            in_specs=[vmem] * 5,
            out_specs=(hbm,) * 7,
            scratch_shapes=[spare, spare, spare, spare, dma((3,)), dma((len(CHUNKS), 4))],
            compiler_params=pltpu.CompilerParams(vmem_limit_bytes=40 * 2 ** 20),
        )(*inner)
        return tuple(jnp.swapaxes(x, -1, -2) for x in outs)

    spec_3d = P(None, 'row', 'col')
    spec_2d = P('row', 'col')
    return jax.shard_map(ocean_step, mesh=mesh, in_specs=(spec_3d,) * 4 + (spec_2d,) * 5, out_specs=(spec_2d,) * 3 + (spec_3d,) * 4, check_vma=False)
```

```python
import functools
import itertools

import jax
import jax.numpy as jnp
import numpy as np
from jax import lax
from jax.experimental import pallas as pl
from jax.experimental.pallas import tpu as pltpu
from jax.sharding import PartitionSpec as P

LEVELS = 62
NI = 64
NJ = 128
HALO = 32
SUBCYCLES = 30
ADV_COURANT = 0.25
WAVE_COURANT = 0.5
VISC_NUM = 4.0
DIFF_NUM = 1.0
ALPHA_T = 0.3
BETA_S = 0.6

F32 = jnp.float32
MESH = pl.DeviceIdType.MESH
VMEM = pltpu.VMEM
OFF = 8
IPAD = NI + 16
IEXT = NI + 2 * HALO
JEXT = NJ + 2 * HALO
EAST, WEST = slice(NI - 1, NI), slice(0, 1)
OWN = slice(OFF, OFF + NI)
WEST_HALO, EAST_HALO = slice(OFF - 1, OFF), slice(OFF + NI, OFF + NI + 1)
BEFORE, AFTER = slice(0, OFF), slice(OFF + NI, IPAD)
CORE = slice(HALO, HALO + NI)
LOW, HIGH = slice(0, HALO), slice(HALO + NI, IEXT)
FAR_EAST, FAR_WEST = slice(NI - HALO, NI), slice(0, HALO)


def solve_constants(diff):
    ratio, inner, last = [], [], []
    c_prev = 0.0
    for k in range(LEVELS):
        lower = diff if k > 0 else 0.0
        pivot = 1.0 + diff + lower - lower * c_prev
        inner.append(1.0 / pivot)
        last.append(1.0 / (1.0 + lower - lower * c_prev))
        c_prev = diff / pivot
        ratio.append(c_prev)
    return ratio, inner, last


RATIO_V, INNER_V, LAST_V = solve_constants(VISC_NUM)
RATIO_D, INNER_D, LAST_D = solve_constants(DIFF_NUM)


def sm_weights():
    s = np.arange(1, SUBCYCLES + 1, dtype=np.float64) / (SUBCYCLES + 1)
    raw = s ** 2 * (1.0 - s ** 4)
    return raw / np.sum(raw)


WEIGHTS = sm_weights()
TAIL_WEIGHTS = np.cumsum(WEIGHTS[::-1])[::-1]
MEAN_STEP = float(np.sum(WEIGHTS * np.arange(1, SUBCYCLES + 1)))
MESSAGES = 33
STAGGER = 500
TALL = 16
PARTS = ((0, 16), (16, 32), (32, 48), (48, LEVELS))
SPARE = 2 * LEVELS
LAG_M = 2
LAG = 4
CHUNK = 24


def rot(x, shift):
    shift = shift % x.shape[-1]
    return pltpu.roll(x, shift, 1) if shift else x


def back(x):
    return rot(x, 1)


def ahead(x):
    return rot(x, -1)


def keep(mask, x):
    return jnp.where(mask, x, 0.0)


def pos(x):
    return jnp.maximum(x, 0.0)


def neg(x):
    return jnp.minimum(x, 0.0)


def per_level(x, count):
    return x / jnp.maximum(count, 1.0)


ETA, STEP, WET_DEP, TU, TV = range(5)
WIDE = 3
DEP, KMT, SOUTH_V = range(3)
U, V, T, S, MEAN, PRES, T_FLUX, S_FLUX = range(8)
UV, TS = range(2)


def exchange_kernel(
    col_count, row_count,
    u_hbm, v_hbm, t_hbm, s_hbm, eta_hbm, tu_hbm, tv_hbm, dep_hbm, kmt_hbm,
    du_o, dv_o, dt_o, ds_o, flat_o,
    u3, v3, t3, s3, p3, un3, us3, vn3, vs3, tn3, sn3, st2, nd2, near_w, near_e, near_u, kmt_i, ext2, pk2n, pk2s, hs2, hn2,
    pack, mn, ms, in_s, in_n, rr,
    ff, extf, pkfn, pkfs, hsf, hnf, fold, fold_in,
    kmu, kmw, kmv, hu2, hv2, smr,
    b_e0, b_e1, b_d, b_p, b_wu, b_ww, b_wv, b_pu, b_pv, b_s, b_g,
    ld3, ld2, snd, rcv,
):
    c = lax.axis_index("col")
    r = lax.axis_index("row")
    has_n = r < row_count - 1
    has_s = r > 0
    label = itertools.count()
    east = lax.rem(c + 1, col_count)
    west = lax.rem(c + col_count - 1, col_count)
    up, down = r + 1, r - 1

    barrier = pltpu.get_barrier_semaphore()

    def greet(cc, row):
        pl.semaphore_signal(barrier, inc=1, device_id=(cc, row), device_id_type=MESH)

    greet(east, r)
    greet(west, r)

    @pl.when(has_n)
    def _():
        for cc in (west, c, east):
            greet(cc, up)

    @pl.when(has_s)
    def _():
        for cc in (west, c, east):
            greet(cc, down)

    loads2 = []
    for f, (src, dst) in enumerate((
            (eta_hbm, st2.at[ETA]), (tu_hbm, st2.at[TU]), (tv_hbm, st2.at[TV]),
            (dep_hbm, nd2.at[DEP, :NI, :]), (kmt_hbm, kmt_i))):
        loads2.append(pltpu.make_async_copy(src, dst, ld2.at[f]))
    loads3 = []
    for f, (src, dst) in enumerate(((t_hbm, t3), (s_hbm, s3), (u_hbm, u3), (v_hbm, v3))):
        loads3.append([
            pltpu.make_async_copy(src.at[lo:hi], dst.at[lo:hi, OWN, :], ld3.at[f, n])
            for n, (lo, hi) in enumerate(PARTS)])

    def fetch(f):
        for cp in loads3[f]:
            cp.start()

    def landed(f):
        for cp in loads3[f]:
            cp.wait()

    fetch(0)
    for cp in loads2:
        cp.start()
    pl.delay(STAGGER)
    fetch(1)
    pl.delay(STAGGER)
    fetch(2)

    def remote(src, dst, cc, row):
        n = next(label)
        return pltpu.make_async_remote_copy(
            src_ref=src, dst_ref=dst, send_sem=snd.at[n], recv_sem=rcv.at[n],
            device_id=(cc, row), device_id_type=MESH)

    def each(go_ew, ew, cond_n, go_n, no, cond_s, so):
        for cp in ew:
            go_ew(cp)
        if no:
            @pl.when(cond_n)
            def _():
                for cp in no:
                    go_n(cp)
        if so:
            @pl.when(cond_s)
            def _():
                for cp in so:
                    go_n(cp)

    def start(ew=(), no=(), so=()):
        go = lambda cp: cp.start()
        each(go, ew, has_n, go, no, has_s, so)

    def recv(ew=(), no=(), so=()):
        go = lambda cp: cp.wait_recv()
        each(go, ew, has_s, go, no, has_n, so)

    def sent(ew=(), no=(), so=()):
        go = lambda cp: cp.wait_send()
        each(go, ew, has_n, go, no, has_s, so)

    g1 = []
    for src, dst in ((u_hbm, u3), (v_hbm, v3), (t_hbm, t3), (s_hbm, s3)):
        g1.append(remote(src.at[:, EAST, :], dst.at[:, WEST_HALO, :], east, r))
        g1.append(remote(src.at[:, WEST, :], dst.at[:, EAST_HALO, :], west, r))

    def near_ns(pn, ps, hs, hn):
        if hs.shape[0] > NI:
            hs, hn = hs.at[CORE, :], hn.at[CORE, :]
        return [remote(pn, hs, c, up)], [remote(ps, hn, c, down)]

    def corners(pn, ps, hs, hn):
        no = [
            remote(pn.at[FAR_EAST, :], hs.at[LOW, :], east, up),
            remote(pn.at[FAR_WEST, :], hs.at[HIGH, :], west, up),
        ]
        so = [
            remote(ps.at[FAR_EAST, :], hn.at[LOW, :], east, down),
            remote(ps.at[FAR_WEST, :], hn.at[HIGH, :], west, down),
        ]
        return no, so

    def side_ew(own, ext):
        return [
            remote(own.at[:ext.shape[0], FAR_EAST, :], ext.at[:, LOW, :], east, r),
            remote(own.at[:ext.shape[0], FAR_WEST, :], ext.at[:, HIGH, :], west, r),
        ]

    lane64 = lax.broadcasted_iota(jnp.int32, (NI, NJ), 1)
    group64 = lane64 // HALO

    def pack_flat(fields, src, pn, ps):
        top = jnp.zeros((NI, NJ), F32)
        bot = jnp.zeros((NI, NJ), F32)
        for q, f in enumerate(fields):
            x = src[f]
            top = jnp.where(group64 == q, rot(x, HALO * q + HALO), top)
            bot = jnp.where(group64 == q, rot(x, HALO * q), bot)
        pn[...] = top
        ps[...] = bot

    lane8 = lax.broadcasted_iota(jnp.int32, (8, NJ), 1)
    first8 = lane8 == 0
    last8 = lane8 == NJ - 1
    slot64 = lane64 >> 1
    even64 = (lane64 & 1) == 0

    def rows(ib, off=0, size=8):
        return pl.ds(pl.multiple_of(ib * size, 8) + off, size)

    def edge_lanes(size):
        lane = lax.broadcasted_iota(jnp.int32, (size, NJ), 1)
        return lane == 0, lane == NJ - 1

    def pack_edges(f, ref):
        acc = jnp.zeros((NI, NJ), F32)
        for k in range(LEVELS):
            acc = jnp.where(slot64 == k, rot(ref[k, OWN, :], 2 * k + 1), acc)
        pack[f] = acc

    def pack_pair(a):
        x, y = pack[2 * a], pack[2 * a + 1]
        return jnp.where(even64, y, back(x)), jnp.where(even64, ahead(x), y)

    def with_near(top, bottom):
        for f in (DEP, KMT):
            x = nd2[f, :NI, :]
            spare = lane64 == SPARE + f
            top = jnp.where(spare, rot(x, SPARE + f + 1), top)
            bottom = jnp.where(spare, rot(x, SPARE + f), bottom)
        top = jnp.where(lane64 == SPARE + SOUTH_V, rot(st2[TV], SPARE + SOUTH_V + 1), top)
        return top, bottom

    landed(0)
    pack_edges(T, t3)
    fetch(3)
    for cp in loads2:
        cp.wait()
    kmt = kmt_i[...].astype(F32)
    nd2[KMT, :NI, :] = kmt
    nd2[:, NI:, :] = jnp.zeros((2, OFF, NJ), F32)
    st2[WET_DEP] = keep(kmt > 0, nd2[DEP, :NI, :])

    pl.semaphore_wait(barrier, 2 + 3 * has_n.astype(jnp.int32) + 3 * has_s.astype(jnp.int32))
    g0 = [
        remote(nd2.at[:, EAST, :], near_w.at[:, WEST, :], east, r),
        remote(nd2.at[:, WEST, :], near_e.at[:, WEST, :], west, r),
        remote(st2.at[TU:TU + 1, EAST, :], near_u.at[:, WEST, :], east, r),
    ]
    start(g0 + g1)

    landed(1)
    pack_edges(S, s3)
    mn[TS], ms[TS] = with_near(*pack_pair(TS))
    g3n, g3s = near_ns(mn.at[TS], ms.at[TS], in_s.at[TS, OWN, :], in_n.at[TS, OWN, :])
    start((), g3n, g3s)
    landed(2)
    pack_edges(U, u3)
    landed(3)
    pack_edges(V, v3)
    mn[UV], ms[UV] = pack_pair(UV)
    g5n, g5s = near_ns(mn.at[UV], ms.at[UV], in_s.at[UV, OWN, :], in_n.at[UV, OWN, :])
    g7n = [remote(mn.at[UV, :OFF, :], in_s.at[UV, AFTER, :], west, up)]
    g7s = [remote(ms.at[UV, NI - OFF:NI, :], in_n.at[UV, BEFORE, :], east, down)]
    start((), g5n + g7n, g5s + g7s)
    def local_body(ib, carry):
        mid, at = rows(ib, OFF, TALL), rows(ib, 0, TALL)
        km = nd2[KMT, at, :]
        thick = 2.0 * per_level(nd2[DEP, at, :], km)
        total = jnp.zeros((TALL, NJ), F32)
        for k in range(LEVELS):
            u, v = u3[k, mid, :], v3[k, mid, :]
            u = 0.25 * u
            un3[k, mid, :] = ahead(u)
            us3[k, at, :] = back(u)
            vn3[k, at, :] = ahead(v)
            vs3[k, mid, :] = back(v)
            dens = keep(km > k, BETA_S * s3[k, mid, :] - ALPHA_T * t3[k, mid, :])
            total = total + dens
            p3[k, mid, :] = (total - 0.5 * dens) * thick
        return carry
    blocks = NI // 8
    lax.fori_loop(0, NI // TALL, local_body, 0)

    recv(g0, g3n, g3s)
    for f in (DEP, KMT):
        nd2[f, NI:NI + 1, :] = near_e[f, WEST, :]
    has_nf = keep(has_n, 1.0).astype(F32)
    has_sf = keep(has_s, 1.0).astype(F32)
    big_n = jnp.full((NI, 1), has_nf) > 0.5
    big_s = jnp.full((NI, 1), has_sf) > 0.5
    depth = nd2[DEP, :NI, :]
    dep_n = keep(big_n, in_n[TS, OWN, SPARE + DEP:SPARE + DEP + 1])
    kmt_n = keep(big_n, in_n[TS, OWN, SPARE + KMT:SPARE + KMT + 1])
    kmt_s = keep(big_s, in_s[TS, OWN, SPARE + KMT:SPARE + KMT + 1])
    last64 = lane64 == NJ - 1
    kmt_north = jnp.where(last64, kmt_n, ahead(kmt))
    dep_north = jnp.where(last64, dep_n, ahead(depth))
    kmv_v = jnp.minimum(kmt, kmt_north)
    kmv[...] = kmv_v
    hv2[...] = keep(kmv_v > 0, 0.5 * (depth + dep_north))

    kmu_v = jnp.minimum(kmt, nd2[KMT, 1:NI + 1, :])
    kmu[...] = kmu_v
    hu2[...] = keep(kmu_v > 0, 0.5 * (depth + nd2[DEP, 1:NI + 1, :]))
    first_col = lax.broadcasted_iota(jnp.int32, (NI, NJ), 0) == 0
    kmw_v = jnp.minimum(kmt, jnp.where(first_col, near_w[KMT, WEST, :], pltpu.roll(kmt, 1, 0)))
    kmw[...] = kmw_v

    u0, v0 = keep(kmu_v > 0, st2[TU]), keep(kmv_v > 0, st2[TV])
    u0_west = jnp.where(first_col, keep(kmw_v > 0, near_u[0, WEST, :]), pltpu.roll(u0, 1, 0))
    v_s = in_s[TS, OWN, SPARE + SOUTH_V:SPARE + SOUTH_V + 1]
    v0_south = jnp.where(lane64 == 0, keep(jnp.minimum(kmt_s, kmt) > 0, v_s), back(v0))
    st2[STEP] = -WAVE_COURANT * ((u0 - u0_west) + (v0 - v0_south))
    wide2 = pk2n.at[0], pk2s.at[0], hs2.at[0], hn2.at[0]
    pack_flat(range(WIDE), st2, *wide2[:2])
    g2 = side_ew(st2, ext2)
    g2a_n, g2a_s = near_ns(*wide2)
    gc_n, gc_s = corners(*wide2)
    start(g2, g2a_n + gc_n, g2a_s + gc_s)
    for f in range(WIDE):
        ext2[f, CORE, :] = st2[f]

    def unpack_pair(a, where):
        north = keep(has_nf > 0.5, in_n[a, where, :])
        south = keep(has_sf > 0.5, in_s[a, where, :])
        even = (lax.broadcasted_iota(jnp.int32, north.shape, 1) & 1) == 0
        first = jnp.where(even, north, south)
        rr[2 * a, where, :] = 0.25 * first if a == UV else first
        rr[2 * a + 1, where, :] = jnp.where(even, ahead(north), back(south))

    def mean_rows():
        mean_n = rr[U, OWN, :] + rr[U, OFF - 1:OFF + NI - 1, :]
        mean_s = rr[V, OWN, :] + rr[V, OFF + 1:OFF + NI + 1, :]
        rr[MEAN, OWN, :] = jnp.where(even64, mean_n, mean_s)

    unpack_pair(TS, OWN)
    rt, rs = rr[T, OWN, :], rr[S, OWN, :]
    dens = keep((kmt_n > slot64.astype(F32)) & even64, BETA_S * rs - ALPHA_T * rt)
    above = lax.broadcasted_iota(jnp.int32, (NJ, NJ), 0) <= lax.broadcasted_iota(jnp.int32, (NJ, NJ), 1)
    total = jnp.dot(dens, above.astype(F32), precision=lax.Precision.HIGHEST, preferred_element_type=F32)
    rr[PRES, OWN, :] = (total - 0.5 * dens) * (2.0 * per_level(dep_n, kmt_n))
    recv((), g5n, g5s)
    rr[U, BEFORE, :] = jnp.zeros((OFF, NJ), F32)
    rr[V, AFTER, :] = jnp.zeros((OFF, NJ), F32)
    unpack_pair(UV, OWN)
    mean_rows()
    rv = rr[V, OWN, :]
    face_s = jnp.minimum(kmt_s, kmt[:, 0:1]) > slot64.astype(F32)
    vs_pos = keep(face_s, pos(rv))
    vs_neg = keep(face_s, neg(rv))
    rr[T_FLUX, OWN, :] = jnp.where(even64, rt, vs_pos * rt + vs_neg * pack[T])
    rr[S_FLUX, OWN, :] = jnp.where(even64, rs, vs_pos * rs + vs_neg * pack[S])

    def momentum_body(ib):
        at, mid, below, above = rows(ib), rows(ib, OFF), rows(ib, OFF - 1), rows(ib, OFF + 1)
        km_u = kmu[at, :]
        km_v = kmv[at, :]
        qu, qv, qm, qp = (rr[f, mid, :] for f in (U, V, MEAN, PRES))
        zero = jnp.zeros((8, NJ), F32)
        du, dv, st_u, st_v, sr_u, sr_v = (zero,) * 6
        turned = {}
        for step in range(LEVELS + LAG_M):
            k = step
            if k < LEVELS:
                sh = NJ - 1 - 2 * k
                turned[k] = (
                    rot(qu, sh), rot(qv, sh), rot(qm, sh), rot(qp, sh),
                    ahead(p3[k, mid, :]), ahead(t3[k, mid, :]), ahead(s3[k, mid, :]))
            k = step - LAG_M
            if k < 0:
                continue
            hu, hv, hm, hp, p_next, t_next, s_next = turned.pop(k)
            tn3[k, at, :] = t_next
            sn3[k, at, :] = s_next
            u = u3[k, mid, :]
            ue = u3[k, above, :]
            uw = u3[k, below, :]
            v = v3[k, mid, :]
            ve = v3[k, above, :]
            vw = v3[k, below, :]
            p = p3[k, mid, :]
            pe = p3[k, above, :]
            un_k, vs_k = un3[k, mid, :], vs3[k, mid, :]
            un = jnp.where(last8, hu, un_k)
            us = jnp.where(first8, hu, us3[k, at, :])
            vn = jnp.where(last8, hv, vn3[k, at, :])
            vs = jnp.where(first8, hv, vs_k)
            vm4 = (v + ve) + jnp.where(first8, hm, vs_k + vs3[k, above, :])
            um = 0.25 * (u + uw) + jnp.where(last8, hm, un_k + un3[k, below, :])
            pn = jnp.where(last8, hp, p_next)
            tu = (p - pe) - u * (ue - uw) - vm4 * (un - us)
            tv = (p - pn) - um * (ve - vw) - v * (vn - vs)
            wu = km_u > k
            wv = km_v > k
            st_u = st_u + keep(wu, tu)
            st_v = st_v + keep(wv, tv)
            ru_k = u + (0.5 * ADV_COURANT) * tu
            rv_k = v + (0.5 * ADV_COURANT) * tv
            sr_u = sr_u + keep(wu, ru_k)
            sr_v = sr_v + keep(wv, rv_k)
            du = ru_k + RATIO_V[k - 1] * du if k else ru_k
            dv = rv_k + RATIO_V[k - 1] * dv if k else rv_k
            du_o[k, at, :] = du
            dv_o[k, at, :] = dv
        inv_u = per_level(1.0, km_u)
        inv_v = per_level(1.0, km_v)
        ff[0, at, :] = hu2[at, :] * inv_u * (0.5 * st_u)
        ff[1, at, :] = hv2[at, :] * inv_v * (0.5 * st_v)
        smr[0, at, :] = inv_u * sr_u
        smr[1, at, :] = inv_v * sr_v

    def beside():
        recv(g1, g7n, g7s)
        unpack_pair(UV, BEFORE)
        unpack_pair(UV, AFTER)
        mean_rows()
        km_e = near_e[KMT, WEST, :]
        thick_e = 2.0 * per_level(near_e[DEP, WEST, :], km_e)
        tot_e = jnp.zeros((1, NJ), F32)
        for k in range(LEVELS):
            un3[k, WEST_HALO, :] = ahead(0.25 * u3[k, WEST_HALO, :])
            vs3[k, EAST_HALO, :] = back(v3[k, EAST_HALO, :])
            dens_e = keep(km_e > k, BETA_S * s3[k, EAST_HALO, :] - ALPHA_T * t3[k, EAST_HALO, :])
            tot_e = tot_e + dens_e
            p3[k, EAST_HALO, :] = (tot_e - 0.5 * dens_e) * thick_e

    def loop_body(n, carry):
        pl.when(n == blocks - 2)(beside)
        momentum_body(lax.rem(n + 1, blocks))
        return carry
    lax.fori_loop(0, blocks, loop_body, 0)

    force = pkfn.at[0], pkfs.at[0], hsf.at[0], hnf.at[0]
    pack_flat((0, 1), ff, *force[:2])
    g4 = side_ew(ff, extf)
    g4_n, g4_s = near_ns(*force)
    half = HALO // 2
    g6_n, g6_s = [], []
    for n, (packed, row, out) in enumerate(((pkfn, up, g6_n), (pkfs, down, g6_s))):
        for m, (near, far, cc) in enumerate((
                (slice(NI - half, NI), slice(NI - HALO, NI - half), east),
                (slice(0, half), slice(half, HALO), west))):
            fold[n, m] = jnp.where(group64[:half] < 2, packed[0, near, :], rot(packed[0, far, :], 2 * HALO))
            out.append(remote(fold.at[n, m], fold_in.at[n, m], cc, row))
    start(g4, g6_n + g4_n, g6_s + g4_s)
    for f in range(2):
        extf[f, CORE, :] = ff[f]

    def tracer_body(ib, carry):
        first, last = edge_lanes(TALL)
        at, mid = rows(ib, 0, TALL), rows(ib, OFF, TALL)
        below, above = rows(ib, OFF - 1, TALL), rows(ib, OFF + 1, TALL)
        km_u = kmu[at, :]
        km_w = kmw[at, :]
        km_v = kmv[at, :]
        fields = ((t3, tn3, rr[T_FLUX, mid, :], dt_o), (s3, sn3, rr[S_FLUX, mid, :], ds_o))
        prev = [None, None]
        turned, flux = {}, {}
        for step in range(LEVELS + 2 * LAG):
            k = step
            if k < LEVELS:
                sh = NJ - 1 - 2 * k
                turned[k] = [rot(q, sh) for _, _, q, _ in fields]
            k = step - LAG
            if 0 <= k < LEVELS:
                v = keep(km_v > k, v3[k, mid, :])
                northward = v > 0
                flux[k] = []
                for (ref, next_ref, _, _), halo in zip(fields, turned.pop(k)):
                    xn = jnp.where(last, halo, next_ref[k, at, :])
                    fn = v * jnp.where(northward, ref[k, mid, :], xn)
                    flux[k].append((fn, back(fn), halo))
            k = step - 2 * LAG
            if k >= 0:
                u = keep(km_u > k, u3[k, mid, :])
                w = keep(km_w > k, u3[k, below, :])
                eastward, from_west = u > 0, w > 0
                for n, ((ref, _, _, out), (fn, fs, halo)) in enumerate(zip(fields, flux.pop(k))):
                    fs = jnp.where(first, halo, fs)
                    x = ref[k, mid, :]
                    fe = u * jnp.where(eastward, x, ref[k, above, :])
                    fw = w * jnp.where(from_west, ref[k, below, :], x)
                    rhs = x - ADV_COURANT * ((fe - fw) + (fn - fs))
                    prev[n] = rhs + RATIO_D[k - 1] * prev[n] if k else rhs
                    out[k, at, :] = prev[n]
        return carry
    lax.fori_loop(0, NI // TALL, tracer_body, 0)

    recv(g2, g2a_n + gc_n, g2a_s + gc_s)
    low_ok = jnp.full((HALO, IEXT), has_sf) > 0.5
    high_ok = jnp.full((HALO, IEXT), has_nf) > 0.5

    def window(ext, hs, hn, q):
        low = keep(low_ok, hs[HALO * q:HALO * (q + 1)])
        high = keep(high_ok, hn[HALO * q:HALO * (q + 1)])
        return jnp.concatenate([low, ext.T, high], axis=0)

    hs_t, hn_t = hs2[0].T, hn2[0].T
    win = pl.ds(8, JEXT)
    north_of = pl.ds(9, JEXT)
    south_of = pl.ds(7, JEXT)
    zpad = jnp.zeros((8, IEXT), F32)
    for ref in (b_e0, b_e1, b_wv, b_pv, b_s, b_g):
        ref[0:8, :] = zpad
        ref[8 + JEXT:16 + JEXT, :] = zpad
    dp_w = window(ext2[WET_DEP], hs_t, hn_t, WET_DEP)
    b_s[win, :] = dp_w
    dp_n, dp_e = b_s[north_of, :], ahead(dp_w)
    wet_u = (dp_w > 0) & (dp_e > 0)
    wet_v = (dp_w > 0) & (dp_n > 0)
    wu = keep(wet_u, (0.25 * WAVE_COURANT) * (dp_w + dp_e))
    wv = keep(wet_v, (0.25 * WAVE_COURANT) * (dp_w + dp_n))
    b_wu[...] = wu
    b_ww[...] = back(wu)
    b_wv[win, :] = wv
    b_e0[win, :] = keep(dp_w > 0, window(ext2[ETA], hs_t, hn_t, ETA))
    b_d[...] = window(ext2[STEP], hs_t, hn_t, STEP)

    def tracer_back(ib, carry):
        at = rows(ib, 0, TALL)
        kt = nd2[KMT, at, :]
        xt = xs = jnp.zeros((TALL, NJ), F32)
        for k in range(LEVELS - 1, -1, -1):
            fac = jnp.where(kt > k + 1, INNER_D[k], keep(kt > k, LAST_D[k]))
            xt = fac * dt_o[k, at, :] + RATIO_D[k] * xt
            xs = fac * ds_o[k, at, :] + RATIO_D[k] * xs
            dt_o[k, at, :] = xt
            ds_o[k, at, :] = xs
        return carry
    lax.fori_loop(0, NI // TALL, tracer_back, 0)

    recv(g4, g4_n + g6_n, g4_s + g6_s)
    for n, ref in enumerate((hsf, hnf)):
        for m, (near, far) in enumerate((
                (slice(half, HALO), slice(0, half)),
                (slice(IEXT - HALO, IEXT - half), slice(IEXT - half, IEXT)))):
            ref[0, near, :] = fold_in[n, m]
            ref[0, far, :] = rot(fold_in[n, m], 2 * HALO)
    hsf_t = hsf[0].T
    hnf_t = hnf[0].T
    push = ADV_COURANT / SUBCYCLES
    pu = keep(wet_u, push * window(extf[0], hsf_t, hnf_t, 0))
    pv = keep(wet_v, push * window(extf[1], hsf_t, hnf_t, 1))
    b_pu[...] = pu
    b_pv[win, :] = pv
    b_p[...] = -WAVE_COURANT * ((pu - back(pu)) + (pv - b_pv[south_of, :]))

    eta_bufs = (b_e0, b_e1)
    turned = {}
    for n in range(1, SUBCYCLES + 1):
        old, new = eta_bufs[(n - 1) % 2], eta_bufs[n % 2]
        fresh = {}
        for ch in range(JEXT // CHUNK):
            lo = CHUNK * ch
            if lo + CHUNK - 1 < HALO - (SUBCYCLES - n) or lo > HALO + NJ + (SUBCYCLES - n):
                continue
            here = pl.ds(lo, CHUNK)
            mid = pl.ds(8 + lo, CHUNK)
            e = old[mid, :]
            d = b_d[here, :]
            if n > 1:
                ee, ew = turned[ch]
                gain = b_wu[here, :] * (ee - e) - b_ww[here, :] * (e - ew)
                gain = gain + b_wv[mid, :] * (old[pl.ds(9 + lo, CHUNK), :] - e)
                gain = gain - b_wv[pl.ds(7 + lo, CHUNK), :] * (e - old[pl.ds(7 + lo, CHUNK), :])
                d = d + (gain + b_p[here, :])
                b_d[here, :] = d
            e = e + d
            new[mid, :] = e
            if n < SUBCYCLES:
                fresh[ch] = (ahead(e), back(e))
            if lo + CHUNK > HALO and lo <= HALO + NJ:
                tail = float(TAIL_WEIGHTS[n - 1])
                if n == 1:
                    b_s[mid, :] = e
                    b_g[mid, :] = tail * e
                else:
                    b_s[mid, :] = b_s[mid, :] + e
                    b_g[mid, :] = b_g[mid, :] + tail * e
        turned = fresh

    mid = pl.ds(8 + HALO, NJ)
    above = pl.ds(9 + HALO, NJ)
    core = pl.ds(HALO, NJ)
    last = eta_bufs[SUBCYCLES % 2]
    flat_o[0] = last[mid, :].T[CORE]
    wu = b_wu[core, :] * 2.0
    wv = b_wv[mid, :] * 2.0
    pu, pv = b_pu[core, :], b_pv[mid, :]
    u0, v0 = keep(kmu[...] > 0, st2[TU]), keep(kmv[...] > 0, st2[TV])
    s, g = b_s[mid, :], b_g[mid, :]
    flat_o[1] = u0 + (SUBCYCLES * pu - wu * (ahead(s) - s)).T[CORE]
    flat_o[2] = v0 + (SUBCYCLES * pv - wv * (b_s[above, :] - s)).T[CORE]
    mean_u = u0 + (MEAN_STEP * pu - wu * (ahead(g) - g)).T[CORE]
    mean_v = v0 + (MEAN_STEP * pv - wv * (b_g[above, :] - g)).T[CORE]
    for f, (mean, depth_ref, km_ref) in enumerate(((mean_u, hu2, kmu), (mean_v, hv2, kmv))):
        d = depth_ref[...]
        flat_o[3 + f] = mean / jnp.where(d > 0, d, 1.0) - smr[f]
        flat_o[5 + f] = km_ref[...]

    sent(g0 + g1)
    sent(g2, g3n + g5n + g7n, g3s + g5s + g7s)
    sent((), g2a_n + gc_n, g2a_s + gc_s)
    sent(g4, g4_n + g6_n, g4_s + g6_s)


CHUNKS = ((42, LEVELS), (21, 42), (0, 21))


def back_kernel(du, dv, t, s, flat, eta_h, tu_h, tv_h, u_h, v_h, t_h, s_h, xu, xv, sem2, sem3):
    whole = ((t, t_h), (s, s_h), (flat.at[0], eta_h), (flat.at[1], tu_h), (flat.at[2], tv_h))
    copies = [pltpu.make_async_copy(src, out, sem2.at[f]) for f, (src, out) in enumerate(whole)]
    for cp in copies:
        cp.start()
    results = ((xu, u_h), (xv, v_h))
    for n, (lo, hi) in enumerate(CHUNKS):
        def body(ib, carry):
            rows = pl.ds(pl.multiple_of(ib * 8, 8), 8)
            cu, cv, ku, kv = (flat[f, rows, :] for f in range(3, 7))
            x, y = (jnp.zeros((8, NJ), F32) if hi == LEVELS else ref[LEVELS, rows, :] for ref, _ in results)
            for k in range(hi - 1, lo - 1, -1):
                wu, wv = ku > k, kv > k
                fu = jnp.where(ku > k + 1, INNER_V[k], keep(wu, LAST_V[k]))
                fv = jnp.where(kv > k + 1, INNER_V[k], keep(wv, LAST_V[k]))
                x = fu * du[k, rows, :] + RATIO_V[k] * x
                y = fv * dv[k, rows, :] + RATIO_V[k] * y
                xu[k, rows, :] = keep(wu, x + cu)
                xv[k, rows, :] = keep(wv, y + cv)
            xu[LEVELS, rows, :] = x
            xv[LEVELS, rows, :] = y
            return carry
        lax.fori_loop(0, NI // 8, body, 0)
        for f, (src, out) in enumerate(results):
            cp = pltpu.make_async_copy(src.at[lo:hi], out.at[lo:hi], sem3.at[n, f])
            cp.start()
            copies.append(cp)
    for cp in copies:
        cp.wait()


def solution(mesh):
    col_count = mesh.shape['col']
    row_count = mesh.shape['row']

    def ocean_step(*args):
        flipped = [jnp.swapaxes(x, -1, -2) for x in args]
        cube = (LEVELS, NI, NJ)
        flat = (NI, NJ)
        dma = pltpu.SemaphoreType.DMA
        hbm = pl.BlockSpec(memory_space=pltpu.HBM)
        vmem = pl.BlockSpec(memory_space=VMEM)
        padded = VMEM((LEVELS, IPAD, NJ), F32)
        pair = VMEM((2,) + flat, F32)
        block = VMEM(cube, F32)
        folded = VMEM((2, 2, HALO // 2, NJ), F32)
        single = VMEM((1,) + flat, F32)
        near = VMEM((2, OFF, NJ), F32)
        wide = VMEM((JEXT + 16, IEXT), F32)
        plain = VMEM((JEXT, IEXT), F32)
        inner = pl.pallas_call(
            functools.partial(exchange_kernel, col_count, row_count),
            out_shape=tuple(VMEM(cube, F32) for _ in range(4)) + (VMEM((7,) + flat, F32),),
            in_specs=[hbm] * 9,
            out_specs=(vmem,) * 5,
            scratch_shapes=[
                padded, padded, padded, padded, padded, padded, block, block, padded, block, block,
                VMEM((5,) + flat, F32), VMEM((2, NI + OFF, NJ), F32), near, near, VMEM((1, OFF, NJ), F32),
                VMEM(flat, jnp.int32), VMEM((WIDE, IEXT, NJ), F32), single, single, VMEM((1, IEXT, NJ), F32), VMEM((1, IEXT, NJ), F32),
                VMEM((4,) + flat, F32), pair, pair,
                VMEM((2, IPAD, NJ), F32), VMEM((2, IPAD, NJ), F32), VMEM((8, IPAD, NJ), F32),
                pair, VMEM((2, IEXT, NJ), F32),
                single, single,
                VMEM((1, IEXT, NJ), F32), VMEM((1, IEXT, NJ), F32), folded, folded,
                VMEM(flat, F32), VMEM(flat, F32), VMEM(flat, F32),
                VMEM(flat, F32), VMEM(flat, F32), pair,
                wide, wide, plain, plain, plain, plain, wide, plain, wide, wide, wide,
                dma((4, len(PARTS))), dma((5,)), dma((MESSAGES,)), dma((MESSAGES,)),
            ],
            compiler_params=pltpu.CompilerParams(
                collective_id=0, has_side_effects=True, vmem_limit_bytes=54 * 2 ** 20),
        )(*flipped)
        spare = VMEM((LEVELS + 1,) + flat, F32)
        outs = pl.pallas_call(
            back_kernel,
            out_shape=tuple(jax.ShapeDtypeStruct(flat, F32) for _ in range(3))
            + tuple(jax.ShapeDtypeStruct(cube, F32) for _ in range(4)),
            in_specs=[vmem] * 5,
            out_specs=(hbm,) * 7,
            scratch_shapes=[spare, spare, dma((5,)), dma((len(CHUNKS), 2))],
            compiler_params=pltpu.CompilerParams(vmem_limit_bytes=40 * 2 ** 20),
        )(*inner)
        return tuple(jnp.swapaxes(x, -1, -2) for x in outs)

    spec_3d = P(None, 'row', 'col')
    spec_2d = P('row', 'col')
    return jax.shard_map(ocean_step, mesh=mesh, in_specs=(spec_3d,) * 4 + (spec_2d,) * 5, out_specs=(spec_2d,) * 3 + (spec_3d,) * 4, check_vma=False)
```

```python
import functools
import itertools

import jax
import jax.numpy as jnp
import numpy as np
from jax import lax
from jax.experimental import pallas as pl
from jax.experimental.pallas import tpu as pltpu
from jax.sharding import PartitionSpec as P

LEVELS = 62
NI = 64
NJ = 128
HALO = 32
SUBCYCLES = 30
ADV_COURANT = 0.25
WAVE_COURANT = 0.5
VISC_NUM = 4.0
DIFF_NUM = 1.0
ALPHA_T = 0.3
BETA_S = 0.6

F32 = jnp.float32
MESH = pl.DeviceIdType.MESH
VMEM = pltpu.VMEM
OFF = 8
IPAD = NI + 16
IEXT = NI + 2 * HALO
JEXT = NJ + 2 * HALO
EAST, WEST = slice(NI - 1, NI), slice(0, 1)
OWN = slice(OFF, OFF + NI)
WEST_HALO, EAST_HALO = slice(OFF - 1, OFF), slice(OFF + NI, OFF + NI + 1)
BEFORE, AFTER = slice(0, OFF), slice(OFF + NI, IPAD)
CORE = slice(HALO, HALO + NI)
LOW, HIGH = slice(0, HALO), slice(HALO + NI, IEXT)
FAR_EAST, FAR_WEST = slice(NI - HALO, NI), slice(0, HALO)


def solve_constants(diff):
    ratio, inner, last = [], [], []
    c_prev = 0.0
    for k in range(LEVELS):
        lower = diff if k > 0 else 0.0
        pivot = 1.0 + diff + lower - lower * c_prev
        inner.append(1.0 / pivot)
        last.append(1.0 / (1.0 + lower - lower * c_prev))
        c_prev = diff / pivot
        ratio.append(c_prev)
    return ratio, inner, last


RATIO_V, INNER_V, LAST_V = solve_constants(VISC_NUM)
RATIO_D, INNER_D, LAST_D = solve_constants(DIFF_NUM)


def sm_weights():
    s = np.arange(1, SUBCYCLES + 1, dtype=np.float64) / (SUBCYCLES + 1)
    raw = s ** 2 * (1.0 - s ** 4)
    return raw / np.sum(raw)


WEIGHTS = sm_weights()
TAIL_WEIGHTS = np.cumsum(WEIGHTS[::-1])[::-1]
MEAN_STEP = float(np.sum(WEIGHTS * np.arange(1, SUBCYCLES + 1)))
MESSAGES = 33
STAGGER = 500
TALL = 16
PARTS = ((0, 16), (16, 32), (32, 48), (48, LEVELS))
SPARE = 2 * LEVELS
LAG_M = 2
LAG = 6
CHUNK = 24


def rot(x, shift):
    shift = shift % x.shape[-1]
    return pltpu.roll(x, shift, 1) if shift else x


def back(x):
    return rot(x, 1)


def ahead(x):
    return rot(x, -1)


def keep(mask, x):
    return jnp.where(mask, x, 0.0)


def pos(x):
    return jnp.maximum(x, 0.0)


def neg(x):
    return jnp.minimum(x, 0.0)


def per_level(x, count):
    return x / jnp.maximum(count, 1.0)


ETA, STEP, WET_DEP, TU, TV = range(5)
WIDE = 3
DEP, KMT, SOUTH_V = range(3)
U, V, T, S, MEAN, PRES, T_FLUX, S_FLUX = range(8)
UV, TS = range(2)


def exchange_kernel(
    col_count, row_count,
    u_hbm, v_hbm, t_hbm, s_hbm, eta_hbm, tu_hbm, tv_hbm, dep_hbm, kmt_hbm,
    du_o, dv_o, dt_o, ds_o, flat_o,
    u3, v3, t3, s3, p3, un3, us3, vn3, vs3, tn3, sn3, st2, nd2, near_w, near_e, near_u, kmt_i, ext2, pk2n, pk2s, hs2, hn2,
    pack, mn, ms, in_s, in_n, rr,
    ff, extf, pkfn, pkfs, hsf, hnf, fold, fold_in,
    kmu, kmw, kmv, hu2, hv2, smr,
    b_e0, b_e1, b_d, b_p, b_wu, b_ww, b_wv, b_pu, b_pv, b_s, b_g,
    ld3, ld2, snd, rcv,
):
    c = lax.axis_index("col")
    r = lax.axis_index("row")
    has_n = r < row_count - 1
    has_s = r > 0
    label = itertools.count()
    east = lax.rem(c + 1, col_count)
    west = lax.rem(c + col_count - 1, col_count)
    up, down = r + 1, r - 1

    barrier = pltpu.get_barrier_semaphore()

    def greet(cc, row):
        pl.semaphore_signal(barrier, inc=1, device_id=(cc, row), device_id_type=MESH)

    greet(east, r)
    greet(west, r)

    @pl.when(has_n)
    def _():
        for cc in (west, c, east):
            greet(cc, up)

    @pl.when(has_s)
    def _():
        for cc in (west, c, east):
            greet(cc, down)

    loads2 = []
    for f, (src, dst) in enumerate((
            (eta_hbm, st2.at[ETA]), (tu_hbm, st2.at[TU]), (tv_hbm, st2.at[TV]),
            (dep_hbm, nd2.at[DEP, :NI, :]), (kmt_hbm, kmt_i))):
        loads2.append(pltpu.make_async_copy(src, dst, ld2.at[f]))
    loads3 = []
    for f, (src, dst) in enumerate(((t_hbm, t3), (s_hbm, s3), (u_hbm, u3), (v_hbm, v3))):
        loads3.append([
            pltpu.make_async_copy(src.at[lo:hi], dst.at[lo:hi, OWN, :], ld3.at[f, n])
            for n, (lo, hi) in enumerate(PARTS)])

    def fetch(f):
        for cp in loads3[f]:
            cp.start()

    def landed(f):
        for cp in loads3[f]:
            cp.wait()

    fetch(0)
    for cp in loads2:
        cp.start()
    pl.delay(STAGGER)
    fetch(1)
    pl.delay(STAGGER)
    fetch(2)

    def remote(src, dst, cc, row):
        n = next(label)
        return pltpu.make_async_remote_copy(
            src_ref=src, dst_ref=dst, send_sem=snd.at[n], recv_sem=rcv.at[n],
            device_id=(cc, row), device_id_type=MESH)

    def each(go_ew, ew, cond_n, go_n, no, cond_s, so):
        for cp in ew:
            go_ew(cp)
        if no:
            @pl.when(cond_n)
            def _():
                for cp in no:
                    go_n(cp)
        if so:
            @pl.when(cond_s)
            def _():
                for cp in so:
                    go_n(cp)

    def start(ew=(), no=(), so=()):
        go = lambda cp: cp.start()
        each(go, ew, has_n, go, no, has_s, so)

    def recv(ew=(), no=(), so=()):
        go = lambda cp: cp.wait_recv()
        each(go, ew, has_s, go, no, has_n, so)

    def sent(ew=(), no=(), so=()):
        go = lambda cp: cp.wait_send()
        each(go, ew, has_n, go, no, has_s, so)

    g1 = []
    for src, dst in ((u_hbm, u3), (v_hbm, v3), (t_hbm, t3), (s_hbm, s3)):
        g1.append(remote(src.at[:, EAST, :], dst.at[:, WEST_HALO, :], east, r))
        g1.append(remote(src.at[:, WEST, :], dst.at[:, EAST_HALO, :], west, r))

    def near_ns(pn, ps, hs, hn):
        if hs.shape[0] > NI:
            hs, hn = hs.at[CORE, :], hn.at[CORE, :]
        return [remote(pn, hs, c, up)], [remote(ps, hn, c, down)]

    def corners(pn, ps, hs, hn):
        no = [
            remote(pn.at[FAR_EAST, :], hs.at[LOW, :], east, up),
            remote(pn.at[FAR_WEST, :], hs.at[HIGH, :], west, up),
        ]
        so = [
            remote(ps.at[FAR_EAST, :], hn.at[LOW, :], east, down),
            remote(ps.at[FAR_WEST, :], hn.at[HIGH, :], west, down),
        ]
        return no, so

    def side_ew(own, ext):
        return [
            remote(own.at[:ext.shape[0], FAR_EAST, :], ext.at[:, LOW, :], east, r),
            remote(own.at[:ext.shape[0], FAR_WEST, :], ext.at[:, HIGH, :], west, r),
        ]

    lane64 = lax.broadcasted_iota(jnp.int32, (NI, NJ), 1)
    group64 = lane64 // HALO

    def pack_flat(fields, src, pn, ps):
        top = jnp.zeros((NI, NJ), F32)
        bot = jnp.zeros((NI, NJ), F32)
        for q, f in enumerate(fields):
            x = src[f]
            top = jnp.where(group64 == q, rot(x, HALO * q + HALO), top)
            bot = jnp.where(group64 == q, rot(x, HALO * q), bot)
        pn[...] = top
        ps[...] = bot

    lane8 = lax.broadcasted_iota(jnp.int32, (8, NJ), 1)
    first8 = lane8 == 0
    last8 = lane8 == NJ - 1
    slot64 = lane64 >> 1
    even64 = (lane64 & 1) == 0

    def rows(ib, off=0, size=8):
        return pl.ds(pl.multiple_of(ib * size, 8) + off, size)

    def edge_lanes(size):
        lane = lax.broadcasted_iota(jnp.int32, (size, NJ), 1)
        return lane == 0, lane == NJ - 1

    def pack_edges(f, ref):
        acc = jnp.zeros((NI, NJ), F32)
        for k in range(LEVELS):
            acc = jnp.where(slot64 == k, rot(ref[k, OWN, :], 2 * k + 1), acc)
        pack[f] = acc

    def pack_pair(a):
        x, y = pack[2 * a], pack[2 * a + 1]
        return jnp.where(even64, y, back(x)), jnp.where(even64, ahead(x), y)

    def with_near(top, bottom):
        for f in (DEP, KMT):
            x = nd2[f, :NI, :]
            spare = lane64 == SPARE + f
            top = jnp.where(spare, rot(x, SPARE + f + 1), top)
            bottom = jnp.where(spare, rot(x, SPARE + f), bottom)
        top = jnp.where(lane64 == SPARE + SOUTH_V, rot(st2[TV], SPARE + SOUTH_V + 1), top)
        return top, bottom

    landed(0)
    pack_edges(T, t3)
    fetch(3)
    for cp in loads2:
        cp.wait()
    kmt = kmt_i[...].astype(F32)
    nd2[KMT, :NI, :] = kmt
    nd2[:, NI:, :] = jnp.zeros((2, OFF, NJ), F32)
    st2[WET_DEP] = keep(kmt > 0, nd2[DEP, :NI, :])

    pl.semaphore_wait(barrier, 2 + 3 * has_n.astype(jnp.int32) + 3 * has_s.astype(jnp.int32))
    g0 = [
        remote(nd2.at[:, EAST, :], near_w.at[:, WEST, :], east, r),
        remote(nd2.at[:, WEST, :], near_e.at[:, WEST, :], west, r),
        remote(st2.at[TU:TU + 1, EAST, :], near_u.at[:, WEST, :], east, r),
    ]
    start(g0 + g1)

    landed(1)
    pack_edges(S, s3)
    mn[TS], ms[TS] = with_near(*pack_pair(TS))
    g3n, g3s = near_ns(mn.at[TS], ms.at[TS], in_s.at[TS, OWN, :], in_n.at[TS, OWN, :])
    start((), g3n, g3s)
    landed(2)
    pack_edges(U, u3)
    landed(3)
    pack_edges(V, v3)
    mn[UV], ms[UV] = pack_pair(UV)
    g5n, g5s = near_ns(mn.at[UV], ms.at[UV], in_s.at[UV, OWN, :], in_n.at[UV, OWN, :])
    g7n = [remote(mn.at[UV, :OFF, :], in_s.at[UV, AFTER, :], west, up)]
    g7s = [remote(ms.at[UV, NI - OFF:NI, :], in_n.at[UV, BEFORE, :], east, down)]
    start((), g5n + g7n, g5s + g7s)
    def local_body(ib, carry):
        mid, at = rows(ib, OFF, TALL), rows(ib, 0, TALL)
        km = nd2[KMT, at, :]
        thick = 2.0 * per_level(nd2[DEP, at, :], km)
        total = jnp.zeros((TALL, NJ), F32)
        for k in range(LEVELS):
            u, v = u3[k, mid, :], v3[k, mid, :]
            u = 0.25 * u
            un3[k, mid, :] = ahead(u)
            us3[k, at, :] = back(u)
            vn3[k, at, :] = ahead(v)
            vs3[k, mid, :] = back(v)
            dens = keep(km > k, BETA_S * s3[k, mid, :] - ALPHA_T * t3[k, mid, :])
            total = total + dens
            p3[k, mid, :] = (total - 0.5 * dens) * thick
        return carry
    blocks = NI // 8
    lax.fori_loop(0, NI // TALL, local_body, 0)

    recv(g0, g3n, g3s)
    for f in (DEP, KMT):
        nd2[f, NI:NI + 1, :] = near_e[f, WEST, :]
    has_nf = keep(has_n, 1.0).astype(F32)
    has_sf = keep(has_s, 1.0).astype(F32)
    big_n = jnp.full((NI, 1), has_nf) > 0.5
    big_s = jnp.full((NI, 1), has_sf) > 0.5
    depth = nd2[DEP, :NI, :]
    dep_n = keep(big_n, in_n[TS, OWN, SPARE + DEP:SPARE + DEP + 1])
    kmt_n = keep(big_n, in_n[TS, OWN, SPARE + KMT:SPARE + KMT + 1])
    kmt_s = keep(big_s, in_s[TS, OWN, SPARE + KMT:SPARE + KMT + 1])
    last64 = lane64 == NJ - 1
    kmt_north = jnp.where(last64, kmt_n, ahead(kmt))
    dep_north = jnp.where(last64, dep_n, ahead(depth))
    kmv_v = jnp.minimum(kmt, kmt_north)
    kmv[...] = kmv_v
    hv2[...] = keep(kmv_v > 0, 0.5 * (depth + dep_north))

    kmu_v = jnp.minimum(kmt, nd2[KMT, 1:NI + 1, :])
    kmu[...] = kmu_v
    hu2[...] = keep(kmu_v > 0, 0.5 * (depth + nd2[DEP, 1:NI + 1, :]))
    first_col = lax.broadcasted_iota(jnp.int32, (NI, NJ), 0) == 0
    kmw_v = jnp.minimum(kmt, jnp.where(first_col, near_w[KMT, WEST, :], pltpu.roll(kmt, 1, 0)))
    kmw[...] = kmw_v

    u0, v0 = keep(kmu_v > 0, st2[TU]), keep(kmv_v > 0, st2[TV])
    u0_west = jnp.where(first_col, keep(kmw_v > 0, near_u[0, WEST, :]), pltpu.roll(u0, 1, 0))
    v_s = in_s[TS, OWN, SPARE + SOUTH_V:SPARE + SOUTH_V + 1]
    v0_south = jnp.where(lane64 == 0, keep(jnp.minimum(kmt_s, kmt) > 0, v_s), back(v0))
    st2[STEP] = -WAVE_COURANT * ((u0 - u0_west) + (v0 - v0_south))
    wide2 = pk2n.at[0], pk2s.at[0], hs2.at[0], hn2.at[0]
    pack_flat(range(WIDE), st2, *wide2[:2])
    g2 = side_ew(st2, ext2)
    g2a_n, g2a_s = near_ns(*wide2)
    gc_n, gc_s = corners(*wide2)
    start(g2, g2a_n + gc_n, g2a_s + gc_s)
    for f in range(WIDE):
        ext2[f, CORE, :] = st2[f]

    def unpack_pair(a, where):
        north = keep(has_nf > 0.5, in_n[a, where, :])
        south = keep(has_sf > 0.5, in_s[a, where, :])
        even = (lax.broadcasted_iota(jnp.int32, north.shape, 1) & 1) == 0
        first = jnp.where(even, north, south)
        rr[2 * a, where, :] = 0.25 * first if a == UV else first
        rr[2 * a + 1, where, :] = jnp.where(even, ahead(north), back(south))

    def mean_rows():
        mean_n = rr[U, OWN, :] + rr[U, OFF - 1:OFF + NI - 1, :]
        mean_s = rr[V, OWN, :] + rr[V, OFF + 1:OFF + NI + 1, :]
        rr[MEAN, OWN, :] = jnp.where(even64, mean_n, mean_s)

    unpack_pair(TS, OWN)
    rt, rs = rr[T, OWN, :], rr[S, OWN, :]
    dens = keep((kmt_n > slot64.astype(F32)) & even64, BETA_S * rs - ALPHA_T * rt)
    above = lax.broadcasted_iota(jnp.int32, (NJ, NJ), 0) <= lax.broadcasted_iota(jnp.int32, (NJ, NJ), 1)
    total = jnp.dot(dens, above.astype(F32), precision=lax.Precision.HIGHEST, preferred_element_type=F32)
    rr[PRES, OWN, :] = (total - 0.5 * dens) * (2.0 * per_level(dep_n, kmt_n))
    recv((), g5n, g5s)
    rr[U, BEFORE, :] = jnp.zeros((OFF, NJ), F32)
    rr[V, AFTER, :] = jnp.zeros((OFF, NJ), F32)
    unpack_pair(UV, OWN)
    mean_rows()
    rv = rr[V, OWN, :]
    face_s = jnp.minimum(kmt_s, kmt[:, 0:1]) > slot64.astype(F32)
    vs_pos = keep(face_s, pos(rv))
    vs_neg = keep(face_s, neg(rv))
    rr[T_FLUX, OWN, :] = jnp.where(even64, rt, vs_pos * rt + vs_neg * pack[T])
    rr[S_FLUX, OWN, :] = jnp.where(even64, rs, vs_pos * rs + vs_neg * pack[S])

    def momentum_body(ib):
        at, mid, below, above = rows(ib), rows(ib, OFF), rows(ib, OFF - 1), rows(ib, OFF + 1)
        km_u = kmu[at, :]
        km_v = kmv[at, :]
        qu, qv, qm, qp = (rr[f, mid, :] for f in (U, V, MEAN, PRES))
        zero = jnp.zeros((8, NJ), F32)
        du, dv, st_u, st_v, sr_u, sr_v = (zero,) * 6
        turned = {}
        for step in range(LEVELS + LAG_M):
            k = step
            if k < LEVELS:
                sh = NJ - 1 - 2 * k
                turned[k] = (
                    rot(qu, sh), rot(qv, sh), rot(qm, sh), rot(qp, sh),
                    ahead(p3[k, mid, :]), ahead(t3[k, mid, :]), ahead(s3[k, mid, :]))
            k = step - LAG_M
            if k < 0:
                continue
            hu, hv, hm, hp, p_next, t_next, s_next = turned.pop(k)
            tn3[k, at, :] = t_next
            sn3[k, at, :] = s_next
            u = u3[k, mid, :]
            ue = u3[k, above, :]
            uw = u3[k, below, :]
            v = v3[k, mid, :]
            ve = v3[k, above, :]
            vw = v3[k, below, :]
            p = p3[k, mid, :]
            pe = p3[k, above, :]
            un_k, vs_k = un3[k, mid, :], vs3[k, mid, :]
            un = jnp.where(last8, hu, un_k)
            us = jnp.where(first8, hu, us3[k, at, :])
            vn = jnp.where(last8, hv, vn3[k, at, :])
            vs = jnp.where(first8, hv, vs_k)
            vm4 = (v + ve) + jnp.where(first8, hm, vs_k + vs3[k, above, :])
            um = 0.25 * (u + uw) + jnp.where(last8, hm, un_k + un3[k, below, :])
            pn = jnp.where(last8, hp, p_next)
            tu = (p - pe) - u * (ue - uw) - vm4 * (un - us)
            tv = (p - pn) - um * (ve - vw) - v * (vn - vs)
            wu = km_u > k
            wv = km_v > k
            st_u = st_u + keep(wu, tu)
            st_v = st_v + keep(wv, tv)
            ru_k = u + (0.5 * ADV_COURANT) * tu
            rv_k = v + (0.5 * ADV_COURANT) * tv
            sr_u = sr_u + keep(wu, ru_k)
            sr_v = sr_v + keep(wv, rv_k)
            du = ru_k + RATIO_V[k - 1] * du if k else ru_k
            dv = rv_k + RATIO_V[k - 1] * dv if k else rv_k
            du_o[k, at, :] = du
            dv_o[k, at, :] = dv
        inv_u = per_level(1.0, km_u)
        inv_v = per_level(1.0, km_v)
        ff[0, at, :] = hu2[at, :] * inv_u * (0.5 * st_u)
        ff[1, at, :] = hv2[at, :] * inv_v * (0.5 * st_v)
        smr[0, at, :] = inv_u * sr_u
        smr[1, at, :] = inv_v * sr_v

    def beside():
        recv(g1, g7n, g7s)
        unpack_pair(UV, BEFORE)
        unpack_pair(UV, AFTER)
        mean_rows()
        km_e = near_e[KMT, WEST, :]
        thick_e = 2.0 * per_level(near_e[DEP, WEST, :], km_e)
        tot_e = jnp.zeros((1, NJ), F32)
        for k in range(LEVELS):
            un3[k, WEST_HALO, :] = ahead(0.25 * u3[k, WEST_HALO, :])
            vs3[k, EAST_HALO, :] = back(v3[k, EAST_HALO, :])
            dens_e = keep(km_e > k, BETA_S * s3[k, EAST_HALO, :] - ALPHA_T * t3[k, EAST_HALO, :])
            tot_e = tot_e + dens_e
            p3[k, EAST_HALO, :] = (tot_e - 0.5 * dens_e) * thick_e

    def loop_body(n, carry):
        pl.when(n == blocks - 2)(beside)
        momentum_body(lax.rem(n + 1, blocks))
        return carry
    lax.fori_loop(0, blocks, loop_body, 0)

    force = pkfn.at[0], pkfs.at[0], hsf.at[0], hnf.at[0]
    g4 = side_ew(ff, extf)
    start(g4)
    pack_flat((0, 1), ff, *force[:2])
    g4_n, g4_s = near_ns(*force)
    half = HALO // 2
    g6_n, g6_s = [], []
    for n, (packed, row, out) in enumerate(((pkfn, up, g6_n), (pkfs, down, g6_s))):
        for m, (near, far, cc) in enumerate((
                (slice(NI - half, NI), slice(NI - HALO, NI - half), east),
                (slice(0, half), slice(half, HALO), west))):
            fold[n, m] = jnp.where(group64[:half] < 2, packed[0, near, :], rot(packed[0, far, :], 2 * HALO))
            out.append(remote(fold.at[n, m], fold_in.at[n, m], cc, row))
    start((), g6_n + g4_n, g6_s + g4_s)
    for f in range(2):
        extf[f, CORE, :] = ff[f]

    def tracer_body(ib, carry):
        first, last = edge_lanes(TALL)
        at, mid = rows(ib, 0, TALL), rows(ib, OFF, TALL)
        below, above = rows(ib, OFF - 1, TALL), rows(ib, OFF + 1, TALL)
        km_u = kmu[at, :]
        km_w = kmw[at, :]
        km_v = kmv[at, :]
        fields = ((t3, tn3, rr[T_FLUX, mid, :], dt_o), (s3, sn3, rr[S_FLUX, mid, :], ds_o))
        prev = [None, None]
        turned, flux = {}, {}
        for step in range(LEVELS + 2 * LAG):
            k = step
            if k < LEVELS:
                sh = NJ - 1 - 2 * k
                turned[k] = [rot(q, sh) for _, _, q, _ in fields]
            k = step - LAG
            if 0 <= k < LEVELS:
                v = keep(km_v > k, v3[k, mid, :])
                northward = v > 0
                flux[k] = []
                for (ref, next_ref, _, _), halo in zip(fields, turned.pop(k)):
                    xn = jnp.where(last, halo, next_ref[k, at, :])
                    fn = v * jnp.where(northward, ref[k, mid, :], xn)
                    flux[k].append((fn, back(fn), halo))
            k = step - 2 * LAG
            if k >= 0:
                u = keep(km_u > k, u3[k, mid, :])
                w = keep(km_w > k, u3[k, below, :])
                eastward, from_west = u > 0, w > 0
                for n, ((ref, _, _, out), (fn, fs, halo)) in enumerate(zip(fields, flux.pop(k))):
                    fs = jnp.where(first, halo, fs)
                    x = ref[k, mid, :]
                    fe = u * jnp.where(eastward, x, ref[k, above, :])
                    fw = w * jnp.where(from_west, ref[k, below, :], x)
                    rhs = x - ADV_COURANT * ((fe - fw) + (fn - fs))
                    prev[n] = rhs + RATIO_D[k - 1] * prev[n] if k else rhs
                    out[k, at, :] = prev[n]
        return carry
    lax.fori_loop(0, NI // TALL, tracer_body, 0)

    recv(g2, g2a_n + gc_n, g2a_s + gc_s)
    low_ok = jnp.full((HALO, IEXT), has_sf) > 0.5
    high_ok = jnp.full((HALO, IEXT), has_nf) > 0.5

    def window(ext, hs, hn, q):
        low = keep(low_ok, hs[HALO * q:HALO * (q + 1)])
        high = keep(high_ok, hn[HALO * q:HALO * (q + 1)])
        return jnp.concatenate([low, ext.T, high], axis=0)

    hs_t, hn_t = hs2[0].T, hn2[0].T
    win = pl.ds(8, JEXT)
    north_of = pl.ds(9, JEXT)
    south_of = pl.ds(7, JEXT)
    zpad = jnp.zeros((8, IEXT), F32)
    for ref in (b_e0, b_e1, b_wv, b_pv, b_s, b_g):
        ref[0:8, :] = zpad
        ref[8 + JEXT:16 + JEXT, :] = zpad
    dp_w = window(ext2[WET_DEP], hs_t, hn_t, WET_DEP)
    b_s[win, :] = dp_w
    dp_n, dp_e = b_s[north_of, :], ahead(dp_w)
    wet_u = (dp_w > 0) & (dp_e > 0)
    wet_v = (dp_w > 0) & (dp_n > 0)
    wu = keep(wet_u, (0.25 * WAVE_COURANT) * (dp_w + dp_e))
    wv = keep(wet_v, (0.25 * WAVE_COURANT) * (dp_w + dp_n))
    b_wu[...] = wu
    b_ww[...] = back(wu)
    b_wv[win, :] = wv
    b_e0[win, :] = keep(dp_w > 0, window(ext2[ETA], hs_t, hn_t, ETA))
    b_d[...] = window(ext2[STEP], hs_t, hn_t, STEP)

    def tracer_back(ib, carry):
        at = rows(ib, 0, TALL)
        kt = nd2[KMT, at, :]
        xt = xs = jnp.zeros((TALL, NJ), F32)
        for k in range(LEVELS - 1, -1, -1):
            fac = jnp.where(kt > k + 1, INNER_D[k], keep(kt > k, LAST_D[k]))
            xt = fac * dt_o[k, at, :] + RATIO_D[k] * xt
            xs = fac * ds_o[k, at, :] + RATIO_D[k] * xs
            dt_o[k, at, :] = xt
            ds_o[k, at, :] = xs
        return carry
    lax.fori_loop(0, NI // TALL, tracer_back, 0)

    recv(g4, g4_n + g6_n, g4_s + g6_s)
    for n, ref in enumerate((hsf, hnf)):
        for m, (near, far) in enumerate((
                (slice(half, HALO), slice(0, half)),
                (slice(IEXT - HALO, IEXT - half), slice(IEXT - half, IEXT)))):
            ref[0, near, :] = fold_in[n, m]
            ref[0, far, :] = rot(fold_in[n, m], 2 * HALO)
    hsf_t = hsf[0].T
    hnf_t = hnf[0].T
    push = ADV_COURANT / SUBCYCLES
    pu = keep(wet_u, push * window(extf[0], hsf_t, hnf_t, 0))
    pv = keep(wet_v, push * window(extf[1], hsf_t, hnf_t, 1))
    b_pu[...] = pu
    b_pv[win, :] = pv
    b_p[...] = -WAVE_COURANT * ((pu - back(pu)) + (pv - b_pv[south_of, :]))

    eta_bufs = (b_e0, b_e1)
    turned = {}
    for n in range(1, SUBCYCLES + 1):
        old, new = eta_bufs[(n - 1) % 2], eta_bufs[n % 2]
        fresh = {}
        for ch in range(JEXT // CHUNK):
            lo = CHUNK * ch
            if lo + CHUNK - 1 < HALO - (SUBCYCLES - n) or lo > HALO + NJ + (SUBCYCLES - n):
                continue
            here = pl.ds(lo, CHUNK)
            mid = pl.ds(8 + lo, CHUNK)
            e = old[mid, :]
            d = b_d[here, :]
            if n > 1:
                ee, ew = turned[ch]
                gain = b_wu[here, :] * (ee - e) - b_ww[here, :] * (e - ew)
                gain = gain + b_wv[mid, :] * (old[pl.ds(9 + lo, CHUNK), :] - e)
                gain = gain - b_wv[pl.ds(7 + lo, CHUNK), :] * (e - old[pl.ds(7 + lo, CHUNK), :])
                d = d + (gain + b_p[here, :])
                b_d[here, :] = d
            e = e + d
            new[mid, :] = e
            if n < SUBCYCLES:
                fresh[ch] = (ahead(e), back(e))
            if lo + CHUNK > HALO and lo <= HALO + NJ:
                tail = float(TAIL_WEIGHTS[n - 1])
                if n == 1:
                    b_s[mid, :] = e
                    b_g[mid, :] = tail * e
                else:
                    b_s[mid, :] = b_s[mid, :] + e
                    b_g[mid, :] = b_g[mid, :] + tail * e
        turned = fresh

    mid = pl.ds(8 + HALO, NJ)
    above = pl.ds(9 + HALO, NJ)
    core = pl.ds(HALO, NJ)
    last = eta_bufs[SUBCYCLES % 2]
    flat_o[0] = last[mid, :].T[CORE]
    wu = b_wu[core, :] * 2.0
    wv = b_wv[mid, :] * 2.0
    pu, pv = b_pu[core, :], b_pv[mid, :]
    u0, v0 = keep(kmu[...] > 0, st2[TU]), keep(kmv[...] > 0, st2[TV])
    s, g = b_s[mid, :], b_g[mid, :]
    flat_o[1] = u0 + (SUBCYCLES * pu - wu * (ahead(s) - s)).T[CORE]
    flat_o[2] = v0 + (SUBCYCLES * pv - wv * (b_s[above, :] - s)).T[CORE]
    mean_u = u0 + (MEAN_STEP * pu - wu * (ahead(g) - g)).T[CORE]
    mean_v = v0 + (MEAN_STEP * pv - wv * (b_g[above, :] - g)).T[CORE]
    for f, (mean, depth_ref, km_ref) in enumerate(((mean_u, hu2, kmu), (mean_v, hv2, kmv))):
        d = depth_ref[...]
        flat_o[3 + f] = mean / jnp.where(d > 0, d, 1.0) - smr[f]
        flat_o[5 + f] = km_ref[...]

    sent(g0 + g1)
    sent(g2, g3n + g5n + g7n, g3s + g5s + g7s)
    sent((), g2a_n + gc_n, g2a_s + gc_s)
    sent(g4, g4_n + g6_n, g4_s + g6_s)


CHUNKS = ((42, LEVELS), (21, 42), (0, 21))


def back_kernel(du, dv, t, s, flat, eta_h, tu_h, tv_h, u_h, v_h, t_h, s_h, xu, xv, sem2, sem3):
    whole = ((t, t_h), (s, s_h), (flat.at[0], eta_h), (flat.at[1], tu_h), (flat.at[2], tv_h))
    copies = [pltpu.make_async_copy(src, out, sem2.at[f]) for f, (src, out) in enumerate(whole)]
    for cp in copies:
        cp.start()
    results = ((xu, u_h), (xv, v_h))
    for n, (lo, hi) in enumerate(CHUNKS):
        def body(ib, carry):
            rows = pl.ds(pl.multiple_of(ib * 8, 8), 8)
            cu, cv, ku, kv = (flat[f, rows, :] for f in range(3, 7))
            x, y = (jnp.zeros((8, NJ), F32) if hi == LEVELS else ref[LEVELS, rows, :] for ref, _ in results)
            for k in range(hi - 1, lo - 1, -1):
                wu, wv = ku > k, kv > k
                fu = jnp.where(ku > k + 1, INNER_V[k], keep(wu, LAST_V[k]))
                fv = jnp.where(kv > k + 1, INNER_V[k], keep(wv, LAST_V[k]))
                x = fu * du[k, rows, :] + RATIO_V[k] * x
                y = fv * dv[k, rows, :] + RATIO_V[k] * y
                xu[k, rows, :] = keep(wu, x + cu)
                xv[k, rows, :] = keep(wv, y + cv)
            xu[LEVELS, rows, :] = x
            xv[LEVELS, rows, :] = y
            return carry
        lax.fori_loop(0, NI // 8, body, 0)
        for f, (src, out) in enumerate(results):
            cp = pltpu.make_async_copy(src.at[lo:hi], out.at[lo:hi], sem3.at[n, f])
            cp.start()
            copies.append(cp)
    for cp in copies:
        cp.wait()


def solution(mesh):
    col_count = mesh.shape['col']
    row_count = mesh.shape['row']

    def ocean_step(*args):
        flipped = [jnp.swapaxes(x, -1, -2) for x in args]
        cube = (LEVELS, NI, NJ)
        flat = (NI, NJ)
        dma = pltpu.SemaphoreType.DMA
        hbm = pl.BlockSpec(memory_space=pltpu.HBM)
        vmem = pl.BlockSpec(memory_space=VMEM)
        padded = VMEM((LEVELS, IPAD, NJ), F32)
        pair = VMEM((2,) + flat, F32)
        block = VMEM(cube, F32)
        folded = VMEM((2, 2, HALO // 2, NJ), F32)
        single = VMEM((1,) + flat, F32)
        near = VMEM((2, OFF, NJ), F32)
        wide = VMEM((JEXT + 16, IEXT), F32)
        plain = VMEM((JEXT, IEXT), F32)
        inner = pl.pallas_call(
            functools.partial(exchange_kernel, col_count, row_count),
            out_shape=tuple(VMEM(cube, F32) for _ in range(4)) + (VMEM((7,) + flat, F32),),
            in_specs=[hbm] * 9,
            out_specs=(vmem,) * 5,
            scratch_shapes=[
                padded, padded, padded, padded, padded, padded, block, block, padded, block, block,
                VMEM((5,) + flat, F32), VMEM((2, NI + OFF, NJ), F32), near, near, VMEM((1, OFF, NJ), F32),
                VMEM(flat, jnp.int32), VMEM((WIDE, IEXT, NJ), F32), single, single, VMEM((1, IEXT, NJ), F32), VMEM((1, IEXT, NJ), F32),
                VMEM((4,) + flat, F32), pair, pair,
                VMEM((2, IPAD, NJ), F32), VMEM((2, IPAD, NJ), F32), VMEM((8, IPAD, NJ), F32),
                pair, VMEM((2, IEXT, NJ), F32),
                single, single,
                VMEM((1, IEXT, NJ), F32), VMEM((1, IEXT, NJ), F32), folded, folded,
                VMEM(flat, F32), VMEM(flat, F32), VMEM(flat, F32),
                VMEM(flat, F32), VMEM(flat, F32), pair,
                wide, wide, plain, plain, plain, plain, wide, plain, wide, wide, wide,
                dma((4, len(PARTS))), dma((5,)), dma((MESSAGES,)), dma((MESSAGES,)),
            ],
            compiler_params=pltpu.CompilerParams(
                collective_id=0, has_side_effects=True, vmem_limit_bytes=54 * 2 ** 20),
        )(*flipped)
        spare = VMEM((LEVELS + 1,) + flat, F32)
        outs = pl.pallas_call(
            back_kernel,
            out_shape=tuple(jax.ShapeDtypeStruct(flat, F32) for _ in range(3))
            + tuple(jax.ShapeDtypeStruct(cube, F32) for _ in range(4)),
            in_specs=[vmem] * 5,
            out_specs=(hbm,) * 7,
            scratch_shapes=[spare, spare, dma((5,)), dma((len(CHUNKS), 2))],
            compiler_params=pltpu.CompilerParams(vmem_limit_bytes=40 * 2 ** 20),
        )(*inner)
        return tuple(jnp.swapaxes(x, -1, -2) for x in outs)

    spec_3d = P(None, 'row', 'col')
    spec_2d = P('row', 'col')
    return jax.shard_map(ocean_step, mesh=mesh, in_specs=(spec_3d,) * 4 + (spec_2d,) * 5, out_specs=(spec_2d,) * 3 + (spec_3d,) * 4, check_vma=False)
```
